32 devices in a mesh: stage: 4 (over y, z), data: 8 (over x, core).
Axes of the slice: x: 4, y: 2, z: 2, core: 2. Of those that a mesh axis runs over, the one named last changes fastest.
The devices are a block of a 4x4x8 slice.
Arguments:
- w_master: float32 [32, 768, 3072], P('stage', 'data'), parts along dimension 0
- momentum: float32 [32, 768, 3072], P('stage', 'data'), parts along dimension 0
- grad: bfloat16 [32, 768, 3072], P('stage', 'data'), parts along dimension 0
Outputs:
- output 1: bfloat16 [32, 768, 3072], P('stage'), parts along dimension 0
- output 2: float32 [32, 768, 3072], P('stage', 'data'), parts along dimension 0
There are 4 independent parts. The reference program is written for one: setup_inputs(seed, part) draws one part's arguments, and reference() takes and returns one part's arrays. A program takes and returns all parts, laid end to end along the dimension named above; each array names one.
All inputs are finite; a program needn't handle non-finite values.
Results may differ from the reference program's by a relative error of at most 0.00643818.
Values are sent between devices in bfloat16 or wider.
A program may use at most 768 MiB of HBM per device.

```python
import math
import jax
import jax.numpy as jnp
from jax import lax

DATA_DEVS = 8
MATS_DEV = 1
D = 768
FF_E = 3072
NS_ITERS = 5

MOMENTUM = 0.95
LEARN_RATE = 0.02
WEIGHT_DECAY = 0.1
NORM_EPS = 1e-7
COEF_A = 3.4445
COEF_B = -4.7750
COEF_C = 2.0315
RMS_SCALE = 0.2 * math.sqrt(max(D, FF_E))


def setup_inputs(seed: int = 0, part: int = 0) -> dict:
    mat_count = MATS_DEV * DATA_DEVS
    key = jax.random.fold_in(jax.random.key(seed), part)
    keys = jax.random.split(key, 7)
    w_master = 0.02 * jax.random.normal(keys[0], (mat_count, D, FF_E), jnp.float32)
    left_fac = jax.random.normal(keys[1], (mat_count, D, 4), jnp.float32)
    right_fac = jax.random.normal(keys[2], (mat_count, 4, FF_E), jnp.float32)
    shared = 0.25 * jnp.einsum("mdr,mrf->mdf", left_fac, right_fac)
    row_scale = jax.random.uniform(keys[3], (mat_count, D, 1), jnp.float32, 0.5, 2.0)
    momentum = row_scale * (jax.random.normal(keys[4], (mat_count, D, FF_E), jnp.float32) + shared)
    grad_scale = jax.random.uniform(keys[5], (mat_count, D, 1), jnp.float32, 0.5, 2.0)
    grad = (grad_scale * jax.random.normal(keys[6], (mat_count, D, FF_E), jnp.float32)).astype(jnp.bfloat16)
    return {"w_master": w_master, "momentum": momentum, "grad": grad}


def newton_schulz(x_mat):
    for iteration in range(NS_ITERS):
        gram_mat = jnp.dot(x_mat, x_mat.T, preferred_element_type=jnp.float32).astype(jnp.bfloat16)
        square = jnp.dot(gram_mat, gram_mat, preferred_element_type=jnp.float32)
        poly_mat = (COEF_B * gram_mat.astype(jnp.float32) + COEF_C * square).astype(jnp.bfloat16)
        prod_mat = jnp.dot(poly_mat, x_mat, preferred_element_type=jnp.float32)
        x_mat = (COEF_A * x_mat.astype(jnp.float32) + prod_mat).astype(jnp.bfloat16)
    return x_mat


def orthogonalize(mom_one):
    frob_norm = jnp.sqrt(jnp.sum(mom_one * mom_one))
    x_mat = (mom_one.astype(jnp.bfloat16).astype(jnp.float32) / (frob_norm + NORM_EPS)).astype(jnp.bfloat16)
    if D > FF_E:
        x_mat = newton_schulz(x_mat.T).T
    else:
        x_mat = newton_schulz(x_mat)
    return x_mat.astype(jnp.float32) * RMS_SCALE


def reference(w_master, momentum, grad):
    mom_new = MOMENTUM * momentum + grad.astype(jnp.float32)

    def update_one(w_and_m):
        w_one, mom_one = w_and_m
        w_new = w_one - LEARN_RATE * (orthogonalize(mom_one) + WEIGHT_DECAY * w_one)
        return w_new.astype(jnp.bfloat16)

    params = lax.map(update_one, (w_master, mom_new))
    return params, mom_new
```

```python
import functools
import math

import jax
import jax.numpy as jnp
from jax import lax
from jax.experimental import pallas as pl
from jax.experimental.pallas import tpu as pltpu
from jax.sharding import PartitionSpec as P

NS_ITERS = 5
MOMENTUM = 0.95
LEARN_RATE = 0.02
WEIGHT_DECAY = 0.1
NORM_EPS = 1e-7
COEF_A = 3.4445
COEF_B = -4.7750
COEF_C = 2.0315

MESH = pl.DeviceIdType.MESH
TILE = 256


def momentum_kernel(mom_ref, grad_ref, new_ref, low_ref, sq_ref):
    mom_new = MOMENTUM * mom_ref[0] + grad_ref[0].astype(jnp.float32)
    new_ref[0] = mom_new
    low_ref[0] = mom_new.astype(jnp.bfloat16)
    square = mom_new * mom_new
    rows, cols = square.shape
    lanes = square[:, :128]
    for start in range(128, cols, 128):
        lanes = lanes + square[:, start : start + 128]
    tile = lanes[:8]
    for start in range(8, rows, 8):
        tile = tile + lanes[start : start + 8]
    sq_ref[0] = tile


def momentum_step(mom, grad):
    mats, rows, cols = mom.shape
    block = pl.BlockSpec((1, rows, cols), lambda i: (i, 0, 0))
    return pl.pallas_call(
        momentum_kernel,
        grid=(mats,),
        in_specs=[block, block],
        out_specs=[block, block, pl.BlockSpec((1, 8, 128), lambda i: (i, 0, 0))],
        out_shape=[
            jax.ShapeDtypeStruct(mom.shape, jnp.float32),
            jax.ShapeDtypeStruct(mom.shape, jnp.bfloat16),
            jax.ShapeDtypeStruct((mats, 8, 128), jnp.float32),
        ],
    )(mom, grad)


def muon_kernel(group, low, sq_in, w, out, x, gram, poly, rows2, relay_a, relay_c, w2, back, new, sq, send, recv, go):
    chips = group // 2
    mats, rows, cols = low.shape
    pair = 2 * rows
    dim = pair * chips
    rms_scale = 0.2 * math.sqrt(max(dim, cols))
    me = lax.axis_index("data")
    c, k = lax.div(me, 2), lax.rem(me, 2)
    sib = 2 * c + 1 - k
    right, left, opp = (lax.rem(c + step, chips) for step in (1, chips - 1, 2))

    def peer_of(chip):
        return 2 * chip + k

    sent, slots = [], {}

    def slot(key):
        return slots.setdefault(key, len(slots))

    def push(src, dst, peer, key):
        copy = pltpu.make_async_remote_copy(
            src_ref=src, dst_ref=dst, send_sem=send.at[len(sent)], recv_sem=recv.at[slot(key)],
            device_id={"data": peer}, device_id_type=MESH)
        copy.start()
        sent.append(copy)

    def local(src, dst, key):
        copy = pltpu.make_async_copy(src, dst, recv.at[slot(key)])
        copy.start()

    def arrived(dst, key):
        pltpu.make_async_copy(dst, dst, recv.at[slot(key)]).wait()

    def span(start, size):
        return pl.ds(pl.multiple_of(start, rows), size)

    def own_rows(chip, half=None):
        if half is None:
            return span(chip * pair, pair)
        return span(chip * pair + half * rows, rows)

    barrier = pltpu.get_barrier_semaphore()
    for step in range(1, group):
        pl.semaphore_signal(barrier, inc=1, device_id={"data": lax.rem(me + step, group)}, device_id_type=MESH)
    pl.semaphore_wait(barrier, group - 1)

    for step, chip in enumerate((opp, right, left, c)):
        push(low.at[2 * chip + 1 - k], rows2.at[chip, span(k * rows, rows)], sib, ("swap", step))
        local(low.at[2 * chip + k], rows2.at[chip, span(k * rows, rows)], ("keep", step))
    for step in range(1, group):
        dest = lax.rem(me + step, group)
        push(sq_in.at[dest], sq.at[step], dest, ("sq", step))
    for step, chip in enumerate((c, left, right, opp)):
        push(w.at[2 * chip + 1 - k], w2.at[chip, span(k * rows, rows)], sib, ("wswap", step))
        local(w.at[2 * chip + k], w2.at[chip, span(k * rows, rows)], ("wkeep", step))

    @pl.when(k == 1)
    def _():
        pl.semaphore_wait(go, 1)

    def swapped(step, chip):
        arrived(rows2.at[chip, span((1 - k) * rows, rows)], ("swap", step))
        arrived(rows2.at[chip, span(k * rows, rows)], ("keep", step))

    swapped(0, opp)
    push(rows2.at[opp, pl.ds(0, rows)], relay_a.at[0], peer_of(right), "a_relay_l")
    push(rows2.at[opp, pl.ds(rows, rows)], relay_a.at[1], peer_of(left), "a_relay_r")
    swapped(1, right)
    push(rows2.at[right], x.at[own_rows(c)], peer_of(right), "a_left")
    swapped(2, left)
    push(rows2.at[left], x.at[own_rows(c)], peer_of(left), "a_right")
    arrived(relay_a.at[0], "a_relay_l")
    push(relay_a.at[0], x.at[own_rows(left, 0)], peer_of(right), "a_opp_l")
    arrived(relay_a.at[1], "a_relay_r")
    push(relay_a.at[1], x.at[own_rows(right, 1)], peer_of(left), "a_opp_r")
    swapped(3, c)

    total = sq_in[me]
    for step in range(1, group):
        arrived(sq.at[step], ("sq", step))
        total = total + sq[step]
    norm = jnp.sqrt(jnp.sum(total, keepdims=True))
    inverse = 1.0 / (norm + NORM_EPS)

    chunk = 32

    def scale(get, base, size):
        @pl.loop(0, size // chunk)
        def _(r):
            part = pl.ds(pl.multiple_of(base + r * chunk, chunk), chunk)
            x[part, :] = (get(r).astype(jnp.float32) * inverse).astype(jnp.bfloat16)

    def in_place(base):
        return lambda r: x[pl.ds(pl.multiple_of(base + r * chunk, chunk), chunk), :]

    scale(lambda r: rows2[c, pl.ds(pl.multiple_of(r * chunk, chunk), chunk), :], c * pair, pair)
    arrived(x.at[own_rows(left)], "a_left")
    scale(in_place(left * pair), left * pair, pair)
    arrived(x.at[own_rows(right)], "a_right")
    scale(in_place(right * pair), right * pair, pair)
    arrived(x.at[own_rows(opp, 0)], "a_opp_l")
    arrived(x.at[own_rows(opp, 1)], "a_opp_r")

    @pl.when(k == 0)
    def _():
        pl.semaphore_signal(go, inc=1, device_id={"data": sib}, device_id_type=MESH)

    scale(in_place(opp * pair), opp * pair, pair)

    @pl.loop(0, NS_ITERS)
    def _(_):
        @pl.loop(0, dim // TILE)
        def _(j):
            part = pl.ds(pl.multiple_of(j * TILE, TILE), TILE)
            gram[:, part] = lax.dot_general(
                x[...], x[part, :], (((1,), (1,)), ((), ())), preferred_element_type=jnp.float32
            ).astype(jnp.bfloat16)

        @pl.loop(0, dim // TILE)
        def _(j):
            part = pl.ds(pl.multiple_of(j * TILE, TILE), TILE)
            square = jnp.dot(gram[...], gram[:, part], preferred_element_type=jnp.float32)
            poly[:, part] = (COEF_B * gram[:, part].astype(jnp.float32) + COEF_C * square).astype(jnp.bfloat16)

        @pl.loop(0, cols // (2 * TILE))
        def _(j):
            part = pl.ds(pl.multiple_of(j * 2 * TILE, 2 * TILE), 2 * TILE)
            old = x[:, part]
            prod = jnp.dot(poly[...], old, preferred_element_type=jnp.float32)
            x[:, part] = (COEF_A * old.astype(jnp.float32) + prod).astype(jnp.bfloat16)

    push(x.at[own_rows(opp, 0)], relay_c.at[0], peer_of(right), "c_relay_l")
    push(x.at[own_rows(opp, 1)], relay_c.at[1], peer_of(left), "c_relay_r")
    push(x.at[own_rows(right)], back.at[c], peer_of(right), "c_left")
    push(x.at[own_rows(left)], back.at[c], peer_of(left), "c_right")

    step_rows = 16
    order = (0, chips - 1, 1, 2)

    def update(step, get):
        chip = lax.rem(c + order[step], chips)

        @pl.loop(0, pair // step_rows)
        def _(r):
            part = pl.ds(pl.multiple_of(r * step_rows, step_rows), step_rows)
            w_part = w2[chip, part, :]
            ortho = get(chip, r).astype(jnp.float32) * rms_scale
            new[chip, part, :] = (w_part - LEARN_RATE * (ortho + WEIGHT_DECAY * w_part)).astype(jnp.bfloat16)

        place = out.at[2 * chip + k, own_rows(c)]
        push(new.at[chip], place, peer_of(right), ("g_left", step))
        push(new.at[chip], place, peer_of(left), ("g_right", step))
        push(new.at[chip], place, sib, ("s_own", step))
        local(new.at[chip], place, ("own", step))

    for step, chip in enumerate((c, left, right, opp)):
        arrived(w2.at[chip, span((1 - k) * rows, rows)], ("wswap", step))
        arrived(w2.at[chip, span(k * rows, rows)], ("wkeep", step))
    update(0, lambda chip, r: x[pl.ds(pl.multiple_of(c * pair + r * step_rows, step_rows), step_rows), :])
    arrived(relay_c.at[0], "c_relay_l")
    push(relay_c.at[0], back.at[left, pl.ds(0, rows)], peer_of(right), "c_opp_l")
    arrived(relay_c.at[1], "c_relay_r")
    push(relay_c.at[1], back.at[right, pl.ds(rows, rows)], peer_of(left), "c_opp_r")

    def from_back(chip, r):
        return back[chip, pl.ds(pl.multiple_of(r * step_rows, step_rows), step_rows), :]

    arrived(back.at[left], "c_left")
    update(1, from_back)
    arrived(back.at[right], "c_right")
    update(2, from_back)
    arrived(back.at[opp, pl.ds(0, rows)], "c_opp_l")
    arrived(back.at[opp, pl.ds(rows, rows)], "c_opp_r")
    update(3, from_back)

    for step in range(chips):
        mat_l = 2 * lax.rem(left + order[step], chips) + k
        mat_r = 2 * lax.rem(right + order[step], chips) + k
        whole_l, whole_r = out.at[mat_l, own_rows(left)], out.at[mat_r, own_rows(right)]
        part_l, part_r = out.at[mat_l, own_rows(left, 0)], out.at[mat_r, own_rows(right, 1)]
        arrived(whole_l, ("g_left", step))
        push(part_l, part_l, peer_of(right), ("f_left", step))
        push(whole_l, whole_l, sib, ("s_left", step))
        arrived(whole_r, ("g_right", step))
        push(part_r, part_r, peer_of(left), ("f_right", step))
        push(whole_r, whole_r, sib, ("s_right", step))
    for step in range(chips):
        mat_o = 2 * lax.rem(opp + order[step], chips) + k
        part_l, part_r = out.at[mat_o, own_rows(opp, 0)], out.at[mat_o, own_rows(opp, 1)]
        arrived(part_l, ("f_left", step))
        push(part_l, part_l, sib, ("s_far_l", step))
        arrived(part_r, ("f_right", step))
        push(part_r, part_r, sib, ("s_far_r", step))
    for step in range(chips):
        mat = 2 * lax.rem(c + order[step], chips)
        arrived(out.at[mat + k, own_rows(c)], ("own", step))
        arrived(out.at[mat + 1 - k, own_rows(c)], ("s_own", step))
        arrived(out.at[2 * lax.rem(left + order[step], chips) + 1 - k, own_rows(left)], ("s_left", step))
        arrived(out.at[2 * lax.rem(right + order[step], chips) + 1 - k, own_rows(right)], ("s_right", step))
        mat_o = 2 * lax.rem(opp + order[step], chips) + 1 - k
        arrived(out.at[mat_o, own_rows(opp, 0)], ("s_far_l", step))
        arrived(out.at[mat_o, own_rows(opp, 1)], ("s_far_r", step))
    for copy in sent:
        copy.wait_send()


def muon_step(group, low, sq_in, w):
    mats, rows, cols = low.shape
    chips, pair = group // 2, 2 * rows
    dim = pair * chips
    hbm = pl.BlockSpec(memory_space=pl.ANY)
    return pl.pallas_call(
        functools.partial(muon_kernel, group),
        in_specs=[hbm, pl.BlockSpec(memory_space=pltpu.VMEM), hbm],
        out_specs=hbm,
        out_shape=jax.ShapeDtypeStruct((mats, dim, cols), jnp.bfloat16),
        scratch_shapes=[
            pltpu.VMEM((dim, cols), jnp.bfloat16),
            pltpu.VMEM((dim, dim), jnp.bfloat16),
            pltpu.VMEM((dim, dim), jnp.bfloat16),
            pltpu.VMEM((chips, pair, cols), jnp.bfloat16),
            pltpu.VMEM((2, rows, cols), jnp.bfloat16),
            pltpu.VMEM((2, rows, cols), jnp.bfloat16),
            pltpu.VMEM((chips, pair, cols), jnp.float32),
            pltpu.VMEM((chips, pair, cols), jnp.bfloat16),
            pltpu.VMEM((chips, pair, cols), jnp.bfloat16),
            pltpu.VMEM((group, 8, 128), jnp.float32),
            pltpu.SemaphoreType.DMA((80,)),
            pltpu.SemaphoreType.DMA((80,)),
            pltpu.SemaphoreType.REGULAR,
        ],
        compiler_params=pltpu.CompilerParams(
            collective_id=0, has_side_effects=True, vmem_limit_bytes=58 * 1024 * 1024
        ),
    )(low, sq_in, w)


def solution(mesh):
    group = mesh.shape["data"]
    row_spec = P("stage", "data", None)
    full_spec = P("stage", None, None)

    def local_step(w_rows, mom_rows, grad_rows):
        mom_new, low, square = momentum_step(mom_rows, grad_rows)
        params = muon_step(group, low, square, w_rows)
        return params, mom_new

    return jax.shard_map(
        local_step, mesh=mesh, in_specs=(row_spec, row_spec, row_spec), out_specs=(full_spec, row_spec), check_vma=False
    )
```

```python
import functools
import math

import jax
import jax.numpy as jnp
from jax import lax
from jax.experimental import pallas as pl
from jax.experimental.pallas import tpu as pltpu
from jax.sharding import PartitionSpec as P

NS_ITERS = 5
MOMENTUM = 0.95
LEARN_RATE = 0.02
WEIGHT_DECAY = 0.1
NORM_EPS = 1e-7
COEF_A = 3.4445
COEF_B = -4.7750
COEF_C = 2.0315

MESH = pl.DeviceIdType.MESH
TILE = 256


def momentum_kernel(mom_ref, grad_ref, new_ref, low_ref, sq_ref):
    mom_new = MOMENTUM * mom_ref[0] + grad_ref[0].astype(jnp.float32)
    new_ref[0] = mom_new
    low_ref[0] = mom_new.astype(jnp.bfloat16)
    square = mom_new * mom_new
    rows, cols = square.shape
    lanes = square[:, :128]
    for start in range(128, cols, 128):
        lanes = lanes + square[:, start : start + 128]
    tile = lanes[:8]
    for start in range(8, rows, 8):
        tile = tile + lanes[start : start + 8]
    sq_ref[0] = tile


def momentum_step(mom, grad):
    mats, rows, cols = mom.shape
    block = pl.BlockSpec((1, rows, cols), lambda i: (i, 0, 0))
    return pl.pallas_call(
        momentum_kernel,
        grid=(mats,),
        in_specs=[block, block],
        out_specs=[block, block, pl.BlockSpec((1, 8, 128), lambda i: (i, 0, 0))],
        out_shape=[
            jax.ShapeDtypeStruct(mom.shape, jnp.float32),
            jax.ShapeDtypeStruct(mom.shape, jnp.bfloat16),
            jax.ShapeDtypeStruct((mats, 8, 128), jnp.float32),
        ],
    )(mom, grad)


def muon_kernel(group, low, sq_in, w, out, x, gram, poly, relay_a, relay_c, w2, sq, send, recv, go, free):
    chips = group // 2
    mats, rows, cols = low.shape
    pair = 2 * rows
    dim = pair * chips
    rms_scale = 0.2 * math.sqrt(max(dim, cols))
    me = lax.axis_index("data")
    c, k = lax.div(me, 2), lax.rem(me, 2)
    sib = 2 * c + 1 - k
    right, left, opp = (lax.rem(c + step, chips) for step in (1, chips - 1, 2))

    def peer_of(chip):
        return 2 * chip + k

    def mine(chip, start=0, size=pair):
        return out.at[2 * chip + k, pl.ds(pl.multiple_of(c * pair + start, rows), size)]

    sent, slots = [], {}

    def slot(key):
        return slots.setdefault(key, len(slots))

    def push(src, dst, peer, key):
        copy = pltpu.make_async_remote_copy(
            src_ref=src, dst_ref=dst, send_sem=send.at[len(sent)], recv_sem=recv.at[slot(key)],
            device_id={"data": peer}, device_id_type=MESH)
        copy.start()
        sent.append(copy)
        return copy

    def local(src, dst, key):
        copy = pltpu.make_async_copy(src, dst, recv.at[slot(key)])
        copy.start()

    def arrived(dst, key):
        pltpu.make_async_copy(dst, dst, recv.at[slot(key)]).wait()

    def span(start, size):
        return pl.ds(pl.multiple_of(start, rows), size)

    def own_rows(chip, half=None):
        if half is None:
            return span(chip * pair, pair)
        return span(chip * pair + half * rows, rows)

    barrier = pltpu.get_barrier_semaphore()
    for step in range(1, group):
        pl.semaphore_signal(barrier, inc=1, device_id={"data": lax.rem(me + step, group)}, device_id_type=MESH)
    pl.semaphore_wait(barrier, group - 1)

    for step, chip in enumerate((opp, right, left, c)):
        push(low.at[2 * chip + 1 - k], out.at[2 * chip + 1 - k, own_rows(c, k)], sib, ("swap", step))
        local(low.at[2 * chip + k], mine(chip, k * rows, rows), ("keep", step))
    for step in range(1, group):
        dest = lax.rem(me + step, group)
        push(sq_in.at[dest], sq.at[step], dest, ("sq", step))
    for step, chip in enumerate((c, left, right, opp)):
        push(w.at[2 * chip + 1 - k], w2.at[chip, span(k * rows, rows)], sib, ("wswap", step))
        local(w.at[2 * chip + k], w2.at[chip, span(k * rows, rows)], ("wkeep", step))

    @pl.when(k == 1)
    def _():
        pl.semaphore_wait(go, 1)

    def swapped(step, chip):
        arrived(mine(chip, (1 - k) * rows, rows), ("swap", step))
        arrived(mine(chip, k * rows, rows), ("keep", step))

    swapped(0, opp)
    mine_sent = [
        push(mine(opp, 0, rows), relay_a.at[0], peer_of(right), "a_relay_l"),
        push(mine(opp, rows, rows), relay_a.at[1], peer_of(left), "a_relay_r"),
    ]
    swapped(1, right)
    mine_sent.append(push(mine(right), x.at[own_rows(c)], peer_of(right), "a_left"))
    swapped(2, left)
    mine_sent.append(push(mine(left), x.at[own_rows(c)], peer_of(left), "a_right"))
    arrived(relay_a.at[0], "a_relay_l")
    push(relay_a.at[0], x.at[own_rows(left, 0)], peer_of(right), "a_opp_l")
    arrived(relay_a.at[1], "a_relay_r")
    push(relay_a.at[1], x.at[own_rows(right, 1)], peer_of(left), "a_opp_r")
    swapped(3, c)

    total = sq_in[me]
    for step in range(1, group):
        arrived(sq.at[step], ("sq", step))
        total = total + sq[step]
    norm = jnp.sqrt(jnp.sum(total, keepdims=True))
    inverse = 1.0 / (norm + NORM_EPS)

    chunk = 32

    def scale(get, base, size):
        @pl.loop(0, size // chunk)
        def _(r):
            part = pl.ds(pl.multiple_of(base + r * chunk, chunk), chunk)
            x[part, :] = (get(r).astype(jnp.float32) * inverse).astype(jnp.bfloat16)

    def in_place(base):
        return lambda r: x[pl.ds(pl.multiple_of(base + r * chunk, chunk), chunk), :]

    scale(lambda r: out[2 * c + k, pl.ds(pl.multiple_of(c * pair + r * chunk, chunk), chunk), :], c * pair, pair)
    arrived(x.at[own_rows(left)], "a_left")
    scale(in_place(left * pair), left * pair, pair)
    arrived(x.at[own_rows(right)], "a_right")
    scale(in_place(right * pair), right * pair, pair)
    arrived(x.at[own_rows(opp, 0)], "a_opp_l")
    arrived(x.at[own_rows(opp, 1)], "a_opp_r")

    @pl.when(k == 0)
    def _():
        pl.semaphore_signal(go, inc=1, device_id={"data": sib}, device_id_type=MESH)

    scale(in_place(opp * pair), opp * pair, pair)

    for copy in mine_sent:
        copy.wait_send()
    for chip in (right, left):
        pl.semaphore_signal(free, inc=1, device_id={"data": peer_of(chip)}, device_id_type=MESH)

    @pl.loop(0, NS_ITERS)
    def _(_):
        @pl.loop(0, dim // TILE)
        def _(j):
            part = pl.ds(pl.multiple_of(j * TILE, TILE), TILE)
            gram[:, part] = lax.dot_general(
                x[...], x[part, :], (((1,), (1,)), ((), ())), preferred_element_type=jnp.float32
            ).astype(jnp.bfloat16)

        @pl.loop(0, dim // TILE)
        def _(j):
            part = pl.ds(pl.multiple_of(j * TILE, TILE), TILE)
            square = jnp.dot(gram[...], gram[:, part], preferred_element_type=jnp.float32)
            poly[:, part] = (COEF_B * gram[:, part].astype(jnp.float32) + COEF_C * square).astype(jnp.bfloat16)

        @pl.loop(0, cols // (2 * TILE))
        def _(j):
            part = pl.ds(pl.multiple_of(j * 2 * TILE, 2 * TILE), 2 * TILE)
            old = x[:, part]
            prod = jnp.dot(poly[...], old, preferred_element_type=jnp.float32)
            x[:, part] = (COEF_A * old.astype(jnp.float32) + prod).astype(jnp.bfloat16)

    pl.semaphore_wait(free, 2)
    push(x.at[own_rows(opp, 0)], relay_c.at[0], peer_of(right), "c_relay_l")
    push(x.at[own_rows(opp, 1)], relay_c.at[1], peer_of(left), "c_relay_r")
    push(x.at[own_rows(right)], out.at[2 * c + k, own_rows(right)], peer_of(right), "c_left")
    push(x.at[own_rows(left)], out.at[2 * c + k, own_rows(left)], peer_of(left), "c_right")

    step_rows = 16
    order = (0, chips - 1, 1, 2)

    def update(step, get):
        chip = lax.rem(c + order[step], chips)

        @pl.loop(0, pair // step_rows)
        def _(r):
            part = pl.ds(pl.multiple_of(r * step_rows, step_rows), step_rows)
            w_part = w2[chip, part, :]
            ortho = get(chip, r).astype(jnp.float32) * rms_scale
            out[2 * chip + k, pl.ds(pl.multiple_of(c * pair + r * step_rows, step_rows), step_rows), :] = (w_part - LEARN_RATE * (ortho + WEIGHT_DECAY * w_part)).astype(jnp.bfloat16)

        place = mine(chip)
        push(place, place, peer_of(right), ("g_left", step))
        push(place, place, peer_of(left), ("g_right", step))
        push(place, place, sib, ("s_own", step))

    for step, chip in enumerate((c, left, right, opp)):
        arrived(w2.at[chip, span((1 - k) * rows, rows)], ("wswap", step))
        arrived(w2.at[chip, span(k * rows, rows)], ("wkeep", step))
    update(0, lambda chip, r: x[pl.ds(pl.multiple_of(c * pair + r * step_rows, step_rows), step_rows), :])
    arrived(relay_c.at[0], "c_relay_l")
    push(relay_c.at[0], out.at[2 * left + k, own_rows(right, 0)], peer_of(right), "c_opp_l")
    arrived(relay_c.at[1], "c_relay_r")
    push(relay_c.at[1], out.at[2 * right + k, own_rows(left, 1)], peer_of(left), "c_opp_r")

    def from_back(chip, r):
        return out[2 * chip + k, pl.ds(pl.multiple_of(c * pair + r * step_rows, step_rows), step_rows), :]

    arrived(mine(left), "c_left")
    update(1, from_back)
    arrived(mine(right), "c_right")
    update(2, from_back)
    arrived(mine(opp, 0, rows), "c_opp_l")
    arrived(mine(opp, rows, rows), "c_opp_r")
    update(3, from_back)

    for step in range(chips):
        mat_l = 2 * lax.rem(left + order[step], chips) + k
        mat_r = 2 * lax.rem(right + order[step], chips) + k
        whole_l, whole_r = out.at[mat_l, own_rows(left)], out.at[mat_r, own_rows(right)]
        part_l, part_r = out.at[mat_l, own_rows(left, 0)], out.at[mat_r, own_rows(right, 1)]
        arrived(whole_l, ("g_left", step))
        push(part_l, part_l, peer_of(right), ("f_left", step))
        push(whole_l, whole_l, sib, ("s_left", step))
        arrived(whole_r, ("g_right", step))
        push(part_r, part_r, peer_of(left), ("f_right", step))
        push(whole_r, whole_r, sib, ("s_right", step))
    for step in range(chips):
        mat_o = 2 * lax.rem(opp + order[step], chips) + k
        part_l, part_r = out.at[mat_o, own_rows(opp, 0)], out.at[mat_o, own_rows(opp, 1)]
        arrived(part_l, ("f_left", step))
        push(part_l, part_l, sib, ("s_far_l", step))
        arrived(part_r, ("f_right", step))
        push(part_r, part_r, sib, ("s_far_r", step))
    for step in range(chips):
        mat = 2 * lax.rem(c + order[step], chips)
        arrived(out.at[mat + 1 - k, own_rows(c)], ("s_own", step))
        arrived(out.at[2 * lax.rem(left + order[step], chips) + 1 - k, own_rows(left)], ("s_left", step))
        arrived(out.at[2 * lax.rem(right + order[step], chips) + 1 - k, own_rows(right)], ("s_right", step))
        mat_o = 2 * lax.rem(opp + order[step], chips) + 1 - k
        arrived(out.at[mat_o, own_rows(opp, 0)], ("s_far_l", step))
        arrived(out.at[mat_o, own_rows(opp, 1)], ("s_far_r", step))
    for copy in sent:
        if not any(copy is done for done in mine_sent):
            copy.wait_send()


def muon_step(group, low, sq_in, w):
    mats, rows, cols = low.shape
    chips, pair = group // 2, 2 * rows
    dim = pair * chips
    hbm = pl.BlockSpec(memory_space=pl.ANY)
    return pl.pallas_call(
        functools.partial(muon_kernel, group),
        in_specs=[hbm, pl.BlockSpec(memory_space=pltpu.VMEM), hbm],
        out_specs=pl.BlockSpec(memory_space=pltpu.VMEM),
        out_shape=pltpu.VMEM((mats, dim, cols), jnp.bfloat16),
        scratch_shapes=[
            pltpu.VMEM((dim, cols), jnp.bfloat16),
            pltpu.VMEM((dim, dim), jnp.bfloat16),
            pltpu.VMEM((dim, dim), jnp.bfloat16),
            pltpu.VMEM((2, rows, cols), jnp.bfloat16),
            pltpu.VMEM((2, rows, cols), jnp.bfloat16),
            pltpu.VMEM((chips, pair, cols), jnp.float32),
            pltpu.VMEM((group, 8, 128), jnp.float32),
            pltpu.SemaphoreType.DMA((80,)),
            pltpu.SemaphoreType.DMA((80,)),
            pltpu.SemaphoreType.REGULAR,
            pltpu.SemaphoreType.REGULAR,
        ],
        compiler_params=pltpu.CompilerParams(
            collective_id=0, has_side_effects=True, vmem_limit_bytes=22 * 1024 * 1024
        ),
    )(low, sq_in, w)


def store_kernel(src, dst, sem):
    copies = [pltpu.make_async_copy(src.at[i], dst.at[i], sem.at[i]) for i in range(src.shape[0])]
    for copy in copies:
        copy.start()
    for copy in copies:
        copy.wait()


def store_step(full):
    return pl.pallas_call(
        store_kernel,
        in_specs=[pl.BlockSpec(memory_space=pltpu.VMEM)],
        out_specs=pl.BlockSpec(memory_space=pl.ANY),
        out_shape=jax.ShapeDtypeStruct(full.shape, full.dtype),
        scratch_shapes=[pltpu.SemaphoreType.DMA((full.shape[0],))],
        compiler_params=pltpu.CompilerParams(vmem_limit_bytes=1024 * 1024),
    )(full)


def solution(mesh):
    group = mesh.shape["data"]
    row_spec = P("stage", "data", None)
    full_spec = P("stage", None, None)

    def local_step(w_rows, mom_rows, grad_rows):
        mom_new, low, square = momentum_step(mom_rows, grad_rows)
        params = store_step(muon_step(group, low, square, w_rows))
        return params, mom_new

    return jax.shard_map(
        local_step, mesh=mesh, in_specs=(row_spec, row_spec, row_spec), out_specs=(full_spec, row_spec), check_vma=False
    )
```

```python
import functools
import math

import jax
import jax.numpy as jnp
from jax import lax
from jax.experimental import pallas as pl
from jax.experimental.pallas import tpu as pltpu
from jax.sharding import PartitionSpec as P

NS_ITERS = 5
MOMENTUM = 0.95
LEARN_RATE = 0.02
WEIGHT_DECAY = 0.1
NORM_EPS = 1e-7
COEF_A = 3.4445
COEF_B = -4.7750
COEF_C = 2.0315

MESH = pl.DeviceIdType.MESH
TILE = 256
WIDE = 1024
SCALE_ROWS = 32
STEP_ROWS = 16


def ds(start, size):
    return pl.ds(pl.multiple_of(start, math.gcd(size, TILE)), size)


def symmetric(dst, product, finish, dim):
    for j in range(0, dim, TILE):
        cols = slice(j, j + TILE)
        block = finish(product(slice(j, dim), cols), slice(j, dim), cols)
        dst[j:, cols] = block
        for i in range(j + TILE, dim, TILE):
            dst[cols, i : i + TILE] = block[i - j : i - j + TILE].T


def newton_schulz_poly(x, gram, poly):
    dim = gram.shape[0]

    def outer(rows, cols):
        return lax.dot_general(x[rows, :], x[cols, :], (((1,), (1,)), ((), ())), preferred_element_type=jnp.float32)

    def square(rows, cols):
        return jnp.dot(gram[rows, :], gram[:, cols], preferred_element_type=jnp.float32)

    symmetric(gram, outer, lambda prod, rows, cols: prod.astype(jnp.bfloat16), dim)
    symmetric(
        poly,
        square,
        lambda prod, rows, cols: (COEF_B * gram[rows, cols].astype(jnp.float32) + COEF_C * prod).astype(jnp.bfloat16),
        dim,
    )


def newton_schulz_step(x, poly, part):
    old = x[:, part]
    prod = jnp.dot(poly[...], old, preferred_element_type=jnp.float32)
    x[:, part] = (COEF_A * old.astype(jnp.float32) + prod).astype(jnp.bfloat16)


def muon_kernel(group, mom, grad, w, out, mom_new, w_sib, x, gram, poly, relay, w_buf, sq, send, recv, go, free):
    chips = group // 2
    mats, rows, cols = mom.shape
    pair = 2 * rows
    dim = pair * chips
    rms_scale = 0.2 * math.sqrt(max(dim, cols))
    me = lax.axis_index("data")
    c, k = lax.div(me, 2), lax.rem(me, 2)
    sib = 2 * c + 1 - k
    right, left, opp = (lax.rem(c + step, chips) for step in (1, chips - 1, 2))

    def peer_of(chip):
        return 2 * chip + k

    def own_rows(chip, half=None):
        if half is None:
            return ds(chip * pair, pair)
        return ds(chip * pair + half * rows, rows)

    def mine(chip, half=None):
        return out.at[2 * chip + k, own_rows(c, half)]

    sent, slots = [], {}

    def slot(key):
        return slots.setdefault(key, len(slots))

    def remote(src, dst, peer, key):
        copy = pltpu.make_async_remote_copy(
            src_ref=src, dst_ref=dst, send_sem=send.at[len(sent)], recv_sem=recv.at[slot(key)],
            device_id={"data": peer}, device_id_type=MESH)
        sent.append(copy)
        return copy

    def push(src, dst, peer, key):
        copy = remote(src, dst, peer, key)
        copy.start()
        return copy

    def load(src, dst, key):
        pltpu.make_async_copy(src, dst, recv.at[slot(key)]).start()

    def arrived(dst, key):
        pltpu.make_async_copy(dst, dst, recv.at[slot(key)]).wait()

    steps = (opp, right, left, c)
    for step, chip in enumerate(steps):
        for par in range(2):
            load(mom.at[2 * chip + par], mom_new.at[2 * chip + par], ("mom", step, par))
            load(grad.at[2 * chip + par], out.at[2 * chip + k, own_rows(left, par)], ("grad", step, par))

    barrier = pltpu.get_barrier_semaphore()
    for step in range(1, group):
        pl.semaphore_signal(barrier, inc=1, device_id={"data": lax.rem(me + step, group)}, device_id_type=MESH)
    pl.semaphore_wait(barrier, group - 1)

    def momentum(step, chip, par):
        mat = 2 * chip + par
        base = jnp.where(k == par, c * pair + k * rows, right * pair)
        arrived(mom_new.at[mat], ("mom", step, par))
        arrived(out.at[2 * chip + k, own_rows(left, par)], ("grad", step, par))

        def body(r, total):
            part = ds(r * STEP_ROWS, STEP_ROWS)
            low = out[2 * chip + k, ds(left * pair + par * rows + r * STEP_ROWS, STEP_ROWS), :]
            new = MOMENTUM * mom_new[mat, part, :] + low.astype(jnp.float32)
            mom_new[mat, part, :] = new
            out[2 * chip + k, ds(base + r * STEP_ROWS, STEP_ROWS), :] = new.astype(jnp.bfloat16)
            square = new * new
            lanes = square[:, :128]
            for start in range(128, cols, 128):
                lanes = lanes + square[:, start : start + 128]
            for start in range(0, STEP_ROWS, 8):
                total = total + lanes[start : start + 8]
            return total

        sq[0, mat] = lax.fori_loop(0, rows // STEP_ROWS, body, jnp.zeros((8, 128), jnp.float32))

    swap = [
        remote(out.at[2 * chip + k, own_rows(right, 0)], out.at[2 * chip + 1 - k, own_rows(c, k)], sib, ("swap", step))
        for step, chip in enumerate(steps)
    ]
    exchange = [
        [
            remote(mine(opp, 0), relay.at[0], peer_of(right), "a_relay_l"),
            remote(mine(opp, 1), relay.at[1], peer_of(left), "a_relay_r"),
        ],
        [remote(mine(right), x.at[own_rows(c)], peer_of(right), "a_left")],
        [remote(mine(left), x.at[own_rows(c)], peer_of(left), "a_right")],
        [],
    ]

    def send_rows(step, chip):
        arrived(mine(chip, 1 - k), ("swap", step))
        for copy in exchange[step]:
            copy.start()

    for step, chip in enumerate(steps):
        momentum(step, chip, 0)

        @pl.when(k == 1)
        def _():
            swap[step].start()

        @pl.when(k == 0)
        def _():
            send_rows(step, chip)

    for step, chip in enumerate(steps):
        momentum(step, chip, 1)

        @pl.when(k == 0)
        def _():
            swap[step].start()

    for step in range(1, group):
        dest = lax.rem(me + step, group)
        push(sq.at[0, dest], sq.at[1, step], dest, ("sq", step))
    for step, chip in enumerate((c, left, right, opp)):
        push(w.at[2 * chip + 1 - k], w_sib.at[chip], sib, ("w_swap", step))

    @pl.when(k == 1)
    def _():
        pl.semaphore_wait(go, 1)
        for step, chip in enumerate(steps):
            send_rows(step, chip)

    arrived(relay.at[0], "a_relay_l")
    pass_right = push(relay.at[0], x.at[own_rows(left, 0)], peer_of(right), "a_opp_l")
    arrived(relay.at[1], "a_relay_r")
    pass_left = push(relay.at[1], x.at[own_rows(right, 1)], peer_of(left), "a_opp_r")

    total = sq[0, me]
    for step in range(1, group):
        arrived(sq.at[1, step], ("sq", step))
        total = total + sq[1, step]
    norm = jnp.sqrt(jnp.sum(total, keepdims=True))
    inverse = 1.0 / (norm + NORM_EPS)

    def scale(get, base):
        @pl.loop(0, pair // SCALE_ROWS)
        def _(r):
            part = ds(base + r * SCALE_ROWS, SCALE_ROWS)
            x[part, :] = (get(part).astype(jnp.float32) * inverse).astype(jnp.bfloat16)

    scale(lambda part: out[2 * c + k, part, :], c * pair)
    arrived(x.at[own_rows(left)], "a_left")
    scale(lambda part: x[part, :], left * pair)
    arrived(x.at[own_rows(right)], "a_right")
    scale(lambda part: x[part, :], right * pair)
    arrived(x.at[own_rows(opp, 0)], "a_opp_l")
    arrived(x.at[own_rows(opp, 1)], "a_opp_r")

    @pl.when(k == 0)
    def _():
        pl.semaphore_signal(go, inc=1, device_id={"data": sib}, device_id_type=MESH)

    scale(lambda part: x[part, :], opp * pair)

    waited = swap + sum(exchange, []) + [pass_right, pass_left]
    for copy in waited:
        copy.wait_send()
    for chip in (right, left):
        pl.semaphore_signal(free, inc=1, device_id={"data": peer_of(chip)}, device_id_type=MESH)

    order = (c, left, right, opp)

    def load_w(step):
        load(w.at[2 * order[step] + k], w_buf.at[step % 2, ds(k * rows, rows)], ("w_own", step))
        arrived(w_sib.at[order[step]], ("w_swap", step))
        load(w_sib.at[order[step]], w_buf.at[step % 2, ds((1 - k) * rows, rows)], ("w_sib", step))

    load_w(0)
    load_w(1)

    @pl.loop(0, NS_ITERS - 1)
    def _(_):
        newton_schulz_poly(x, gram, poly)

        @pl.loop(0, cols // WIDE)
        def _(j):
            newton_schulz_step(x, poly, ds(j * WIDE, WIDE))

    newton_schulz_poly(x, gram, poly)
    pl.semaphore_wait(free, 2)

    chunks = [pl.ds(start, WIDE) for start in range(0, cols, WIDE)]
    for n, part in enumerate(chunks):
        newton_schulz_step(x, poly, part)
        push(x.at[own_rows(opp, 0), part], relay.at[0, :, part], peer_of(right), ("c_relay_l", n))
        push(x.at[own_rows(opp, 1), part], relay.at[1, :, part], peer_of(left), ("c_relay_r", n))
        push(x.at[own_rows(right), part], out.at[2 * c + k, own_rows(right), part], peer_of(right), ("c_left", n))
        push(x.at[own_rows(left), part], out.at[2 * c + k, own_rows(left), part], peer_of(left), ("c_right", n))

    def update(step, get):
        chip = order[step]
        arrived(w_buf.at[step % 2, ds(k * rows, rows)], ("w_own", step))
        arrived(w_buf.at[step % 2, ds((1 - k) * rows, rows)], ("w_sib", step))

        @pl.loop(0, pair // STEP_ROWS)
        def _(r):
            w_part = w_buf[step % 2, ds(r * STEP_ROWS, STEP_ROWS), :]
            part = ds(c * pair + r * STEP_ROWS, STEP_ROWS)
            ortho = get(chip, part).astype(jnp.float32) * rms_scale
            out[2 * chip + k, part, :] = (w_part - LEARN_RATE * (ortho + WEIGHT_DECAY * w_part)).astype(jnp.bfloat16)

        if step + 2 < chips:
            load_w(step + 2)
        push(mine(chip), mine(chip), peer_of(right), ("g_left", step))
        push(mine(chip), mine(chip), peer_of(left), ("g_right", step))
        push(mine(chip), mine(chip), sib, ("s_own", step))

    update(0, lambda chip, part: x[part, :])
    for n, part in enumerate(chunks):
        arrived(relay.at[0, :, part], ("c_relay_l", n))
        push(relay.at[0, :, part], out.at[2 * left + k, own_rows(right, 0), part], peer_of(right), ("c_opp_l", n))
        arrived(relay.at[1, :, part], ("c_relay_r", n))
        push(relay.at[1, :, part], out.at[2 * right + k, own_rows(left, 1), part], peer_of(left), ("c_opp_r", n))

    def returned(chip, part):
        return out[2 * chip + k, part, :]

    def x_rows(chip, half, part):
        return out.at[2 * chip + k, own_rows(c, half), part]

    for n, part in enumerate(chunks):
        arrived(x_rows(left, None, part), ("c_left", n))
    update(1, returned)
    for n, part in enumerate(chunks):
        arrived(x_rows(right, None, part), ("c_right", n))
    update(2, returned)
    for n, part in enumerate(chunks):
        arrived(x_rows(opp, 0, part), ("c_opp_l", n))
        arrived(x_rows(opp, 1, part), ("c_opp_r", n))
    update(3, returned)

    def near(chip, step):
        return lax.rem(chip + (0, chips - 1, 1, 2)[step], chips)

    for step in range(chips):
        mat_l, mat_r = 2 * near(left, step) + k, 2 * near(right, step) + k
        whole_l, whole_r = out.at[mat_l, own_rows(left)], out.at[mat_r, own_rows(right)]
        part_l, part_r = out.at[mat_l, own_rows(left, 0)], out.at[mat_r, own_rows(right, 1)]
        arrived(whole_l, ("g_left", step))
        push(part_l, part_l, peer_of(right), ("f_left", step))
        push(whole_l, whole_l, sib, ("s_left", step))
        arrived(whole_r, ("g_right", step))
        push(part_r, part_r, peer_of(left), ("f_right", step))
        push(whole_r, whole_r, sib, ("s_right", step))
    for step in range(chips):
        mat = 2 * near(opp, step) + k
        part_l, part_r = out.at[mat, own_rows(opp, 0)], out.at[mat, own_rows(opp, 1)]
        arrived(part_l, ("f_left", step))
        push(part_l, part_l, sib, ("s_far_l", step))
        arrived(part_r, ("f_right", step))
        push(part_r, part_r, sib, ("s_far_r", step))
    for step in range(chips):
        arrived(out.at[2 * near(c, step) + 1 - k, own_rows(c)], ("s_own", step))
        arrived(out.at[2 * near(left, step) + 1 - k, own_rows(left)], ("s_left", step))
        arrived(out.at[2 * near(right, step) + 1 - k, own_rows(right)], ("s_right", step))
        arrived(out.at[2 * near(opp, step) + 1 - k, own_rows(opp, 0)], ("s_far_l", step))
        arrived(out.at[2 * near(opp, step) + 1 - k, own_rows(opp, 1)], ("s_far_r", step))
    for copy in sent:
        if not any(copy is done for done in waited):
            copy.wait_send()


def muon_step(group, mom, grad, w):
    mats, rows, cols = mom.shape
    chips, pair = group // 2, 2 * rows
    dim = pair * chips
    hbm = pl.BlockSpec(memory_space=pl.ANY)
    vmem = pl.BlockSpec(memory_space=pltpu.VMEM)
    return pl.pallas_call(
        functools.partial(muon_kernel, group),
        in_specs=[hbm, hbm, hbm],
        out_specs=[vmem, vmem, hbm],
        out_shape=[
            pltpu.VMEM((mats, dim, cols), jnp.bfloat16),
            pltpu.VMEM((mats, rows, cols), jnp.float32),
            pltpu.HBM((chips, rows, cols), jnp.float32),
        ],
        scratch_shapes=[
            pltpu.VMEM((dim, cols), jnp.bfloat16),
            pltpu.VMEM((dim, dim), jnp.bfloat16),
            pltpu.VMEM((dim, dim), jnp.bfloat16),
            pltpu.VMEM((2, rows, cols), jnp.bfloat16),
            pltpu.VMEM((2, pair, cols), jnp.float32),
            pltpu.VMEM((2, group, 8, 128), jnp.float32),
            pltpu.SemaphoreType.DMA((128,)),
            pltpu.SemaphoreType.DMA((128,)),
            pltpu.SemaphoreType.REGULAR,
            pltpu.SemaphoreType.REGULAR,
        ],
        compiler_params=pltpu.CompilerParams(
            collective_id=0, has_side_effects=True, vmem_limit_bytes=15 * 1024 * 1024
        ),
    )(mom, grad, w)


def store_kernel(src, dst, sem):
    copies = [pltpu.make_async_copy(src.at[i], dst.at[i], sem.at[i]) for i in range(src.shape[0])]
    for copy in copies:
        copy.start()
    for copy in copies:
        copy.wait()


def store_step(full):
    return pl.pallas_call(
        store_kernel,
        in_specs=[pl.BlockSpec(memory_space=pltpu.VMEM)],
        out_specs=pl.BlockSpec(memory_space=pl.ANY),
        out_shape=jax.ShapeDtypeStruct(full.shape, full.dtype),
        scratch_shapes=[pltpu.SemaphoreType.DMA((full.shape[0],))],
        compiler_params=pltpu.CompilerParams(vmem_limit_bytes=1024 * 1024),
    )(full)


def solution(mesh):
    group = mesh.shape["data"]
    row_spec = P("stage", "data", None)
    full_spec = P("stage", None, None)

    def local_step(w_rows, mom_rows, grad_rows):
        params, mom_new, _ = muon_step(group, mom_rows, grad_rows, w_rows)
        return store_step(params), store_step(mom_new)

    return jax.shard_map(
        local_step, mesh=mesh, in_specs=(row_spec, row_spec, row_spec), out_specs=(full_spec, row_spec), check_vma=False
    )
```

```python
import functools
import math

import jax
import jax.numpy as jnp
from jax import lax
from jax.experimental import pallas as pl
from jax.experimental.pallas import tpu as pltpu
from jax.sharding import PartitionSpec as P

NS_ITERS = 5
MOMENTUM = 0.95
LEARN_RATE = 0.02
WEIGHT_DECAY = 0.1
NORM_EPS = 1e-7
COEF_A = 3.4445
COEF_B = -4.7750
COEF_C = 2.0315

MESH = pl.DeviceIdType.MESH
TILE = 256
WIDE = 1024
SCALE_ROWS = 32
STEP_ROWS = 16


def ds(start, size):
    return pl.ds(pl.multiple_of(start, math.gcd(size, TILE)), size)


def symmetric(dst, product, finish, dim):
    for j in range(0, dim, TILE):
        cols = slice(j, j + TILE)
        block = finish(product(slice(j, dim), cols), slice(j, dim), cols)
        dst[j:, cols] = block
        for i in range(j + TILE, dim, TILE):
            dst[cols, i : i + TILE] = block[i - j : i - j + TILE].T


def newton_schulz_poly(x, gram, poly):
    dim = gram.shape[0]

    def outer(rows, cols):
        return lax.dot_general(x[rows, :], x[cols, :], (((1,), (1,)), ((), ())), preferred_element_type=jnp.float32)

    def square(rows, cols):
        return jnp.dot(gram[rows, :], gram[:, cols], preferred_element_type=jnp.float32)

    symmetric(gram, outer, lambda prod, rows, cols: prod.astype(jnp.bfloat16), dim)
    symmetric(
        poly,
        square,
        lambda prod, rows, cols: (COEF_B * gram[rows, cols].astype(jnp.float32) + COEF_C * prod).astype(jnp.bfloat16),
        dim,
    )


def newton_schulz_step(x, poly, part):
    old = x[:, part]
    prod = jnp.dot(poly[...], old, preferred_element_type=jnp.float32)
    x[:, part] = (COEF_A * old.astype(jnp.float32) + prod).astype(jnp.bfloat16)


def muon_kernel(group, mom, grad, w, out, mom_new, w_sib, tail_r, tail_l, x, gram, poly, relay, w_buf, sq, send, recv, go, free):
    chips = group // 2
    mats, rows, cols = mom.shape
    pair = 2 * rows
    dim = pair * chips
    rms_scale = 0.2 * math.sqrt(max(dim, cols))
    me = lax.axis_index("data")
    c, k = lax.div(me, 2), lax.rem(me, 2)
    sib = 2 * c + 1 - k
    right, left, opp = (lax.rem(c + step, chips) for step in (1, chips - 1, 2))

    def peer_of(chip):
        return 2 * chip + k

    def own_rows(chip, half=None):
        if half is None:
            return ds(chip * pair, pair)
        return ds(chip * pair + half * rows, rows)

    def mine(chip, half=None):
        return out.at[2 * chip + k, own_rows(c, half)]

    sent, slots = [], {}

    def slot(key):
        return slots.setdefault(key, len(slots))

    def remote(src, dst, peer, key):
        copy = pltpu.make_async_remote_copy(
            src_ref=src, dst_ref=dst, send_sem=send.at[len(sent)], recv_sem=recv.at[slot(key)],
            device_id={"data": peer}, device_id_type=MESH)
        sent.append(copy)
        return copy

    def push(src, dst, peer, key):
        copy = remote(src, dst, peer, key)
        copy.start()
        return copy

    def load(src, dst, key):
        pltpu.make_async_copy(src, dst, recv.at[slot(key)]).start()

    def arrived(dst, key):
        pltpu.make_async_copy(dst, dst, recv.at[slot(key)]).wait()

    steps = (opp, right, left, c)
    for step, chip in enumerate(steps):
        for par in range(2):
            load(mom.at[2 * chip + par], mom_new.at[2 * chip + par], ("mom", step, par))
            load(grad.at[2 * chip + par], out.at[2 * chip + k, own_rows(left, par)], ("grad", step, par))

    barrier = pltpu.get_barrier_semaphore()
    for step in range(1, group):
        pl.semaphore_signal(barrier, inc=1, device_id={"data": lax.rem(me + step, group)}, device_id_type=MESH)
    pl.semaphore_wait(barrier, group - 1)

    def momentum(step, chip, par):
        mat = 2 * chip + par
        base = jnp.where(k == par, c * pair + k * rows, right * pair)
        arrived(mom_new.at[mat], ("mom", step, par))
        arrived(out.at[2 * chip + k, own_rows(left, par)], ("grad", step, par))

        def body(r, total):
            part = ds(r * STEP_ROWS, STEP_ROWS)
            low = out[2 * chip + k, ds(left * pair + par * rows + r * STEP_ROWS, STEP_ROWS), :]
            new = MOMENTUM * mom_new[mat, part, :] + low.astype(jnp.float32)
            mom_new[mat, part, :] = new
            out[2 * chip + k, ds(base + r * STEP_ROWS, STEP_ROWS), :] = new.astype(jnp.bfloat16)
            square = new * new
            lanes = square[:, :128]
            for start in range(128, cols, 128):
                lanes = lanes + square[:, start : start + 128]
            for start in range(0, STEP_ROWS, 8):
                total = total + lanes[start : start + 8]
            return total

        sq[0, mat] = lax.fori_loop(0, rows // STEP_ROWS, body, jnp.zeros((8, 128), jnp.float32))

    swap = [
        remote(out.at[2 * chip + k, own_rows(right, 0)], out.at[2 * chip + 1 - k, own_rows(c, k)], sib, ("swap", step))
        for step, chip in enumerate(steps)
    ]
    exchange = [
        [
            remote(mine(opp, 0), relay.at[0], peer_of(right), "a_relay_l"),
            remote(mine(opp, 1), relay.at[1], peer_of(left), "a_relay_r"),
        ],
        [remote(mine(right), x.at[own_rows(c)], peer_of(right), "a_left")],
        [remote(mine(left), x.at[own_rows(c)], peer_of(left), "a_right")],
        [],
    ]

    def send_rows(step, chip):
        arrived(mine(chip, 1 - k), ("swap", step))
        for copy in exchange[step]:
            copy.start()

    for step, chip in enumerate(steps):
        momentum(step, chip, 0)

        @pl.when(k == 1)
        def _():
            swap[step].start()

        @pl.when(k == 0)
        def _():
            send_rows(step, chip)

    for step, chip in enumerate(steps):
        momentum(step, chip, 1)

        @pl.when(k == 0)
        def _():
            swap[step].start()

    for step in range(1, group):
        dest = lax.rem(me + step, group)
        push(sq.at[0, dest], sq.at[1, step], dest, ("sq", step))
    for step, chip in enumerate((c, left, right, opp)):
        push(w.at[2 * chip + 1 - k], w_sib.at[chip], sib, ("w_swap", step))

    @pl.when(k == 1)
    def _():
        pl.semaphore_wait(go, 1)
        for step, chip in enumerate(steps):
            send_rows(step, chip)

    arrived(relay.at[0], "a_relay_l")
    pass_right = push(relay.at[0], x.at[own_rows(left, 0)], peer_of(right), "a_opp_l")
    arrived(relay.at[1], "a_relay_r")
    pass_left = push(relay.at[1], x.at[own_rows(right, 1)], peer_of(left), "a_opp_r")

    total = sq[0, me]
    for step in range(1, group):
        arrived(sq.at[1, step], ("sq", step))
        total = total + sq[1, step]
    norm = jnp.sqrt(jnp.sum(total, keepdims=True))
    inverse = 1.0 / (norm + NORM_EPS)

    def scale(get, base):
        @pl.loop(0, pair // SCALE_ROWS)
        def _(r):
            part = ds(base + r * SCALE_ROWS, SCALE_ROWS)
            x[part, :] = (get(part).astype(jnp.float32) * inverse).astype(jnp.bfloat16)

    scale(lambda part: out[2 * c + k, part, :], c * pair)
    arrived(x.at[own_rows(left)], "a_left")
    scale(lambda part: x[part, :], left * pair)
    arrived(x.at[own_rows(right)], "a_right")
    scale(lambda part: x[part, :], right * pair)
    arrived(x.at[own_rows(opp, 0)], "a_opp_l")
    arrived(x.at[own_rows(opp, 1)], "a_opp_r")

    @pl.when(k == 0)
    def _():
        pl.semaphore_signal(go, inc=1, device_id={"data": sib}, device_id_type=MESH)

    scale(lambda part: x[part, :], opp * pair)

    waited = swap + sum(exchange, []) + [pass_right, pass_left]
    for copy in waited:
        copy.wait_send()
    for chip in (right, left):
        pl.semaphore_signal(free, inc=1, device_id={"data": peer_of(chip)}, device_id_type=MESH)

    order = (c, left, right, opp)

    def load_w(step):
        load(w.at[2 * order[step] + k], w_buf.at[step % 2, ds(k * rows, rows)], ("w_own", step))
        arrived(w_sib.at[order[step]], ("w_swap", step))
        load(w_sib.at[order[step]], w_buf.at[step % 2, ds((1 - k) * rows, rows)], ("w_sib", step))

    load_w(0)
    load_w(1)

    @pl.loop(0, NS_ITERS - 1)
    def _(_):
        newton_schulz_poly(x, gram, poly)
        newton_schulz_step(x, poly, pl.ds(0, cols))

    newton_schulz_poly(x, gram, poly)
    pl.semaphore_wait(free, 2)

    chunks = [pl.ds(start, WIDE) for start in range(0, cols, WIDE)]
    for n, part in enumerate(chunks):
        newton_schulz_step(x, poly, part)
        push(x.at[own_rows(opp, 0), part], relay.at[0, :, part], peer_of(right), ("c_relay_l", n))
        push(x.at[own_rows(opp, 1), part], relay.at[1, :, part], peer_of(left), ("c_relay_r", n))
        push(x.at[own_rows(right), part], out.at[2 * c + k, own_rows(right), part], peer_of(right), ("c_left", n))
        push(x.at[own_rows(left), part], out.at[2 * c + k, own_rows(left), part], peer_of(left), ("c_right", n))

    def update(step, get):
        chip = order[step]
        arrived(w_buf.at[step % 2, ds(k * rows, rows)], ("w_own", step))
        arrived(w_buf.at[step % 2, ds((1 - k) * rows, rows)], ("w_sib", step))

        @pl.loop(0, pair // STEP_ROWS)
        def _(r):
            w_part = w_buf[step % 2, ds(r * STEP_ROWS, STEP_ROWS), :]
            part = ds(c * pair + r * STEP_ROWS, STEP_ROWS)
            ortho = get(chip, part).astype(jnp.float32) * rms_scale
            out[2 * chip + k, part, :] = (w_part - LEARN_RATE * (ortho + WEIGHT_DECAY * w_part)).astype(jnp.bfloat16)

        if step + 2 < chips:
            load_w(step + 2)
        push(mine(chip), mine(chip), peer_of(right), ("g_left", step))
        push(mine(chip), mine(chip), peer_of(left), ("g_right", step))
        push(mine(chip), mine(chip), sib, ("s_own", step))

    update(0, lambda chip, part: x[part, :])
    for n, part in enumerate(chunks):
        arrived(relay.at[0, :, part], ("c_relay_l", n))
        push(relay.at[0, :, part], out.at[2 * left + k, own_rows(right, 0), part], peer_of(right), ("c_opp_l", n))
        arrived(relay.at[1, :, part], ("c_relay_r", n))
        push(relay.at[1, :, part], out.at[2 * right + k, own_rows(left, 1), part], peer_of(left), ("c_opp_r", n))

    def returned(chip, part):
        return out[2 * chip + k, part, :]

    def x_rows(chip, half, part):
        return out.at[2 * chip + k, own_rows(c, half), part]

    for n, part in enumerate(chunks):
        arrived(x_rows(left, None, part), ("c_left", n))
    update(1, returned)
    for n, part in enumerate(chunks):
        arrived(x_rows(right, None, part), ("c_right", n))
    update(2, returned)
    for n, part in enumerate(chunks):
        arrived(x_rows(opp, 0, part), ("c_opp_l", n))
        arrived(x_rows(opp, 1, part), ("c_opp_r", n))
    update(3, returned)

    def near(chip, step):
        return lax.rem(chip + (0, chips - 1, 1, 2)[step], chips)

    last = chips - 1
    for step in range(chips):
        mat_l, mat_r = 2 * near(left, step) + k, 2 * near(right, step) + k
        whole_l, whole_r = out.at[mat_l, own_rows(left)], out.at[mat_r, own_rows(right)]
        part_l, part_r = out.at[mat_l, own_rows(left, 0)], out.at[mat_r, own_rows(right, 1)]
        arrived(whole_l, ("g_left", step))
        if step < last:
            push(part_l, part_l, peer_of(right), ("f_left", step))
        else:
            load(part_l, tail_r, "tail_r")
        push(whole_l, whole_l, sib, ("s_left", step))
        arrived(whole_r, ("g_right", step))
        if step < last:
            push(part_r, part_r, peer_of(left), ("f_right", step))
        else:
            load(part_r, tail_l, "tail_l")
        push(whole_r, whole_r, sib, ("s_right", step))
    for step in range(last):
        mat = 2 * near(opp, step) + k
        part_l, part_r = out.at[mat, own_rows(opp, 0)], out.at[mat, own_rows(opp, 1)]
        arrived(part_l, ("f_left", step))
        push(part_l, part_l, sib, ("s_far_l", step))
        arrived(part_r, ("f_right", step))
        push(part_r, part_r, sib, ("s_far_r", step))
    for step in range(chips):
        arrived(out.at[2 * near(c, step) + 1 - k, own_rows(c)], ("s_own", step))
        arrived(out.at[2 * near(left, step) + 1 - k, own_rows(left)], ("s_left", step))
        arrived(out.at[2 * near(right, step) + 1 - k, own_rows(right)], ("s_right", step))
        if step < last:
            arrived(out.at[2 * near(opp, step) + 1 - k, own_rows(opp, 0)], ("s_far_l", step))
            arrived(out.at[2 * near(opp, step) + 1 - k, own_rows(opp, 1)], ("s_far_r", step))
    arrived(tail_r, "tail_r")
    arrived(tail_l, "tail_l")
    for copy in sent:
        if not any(copy is done for done in waited):
            copy.wait_send()


def muon_step(group, mom, grad, w):
    mats, rows, cols = mom.shape
    chips, pair = group // 2, 2 * rows
    dim = pair * chips
    hbm = pl.BlockSpec(memory_space=pl.ANY)
    vmem = pl.BlockSpec(memory_space=pltpu.VMEM)
    return pl.pallas_call(
        functools.partial(muon_kernel, group),
        in_specs=[hbm, hbm, hbm],
        out_specs=[vmem, vmem, hbm, hbm, hbm],
        out_shape=[
            pltpu.VMEM((mats, dim, cols), jnp.bfloat16),
            pltpu.VMEM((mats, rows, cols), jnp.float32),
            pltpu.HBM((chips, rows, cols), jnp.float32),
            pltpu.HBM((rows, cols), jnp.bfloat16),
            pltpu.HBM((rows, cols), jnp.bfloat16),
        ],
        scratch_shapes=[
            pltpu.VMEM((dim, cols), jnp.bfloat16),
            pltpu.VMEM((dim, dim), jnp.bfloat16),
            pltpu.VMEM((dim, dim), jnp.bfloat16),
            pltpu.VMEM((2, rows, cols), jnp.bfloat16),
            pltpu.VMEM((2, pair, cols), jnp.float32),
            pltpu.VMEM((2, group, 8, 128), jnp.float32),
            pltpu.SemaphoreType.DMA((128,)),
            pltpu.SemaphoreType.DMA((128,)),
            pltpu.SemaphoreType.REGULAR,
            pltpu.SemaphoreType.REGULAR,
        ],
        compiler_params=pltpu.CompilerParams(
            collective_id=0, has_side_effects=True, vmem_limit_bytes=15 * 1024 * 1024
        ),
    )(mom, grad, w)


def store_kernel(src, dst, sem):
    copies = [pltpu.make_async_copy(src.at[i], dst.at[i], sem.at[i]) for i in range(src.shape[0])]
    for copy in copies:
        copy.start()
    for copy in copies:
        copy.wait()


def store_step(full):
    return pl.pallas_call(
        store_kernel,
        in_specs=[pl.BlockSpec(memory_space=pltpu.VMEM)],
        out_specs=pl.BlockSpec(memory_space=pl.ANY),
        out_shape=jax.ShapeDtypeStruct(full.shape, full.dtype),
        scratch_shapes=[pltpu.SemaphoreType.DMA((full.shape[0],))],
        compiler_params=pltpu.CompilerParams(vmem_limit_bytes=1024 * 1024),
        cost_estimate=pl.CostEstimate(flops=1000 * full.size, bytes_accessed=2 * full.size, transcendentals=0),
    )(full)


def tail_kernel(params, near_l, near_r, far_l, far_r, out, buf, sem):
    rows = buf.shape[1]
    pair = 2 * rows
    chips = params.shape[1] // pair
    me = lax.axis_index("data")
    c, k = lax.div(me, 2), lax.rem(me, 2)
    start = lax.rem(c + 2, chips) * pair
    pieces = ((near_l, k, 0), (near_r, k, 1), (far_l, 1 - k, 0), (far_r, 1 - k, 1))
    loads = [pltpu.make_async_copy(src, buf.at[n], sem.at[n]) for n, (src, _, _) in enumerate(pieces)]
    stores = [
        pltpu.make_async_copy(buf.at[n], out.at[2 * c + par, pl.ds(pl.multiple_of(start + half * rows, rows), rows)], sem.at[n])
        for n, (_, par, half) in enumerate(pieces)
    ]
    for copy in loads:
        copy.start()
    for copy, store in zip(loads, stores):
        copy.wait()
        store.start()
    for store in stores:
        store.wait()


def tail_step(params, pieces):
    hbm = pl.BlockSpec(memory_space=pl.ANY)
    return pl.pallas_call(
        tail_kernel,
        in_specs=[hbm] * 5,
        out_specs=hbm,
        out_shape=jax.ShapeDtypeStruct(params.shape, params.dtype),
        input_output_aliases={0: 0},
        scratch_shapes=[pltpu.VMEM((4, *pieces[0].shape), pieces[0].dtype), pltpu.SemaphoreType.DMA((4,))],
        compiler_params=pltpu.CompilerParams(vmem_limit_bytes=4 * 1024 * 1024),
    )(params, *pieces)


def solution(mesh):
    group = mesh.shape["data"]
    row_spec = P("stage", "data", None)
    full_spec = P("stage", None, None)

    def local_step(w_rows, mom_rows, grad_rows):
        params, mom_new, _, tail_r, tail_l = muon_step(group, mom_rows, grad_rows, w_rows)
        to_right = [(d, (d + 2) % group) for d in range(group)]
        to_left = [(d, (d - 2) % group) for d in range(group)]
        swap = [(d, d + 1 - 2 * (d % 2)) for d in range(group)]
        near = [lax.ppermute(tail_r, "data", to_right), lax.ppermute(tail_l, "data", to_left)]
        params = store_step(params)
        *near, params = lax.optimization_barrier((*near, params))
        far = [lax.ppermute(piece, "data", swap) for piece in near]
        mom_new = store_step(mom_new)
        *far, mom_new = lax.optimization_barrier((*far, mom_new))
        return tail_step(params, near + far), mom_new

    return jax.shard_map(
        local_step, mesh=mesh, in_specs=(row_spec, row_spec, row_spec), out_specs=(full_spec, row_spec), check_vma=False
    )
```

```python
import functools
import math

import jax
import jax.numpy as jnp
from jax import lax
from jax.experimental import pallas as pl
from jax.experimental.pallas import tpu as pltpu
from jax.sharding import PartitionSpec as P

NS_ITERS = 5
MOMENTUM = 0.95
LEARN_RATE = 0.02
WEIGHT_DECAY = 0.1
NORM_EPS = 1e-7
COEF_A = 3.4445
COEF_B = -4.7750
COEF_C = 2.0315

MESH = pl.DeviceIdType.MESH
TILE = 256
WIDE = 1024
SCALE_ROWS = 32
STEP_ROWS = 16


def ds(start, size):
    return pl.ds(pl.multiple_of(start, math.gcd(size, STEP_ROWS)), size)


def symmetric(dst, product, finish, dim):
    for j in range(0, dim, TILE):
        cols = slice(j, j + TILE)
        block = finish(product(slice(j, dim), cols), slice(j, dim), cols)
        dst[j:, cols] = block
        for i in range(j + TILE, dim, TILE):
            dst[cols, i : i + TILE] = block[i - j : i - j + TILE].T


def newton_schulz_poly(x, gram, poly):
    dim = gram.shape[0]

    def outer(rows, cols):
        return lax.dot_general(x[rows, :], x[cols, :], (((1,), (1,)), ((), ())), preferred_element_type=jnp.float32)

    def square(rows, cols):
        return jnp.dot(gram[rows, :], gram[:, cols], preferred_element_type=jnp.float32)

    symmetric(gram, outer, lambda prod, rows, cols: prod.astype(jnp.bfloat16), dim)
    symmetric(
        poly,
        square,
        lambda prod, rows, cols: (COEF_B * gram[rows, cols].astype(jnp.float32) + COEF_C * prod).astype(jnp.bfloat16),
        dim,
    )


def newton_schulz_step(x, poly, part):
    old = x[:, part]
    prod = jnp.dot(poly[...], old, preferred_element_type=jnp.float32)
    x[:, part] = (COEF_A * old.astype(jnp.float32) + prod).astype(jnp.bfloat16)


def muon_kernel(group, mom, grad, w, out, mom_new, w_sib, tail_r, tail_l, x, gram, poly, relay, w_buf, w_ahead, sq, send, recv, go, free):
    chips = group // 2
    mats, rows, cols = mom.shape
    pair = 2 * rows
    dim = pair * chips
    rms_scale = 0.2 * math.sqrt(max(dim, cols))
    me = lax.axis_index("data")
    c, k = lax.div(me, 2), lax.rem(me, 2)
    sib = 2 * c + 1 - k
    right, left, opp = (lax.rem(c + step, chips) for step in (1, chips - 1, 2))

    def peer_of(chip):
        return 2 * chip + k

    def own_rows(chip, half=None):
        if half is None:
            return ds(chip * pair, pair)
        return ds(chip * pair + half * rows, rows)

    ahead = rows // 2
    ahead_start, rest_start, rest = k * (pair - ahead), (1 - k) * ahead, pair - ahead

    def ahead_rows(chip):
        return ds(chip * pair + ahead_start, ahead)

    def rest_rows(chip):
        return ds(chip * pair + rest_start, rest)

    split = STEP_ROWS * (rest // STEP_ROWS // 2)
    sizes = ((rows, rows), (rest - split, split), (split, rest - split), (rows, rows))

    def block(chip, step):
        return rest_rows(chip) if step in (1, 2) else own_rows(chip)

    def block_part(chip, step, way):
        start = rest_start if step in (1, 2) else 0
        return ds(chip * pair + start + way * sizes[step][0], sizes[step][way])

    def mine(chip, half=None):
        return out.at[2 * chip + k, own_rows(c, half)]

    sent, slots = [], {}

    def slot(key):
        return slots.setdefault(key, len(slots))

    def remote(src, dst, peer, key):
        copy = pltpu.make_async_remote_copy(
            src_ref=src, dst_ref=dst, send_sem=send.at[len(sent)], recv_sem=recv.at[slot(key)],
            device_id={"data": peer}, device_id_type=MESH)
        sent.append(copy)
        return copy

    def push(src, dst, peer, key):
        copy = remote(src, dst, peer, key)
        copy.start()
        return copy

    def load(src, dst, key):
        pltpu.make_async_copy(src, dst, recv.at[slot(key)]).start()

    def arrived(dst, key):
        pltpu.make_async_copy(dst, dst, recv.at[slot(key)]).wait()

    steps = (opp, right, left, c)
    for step, chip in enumerate(steps):
        for par in range(2):
            load(mom.at[2 * chip + par], mom_new.at[2 * chip + par], ("mom", step, par))
            load(grad.at[2 * chip + par], out.at[2 * chip + k, own_rows(left, par)], ("grad", step, par))

    barrier = pltpu.get_barrier_semaphore()
    for step in range(1, group):
        pl.semaphore_signal(barrier, inc=1, device_id={"data": lax.rem(me + step, group)}, device_id_type=MESH)
    pl.semaphore_wait(barrier, group - 1)

    def momentum(step, chip, par):
        mat = 2 * chip + par
        base = jnp.where(k == par, c * pair + k * rows, right * pair)
        arrived(mom_new.at[mat], ("mom", step, par))
        arrived(out.at[2 * chip + k, own_rows(left, par)], ("grad", step, par))

        def body(r, total):
            part = ds(r * STEP_ROWS, STEP_ROWS)
            low = out[2 * chip + k, ds(left * pair + par * rows + r * STEP_ROWS, STEP_ROWS), :]
            new = MOMENTUM * mom_new[mat, part, :] + low.astype(jnp.float32)
            mom_new[mat, part, :] = new
            out[2 * chip + k, ds(base + r * STEP_ROWS, STEP_ROWS), :] = new.astype(jnp.bfloat16)
            square = new * new
            lanes = square[:, :128]
            for start in range(128, cols, 128):
                lanes = lanes + square[:, start : start + 128]
            for start in range(0, STEP_ROWS, 8):
                total = total + lanes[start : start + 8]
            return total

        sq[0, mat] = lax.fori_loop(0, rows // STEP_ROWS, body, jnp.zeros((8, 128), jnp.float32))

    swap = [
        remote(out.at[2 * chip + k, own_rows(right, 0)], out.at[2 * chip + 1 - k, own_rows(c, k)], sib, ("swap", step))
        for step, chip in enumerate(steps)
    ]
    exchange = [
        [
            remote(mine(opp, 0), relay.at[0], peer_of(right), "a_relay_l"),
            remote(mine(opp, 1), relay.at[1], peer_of(left), "a_relay_r"),
        ],
        [remote(mine(right), x.at[own_rows(c)], peer_of(right), "a_left")],
        [remote(mine(left), x.at[own_rows(c)], peer_of(left), "a_right")],
        [],
    ]

    def send_rows(step, chip):
        arrived(mine(chip, 1 - k), ("swap", step))
        for copy in exchange[step]:
            copy.start()

    for step, chip in enumerate(steps):
        momentum(step, chip, 0)

        @pl.when(k == 1)
        def _():
            swap[step].start()

        @pl.when(k == 0)
        def _():
            send_rows(step, chip)

    for step, chip in enumerate(steps):
        momentum(step, chip, 1)

        @pl.when(k == 0)
        def _():
            swap[step].start()

    for step in range(1, group):
        dest = lax.rem(me + step, group)
        push(sq.at[0, dest], sq.at[1, step], dest, ("sq", step))
    for step, chip in enumerate((c, left, right, opp)):
        push(w.at[2 * chip + 1 - k], w_sib.at[chip], sib, ("w_swap", step))

    @pl.when(k == 1)
    def _():
        pl.semaphore_wait(go, 1)
        for step, chip in enumerate(steps):
            send_rows(step, chip)

    arrived(relay.at[0], "a_relay_l")
    pass_right = push(relay.at[0], x.at[own_rows(left, 0)], peer_of(right), "a_opp_l")
    arrived(relay.at[1], "a_relay_r")
    pass_left = push(relay.at[1], x.at[own_rows(right, 1)], peer_of(left), "a_opp_r")
    push(w.at[2 * right + k, ds(k * ahead, ahead)], w_ahead.at[0], peer_of(right), "w_ahead_l")
    push(w.at[2 * left + k, ds(k * ahead, ahead)], w_ahead.at[1], peer_of(left), "w_ahead_r")

    total = sq[0, me]
    for step in range(1, group):
        arrived(sq.at[1, step], ("sq", step))
        total = total + sq[1, step]
    norm = jnp.sqrt(jnp.sum(total, keepdims=True))
    inverse = 1.0 / (norm + NORM_EPS)

    def scale(get, base):
        @pl.loop(0, pair // SCALE_ROWS)
        def _(r):
            part = ds(base + r * SCALE_ROWS, SCALE_ROWS)
            x[part, :] = (get(part).astype(jnp.float32) * inverse).astype(jnp.bfloat16)

    scale(lambda part: out[2 * c + k, part, :], c * pair)
    arrived(x.at[own_rows(left)], "a_left")
    scale(lambda part: x[part, :], left * pair)
    arrived(x.at[own_rows(right)], "a_right")
    scale(lambda part: x[part, :], right * pair)
    arrived(x.at[own_rows(opp, 0)], "a_opp_l")
    arrived(x.at[own_rows(opp, 1)], "a_opp_r")

    @pl.when(k == 0)
    def _():
        pl.semaphore_signal(go, inc=1, device_id={"data": sib}, device_id_type=MESH)

    scale(lambda part: x[part, :], opp * pair)

    waited = swap + sum(exchange, []) + [pass_right, pass_left]
    for copy in waited:
        copy.wait_send()
    for chip in (right, left):
        pl.semaphore_signal(free, inc=1, device_id={"data": peer_of(chip)}, device_id_type=MESH)

    order = (c, left, right, opp)

    def load_w(step):
        load(w.at[2 * order[step] + k], w_buf.at[step % 2, ds(k * rows, rows)], ("w_own", step))
        arrived(w_sib.at[order[step]], ("w_swap", step))
        load(w_sib.at[order[step]], w_buf.at[step % 2, ds((1 - k) * rows, rows)], ("w_sib", step))

    load_w(0)
    load_w(1)

    @pl.loop(0, NS_ITERS - 1)
    def _(_):
        newton_schulz_poly(x, gram, poly)
        newton_schulz_step(x, poly, pl.ds(0, cols))

    newton_schulz_poly(x, gram, poly)
    pl.semaphore_wait(free, 2)

    chunks = [pl.ds(start, WIDE) for start in range(0, cols, WIDE)]
    for n, part in enumerate(chunks):
        newton_schulz_step(x, poly, part)
        push(x.at[own_rows(opp, 0), part], relay.at[0, :, part], peer_of(right), ("c_relay_l", n))
        push(x.at[own_rows(opp, 1), part], relay.at[1, :, part], peer_of(left), ("c_relay_r", n))
        push(x.at[rest_rows(right), part], out.at[2 * c + k, rest_rows(right), part], peer_of(right), ("c_left", n))
        push(x.at[rest_rows(left), part], out.at[2 * c + k, rest_rows(left), part], peer_of(left), ("c_right", n))

    def new_rows(mat, start, size, w_rows, get):
        @pl.loop(0, size // STEP_ROWS)
        def _(r):
            w_part = w_rows(r)
            part = ds(start + r * STEP_ROWS, STEP_ROWS)
            ortho = get(part).astype(jnp.float32) * rms_scale
            out[mat, part, :] = (w_part - LEARN_RATE * (ortho + WEIGHT_DECAY * w_part)).astype(jnp.bfloat16)

    def update(step, get):
        chip = order[step]
        arrived(w_buf.at[step % 2, ds(k * rows, rows)], ("w_own", step))
        arrived(w_buf.at[step % 2, ds((1 - k) * rows, rows)], ("w_sib", step))
        start, size = (rest_start, rest) if step in (1, 2) else (0, pair)
        new_rows(
            2 * chip + k, c * pair + start, size, lambda r: w_buf[step % 2, ds(start + r * STEP_ROWS, STEP_ROWS), :],
            lambda part: get(chip, part))
        if step + 2 < chips:
            load_w(step + 2)
        place = out.at[2 * chip + k, block(c, step)]
        push(place, place, peer_of(right), ("g_left", step))
        push(place, place, peer_of(left), ("g_right", step))
        push(place, place, sib, ("s_own", step))

    def update_ahead():
        for n, chip in enumerate((left, right)):
            arrived(w_ahead.at[n], ("w_ahead_l", "w_ahead_r")[n])
            new_rows(
                2 * c + k, chip * pair + ahead_start, ahead, lambda r: w_ahead[n, ds(r * STEP_ROWS, STEP_ROWS), :],
                lambda part: x[part, :])
            place = out.at[2 * c + k, ahead_rows(chip)]
            push(place, place, peer_of(right), ("e_left", n))
            push(place, place, peer_of(left), ("e_right", n))
            push(place, place, sib, ("s_ahead", n))

    update(0, lambda chip, part: x[part, :])
    update_ahead()
    for n, part in enumerate(chunks):
        arrived(relay.at[0, :, part], ("c_relay_l", n))
        push(relay.at[0, :, part], out.at[2 * left + k, own_rows(right, 0), part], peer_of(right), ("c_opp_l", n))
        arrived(relay.at[1, :, part], ("c_relay_r", n))
        push(relay.at[1, :, part], out.at[2 * right + k, own_rows(left, 1), part], peer_of(left), ("c_opp_r", n))

    def returned(chip, part):
        return out[2 * chip + k, part, :]

    for n, part in enumerate(chunks):
        arrived(out.at[2 * left + k, rest_rows(c), part], ("c_left", n))
    update(1, returned)
    for n, part in enumerate(chunks):
        arrived(out.at[2 * right + k, rest_rows(c), part], ("c_right", n))
    update(2, returned)
    for n, part in enumerate(chunks):
        arrived(out.at[2 * opp + k, own_rows(c, 0), part], ("c_opp_l", n))
        arrived(out.at[2 * opp + k, own_rows(c, 1), part], ("c_opp_r", n))
    update(3, returned)

    def near(chip, step):
        return lax.rem(chip + (0, chips - 1, 1, 2)[step], chips)

    def pass_on(mat, part, peer, key):
        push(out.at[mat, part], out.at[mat, part], peer, key)

    last = chips - 1
    for step in range(chips):
        mat_l, mat_r = 2 * near(left, step) + k, 2 * near(right, step) + k
        arrived(out.at[mat_l, block(left, step)], ("g_left", step))
        if step < last:
            pass_on(mat_l, block_part(left, step, 0), peer_of(right), ("f_left", step))
        else:
            load(out.at[mat_l, block_part(left, step, 0)], tail_r, "tail_r")
        pass_on(mat_l, block(left, step), sib, ("s_left", step))
        arrived(out.at[mat_r, block(right, step)], ("g_right", step))
        if step < last:
            pass_on(mat_r, block_part(right, step, 1), peer_of(left), ("f_right", step))
        else:
            load(out.at[mat_r, block_part(right, step, 1)], tail_l, "tail_l")
        pass_on(mat_r, block(right, step), sib, ("s_right", step))
        if step == 0:
            arrived(out.at[mat_l, ahead_rows(opp)], ("e_left", 0))
            pass_on(mat_l, ahead_rows(opp), peer_of(right), "fe_left")
            pass_on(mat_l, ahead_rows(opp), sib, ("s_ahead_l", 0))
            arrived(out.at[mat_l, ahead_rows(c)], ("e_left", 1))
            pass_on(mat_l, ahead_rows(c), sib, ("s_ahead_l", 1))
            arrived(out.at[mat_r, ahead_rows(c)], ("e_right", 0))
            pass_on(mat_r, ahead_rows(c), sib, ("s_ahead_r", 0))
            arrived(out.at[mat_r, ahead_rows(opp)], ("e_right", 1))
            pass_on(mat_r, ahead_rows(opp), peer_of(left), "fe_right")
            pass_on(mat_r, ahead_rows(opp), sib, ("s_ahead_r", 1))
    for step in range(last):
        mat = 2 * near(opp, step) + k
        arrived(out.at[mat, block_part(opp, step, 0)], ("f_left", step))
        pass_on(mat, block_part(opp, step, 0), sib, ("s_far_l", step))
        arrived(out.at[mat, block_part(opp, step, 1)], ("f_right", step))
        pass_on(mat, block_part(opp, step, 1), sib, ("s_far_r", step))
        if step == 0:
            arrived(out.at[mat, ahead_rows(right)], "fe_left")
            pass_on(mat, ahead_rows(right), sib, "s_far_ahead_l")
            arrived(out.at[mat, ahead_rows(left)], "fe_right")
            pass_on(mat, ahead_rows(left), sib, "s_far_ahead_r")

    def sib_ahead(chip):
        return ds(chip * pair + (1 - k) * (pair - ahead), ahead)

    def sib_start(chip, step):
        return chip * pair + (k * ahead if step in (1, 2) else 0)

    for step in range(chips):
        size = sum(sizes[step])
        arrived(out.at[2 * near(c, step) + 1 - k, ds(sib_start(c, step), size)], ("s_own", step))
        arrived(out.at[2 * near(left, step) + 1 - k, ds(sib_start(left, step), size)], ("s_left", step))
        arrived(out.at[2 * near(right, step) + 1 - k, ds(sib_start(right, step), size)], ("s_right", step))
        if step < last:
            mat, start = 2 * near(opp, step) + 1 - k, sib_start(opp, step)
            arrived(out.at[mat, ds(start, sizes[step][0])], ("s_far_l", step))
            arrived(out.at[mat, ds(start + sizes[step][0], sizes[step][1])], ("s_far_r", step))
        if step == 0:
            for n, chip in enumerate((left, right)):
                arrived(out.at[2 * c + 1 - k, sib_ahead(chip)], ("s_ahead", n))
            for n, chip in enumerate((opp, c)):
                arrived(out.at[2 * left + 1 - k, sib_ahead(chip)], ("s_ahead_l", n))
            for n, chip in enumerate((c, opp)):
                arrived(out.at[2 * right + 1 - k, sib_ahead(chip)], ("s_ahead_r", n))
            arrived(out.at[2 * opp + 1 - k, sib_ahead(right)], "s_far_ahead_l")
            arrived(out.at[2 * opp + 1 - k, sib_ahead(left)], "s_far_ahead_r")
    arrived(tail_r, "tail_r")
    arrived(tail_l, "tail_l")
    for copy in sent:
        if not any(copy is done for done in waited):
            copy.wait_send()


def muon_step(group, mom, grad, w):
    mats, rows, cols = mom.shape
    chips, pair = group // 2, 2 * rows
    dim = pair * chips
    hbm = pl.BlockSpec(memory_space=pl.ANY)
    vmem = pl.BlockSpec(memory_space=pltpu.VMEM)
    return pl.pallas_call(
        functools.partial(muon_kernel, group),
        in_specs=[hbm, hbm, hbm],
        out_specs=[vmem, vmem, hbm, hbm, hbm],
        out_shape=[
            pltpu.VMEM((mats, dim, cols), jnp.bfloat16),
            pltpu.VMEM((mats, rows, cols), jnp.float32),
            pltpu.HBM((chips, rows, cols), jnp.float32),
            pltpu.HBM((rows, cols), jnp.bfloat16),
            pltpu.HBM((rows, cols), jnp.bfloat16),
        ],
        scratch_shapes=[
            pltpu.VMEM((dim, cols), jnp.bfloat16),
            pltpu.VMEM((dim, dim), jnp.bfloat16),
            pltpu.VMEM((dim, dim), jnp.bfloat16),
            pltpu.VMEM((2, rows, cols), jnp.bfloat16),
            pltpu.VMEM((2, pair, cols), jnp.float32),
            pltpu.VMEM((2, rows // 2, cols), jnp.float32),
            pltpu.VMEM((2, group, 8, 128), jnp.float32),
            pltpu.SemaphoreType.DMA((128,)),
            pltpu.SemaphoreType.DMA((128,)),
            pltpu.SemaphoreType.REGULAR,
            pltpu.SemaphoreType.REGULAR,
        ],
        compiler_params=pltpu.CompilerParams(
            collective_id=0, has_side_effects=True, vmem_limit_bytes=16 * 1024 * 1024
        ),
    )(mom, grad, w)


def store_kernel(src, dst, sem):
    copies = [pltpu.make_async_copy(src.at[i], dst.at[i], sem.at[i]) for i in range(src.shape[0])]
    for copy in copies:
        copy.start()
    for copy in copies:
        copy.wait()


def store_step(full):
    return pl.pallas_call(
        store_kernel,
        in_specs=[pl.BlockSpec(memory_space=pltpu.VMEM)],
        out_specs=pl.BlockSpec(memory_space=pl.ANY),
        out_shape=jax.ShapeDtypeStruct(full.shape, full.dtype),
        scratch_shapes=[pltpu.SemaphoreType.DMA((full.shape[0],))],
        compiler_params=pltpu.CompilerParams(vmem_limit_bytes=1024 * 1024),
        cost_estimate=pl.CostEstimate(flops=1000 * full.size, bytes_accessed=2 * full.size, transcendentals=0),
    )(full)


def tail_kernel(params, near_l, near_r, far_l, far_r, out, buf, sem):
    rows = buf.shape[1]
    pair = 2 * rows
    chips = params.shape[1] // pair
    me = lax.axis_index("data")
    c, k = lax.div(me, 2), lax.rem(me, 2)
    start = lax.rem(c + 2, chips) * pair
    pieces = ((near_l, k, 0), (near_r, k, 1), (far_l, 1 - k, 0), (far_r, 1 - k, 1))
    loads = [pltpu.make_async_copy(src, buf.at[n], sem.at[n]) for n, (src, _, _) in enumerate(pieces)]
    stores = [
        pltpu.make_async_copy(buf.at[n], out.at[2 * c + par, pl.ds(pl.multiple_of(start + half * rows, rows), rows)], sem.at[n])
        for n, (_, par, half) in enumerate(pieces)
    ]
    for copy in loads:
        copy.start()
    for copy, store in zip(loads, stores):
        copy.wait()
        store.start()
    for store in stores:
        store.wait()


def tail_step(params, pieces):
    hbm = pl.BlockSpec(memory_space=pl.ANY)
    return pl.pallas_call(
        tail_kernel,
        in_specs=[hbm] * 5,
        out_specs=hbm,
        out_shape=jax.ShapeDtypeStruct(params.shape, params.dtype),
        input_output_aliases={0: 0},
        scratch_shapes=[pltpu.VMEM((4, *pieces[0].shape), pieces[0].dtype), pltpu.SemaphoreType.DMA((4,))],
        compiler_params=pltpu.CompilerParams(vmem_limit_bytes=4 * 1024 * 1024),
    )(params, *pieces)


def solution(mesh):
    group = mesh.shape["data"]
    row_spec = P("stage", "data", None)
    full_spec = P("stage", None, None)

    def local_step(w_rows, mom_rows, grad_rows):
        params, mom_new, _, tail_r, tail_l = muon_step(group, mom_rows, grad_rows, w_rows)
        to_right = [(d, (d + 2) % group) for d in range(group)]
        to_left = [(d, (d - 2) % group) for d in range(group)]
        swap = [(d, d + 1 - 2 * (d % 2)) for d in range(group)]
        near = [lax.ppermute(tail_r, "data", to_right), lax.ppermute(tail_l, "data", to_left)]
        params = store_step(params)
        *near, params = lax.optimization_barrier((*near, params))
        far = [lax.ppermute(piece, "data", swap) for piece in near]
        mom_new = store_step(mom_new)
        *far, mom_new = lax.optimization_barrier((*far, mom_new))
        return tail_step(params, near + far), mom_new

    return jax.shard_map(
        local_step, mesh=mesh, in_specs=(row_spec, row_spec, row_spec), out_specs=(full_spec, row_spec), check_vma=False
    )
```

```python
import functools
import math

import jax
import jax.numpy as jnp
from jax import lax
from jax.experimental import pallas as pl
from jax.experimental.pallas import tpu as pltpu
from jax.sharding import PartitionSpec as P

NS_ITERS = 5
MOMENTUM = 0.95
LEARN_RATE = 0.02
WEIGHT_DECAY = 0.1
NORM_EPS = 1e-7
COEF_A = 3.4445
COEF_B = -4.7750
COEF_C = 2.0315

MESH = pl.DeviceIdType.MESH
TILE = 256
WIDE = 1024
SCALE_ROWS = 32
STEP_ROWS = 16
PREFETCH = 3


def ds(start, size):
    return pl.ds(pl.multiple_of(start, math.gcd(size, STEP_ROWS)), size)


def symmetric(dst, product, finish, dim):
    for j in range(0, dim, TILE):
        cols = slice(j, j + TILE)
        block = finish(product(slice(j, dim), cols), slice(j, dim), cols)
        dst[j:, cols] = block
        for i in range(j + TILE, dim, TILE):
            dst[cols, i : i + TILE] = block[i - j : i - j + TILE].T


def newton_schulz_poly(x, gram, poly):
    dim = gram.shape[0]

    def outer(rows, cols):
        return lax.dot_general(x[rows, :], x[cols, :], (((1,), (1,)), ((), ())), preferred_element_type=jnp.float32)

    def square(rows, cols):
        return jnp.dot(gram[rows, :], gram[:, cols], preferred_element_type=jnp.float32)

    symmetric(gram, outer, lambda prod, rows, cols: prod.astype(jnp.bfloat16), dim)
    symmetric(
        poly,
        square,
        lambda prod, rows, cols: (COEF_B * gram[rows, cols].astype(jnp.float32) + COEF_C * prod).astype(jnp.bfloat16),
        dim,
    )


def newton_schulz_step(x, poly, part):
    old = x[:, part]
    prod = jnp.dot(poly[...], old, preferred_element_type=jnp.float32)
    x[:, part] = (COEF_A * old.astype(jnp.float32) + prod).astype(jnp.bfloat16)


def muon_kernel(group, mom, grad, w, out, mom_new, w_sib, tail_r, tail_l, x, gram, poly, relay, w_buf, w_ahead, sq, send, recv, go, free):
    chips = group // 2
    mats, rows, cols = mom.shape
    pair = 2 * rows
    dim = pair * chips
    rms_scale = 0.2 * math.sqrt(max(dim, cols))
    me = lax.axis_index("data")
    c, k = lax.div(me, 2), lax.rem(me, 2)
    sib = 2 * c + 1 - k
    right, left, opp = (lax.rem(c + step, chips) for step in (1, chips - 1, 2))

    def peer_of(chip):
        return 2 * chip + k

    def own_rows(chip, half=None):
        if half is None:
            return ds(chip * pair, pair)
        return ds(chip * pair + half * rows, rows)

    ahead = rows // 2
    ahead_start, rest_start, rest = k * (pair - ahead), (1 - k) * ahead, pair - ahead

    def ahead_rows(chip):
        return ds(chip * pair + ahead_start, ahead)

    def rest_rows(chip):
        return ds(chip * pair + rest_start, rest)

    split = STEP_ROWS * (rest // STEP_ROWS // 2)
    sizes = ((rows, rows), (rest - split, split), (split, rest - split), (rows, rows))

    def block(chip, step):
        return rest_rows(chip) if step in (1, 2) else own_rows(chip)

    def block_part(chip, step, way):
        start = rest_start if step in (1, 2) else 0
        return ds(chip * pair + start + way * sizes[step][0], sizes[step][way])

    def mine(chip, half=None):
        return out.at[2 * chip + k, own_rows(c, half)]

    sent, slots = [], {}

    def slot(key):
        return slots.setdefault(key, len(slots))

    def remote(src, dst, peer, key):
        copy = pltpu.make_async_remote_copy(
            src_ref=src, dst_ref=dst, send_sem=send.at[len(sent)], recv_sem=recv.at[slot(key)],
            device_id={"data": peer}, device_id_type=MESH)
        sent.append(copy)
        return copy

    def push(src, dst, peer, key):
        copy = remote(src, dst, peer, key)
        copy.start()
        return copy

    def load(src, dst, key):
        pltpu.make_async_copy(src, dst, recv.at[slot(key)]).start()

    def arrived(dst, key):
        pltpu.make_async_copy(dst, dst, recv.at[slot(key)]).wait()

    steps = (opp, left, right, c)

    def prefetch(n):
        if n < mats:
            par, step = divmod(n, chips)
            chip = steps[step]
            load(mom.at[2 * chip + par], mom_new.at[2 * chip + par], ("mom", step, par))
            load(grad.at[2 * chip + par], out.at[2 * chip + k, own_rows(left, par)], ("grad", step, par))

    for n in range(PREFETCH):
        prefetch(n)

    barrier = pltpu.get_barrier_semaphore()
    for step in range(1, group):
        pl.semaphore_signal(barrier, inc=1, device_id={"data": lax.rem(me + step, group)}, device_id_type=MESH)
    pl.semaphore_wait(barrier, group - 1)

    def momentum(step, chip, par):
        mat = 2 * chip + par
        base = jnp.where(k == par, c * pair + k * rows, right * pair)
        arrived(mom_new.at[mat], ("mom", step, par))
        arrived(out.at[2 * chip + k, own_rows(left, par)], ("grad", step, par))
        prefetch(par * chips + step + PREFETCH)

        def body(r, total):
            part = ds(r * STEP_ROWS, STEP_ROWS)
            low = out[2 * chip + k, ds(left * pair + par * rows + r * STEP_ROWS, STEP_ROWS), :]
            new = MOMENTUM * mom_new[mat, part, :] + low.astype(jnp.float32)
            mom_new[mat, part, :] = new
            out[2 * chip + k, ds(base + r * STEP_ROWS, STEP_ROWS), :] = new.astype(jnp.bfloat16)
            square = new * new
            lanes = square[:, :128]
            for start in range(128, cols, 128):
                lanes = lanes + square[:, start : start + 128]
            for start in range(0, STEP_ROWS, 8):
                total = total + lanes[start : start + 8]
            return total

        sq[0, mat] = lax.fori_loop(0, rows // STEP_ROWS, body, jnp.zeros((8, 128), jnp.float32))

    swap = [
        remote(out.at[2 * chip + k, own_rows(right, 0)], out.at[2 * chip + 1 - k, own_rows(c, k)], sib, ("swap", step))
        for step, chip in enumerate(steps)
    ]
    exchange = [
        [
            remote(mine(opp, 0), relay.at[0], peer_of(right), "a_relay_l"),
            remote(mine(opp, 1), relay.at[1], peer_of(left), "a_relay_r"),
        ],
        [remote(mine(left, half), x.at[own_rows(c, half)], peer_of(left), ("a_right", half)) for half in range(2)],
        [remote(mine(right, half), x.at[own_rows(c, half)], peer_of(right), ("a_left", half)) for half in range(2)],
        [],
    ]

    def swapped(step):
        arrived(mine(steps[step], 1 - k), ("swap", step))

    for step, chip in enumerate(steps):
        momentum(step, chip, 0)

        @pl.when(k == 1)
        def _():
            swap[step].start()

        @pl.when(k == 0)
        def _():
            for copy in exchange[step][:1]:
                copy.start()
            if step > 0:
                swapped(step - 1)
                for copy in exchange[step - 1][1:]:
                    copy.start()

    for step, chip in enumerate(steps):
        momentum(step, chip, 1)

        @pl.when(k == 0)
        def _():
            swap[step].start()
            if step == 0:
                swapped(chips - 1)

    for step in range(1, group):
        dest = lax.rem(me + step, group)
        push(sq.at[0, dest], sq.at[1, step], dest, ("sq", step))
    for step, chip in enumerate((c, left, right, opp)):
        push(w.at[2 * chip + 1 - k], w_sib.at[chip], sib, ("w_swap", step))

    @pl.when(k == 1)
    def _():
        pl.semaphore_wait(go, 1)
        for step in range(chips):
            swapped(step)
            for copy in exchange[step]:
                copy.start()

    arrived(relay.at[0], "a_relay_l")
    pass_right = push(relay.at[0], x.at[own_rows(left, 0)], peer_of(right), "a_opp_l")
    arrived(relay.at[1], "a_relay_r")
    pass_left = push(relay.at[1], x.at[own_rows(right, 1)], peer_of(left), "a_opp_r")
    push(w.at[2 * right + k, ds(k * ahead, ahead)], w_ahead.at[0], peer_of(right), "w_ahead_l")
    push(w.at[2 * left + k, ds(k * ahead, ahead)], w_ahead.at[1], peer_of(left), "w_ahead_r")

    total = sq[0, me]
    for step in range(1, group):
        arrived(sq.at[1, step], ("sq", step))
        total = total + sq[1, step]
    norm = jnp.sqrt(jnp.sum(total, keepdims=True))
    inverse = 1.0 / (norm + NORM_EPS)

    def scale(get, base):
        @pl.loop(0, pair // SCALE_ROWS)
        def _(r):
            part = ds(base + r * SCALE_ROWS, SCALE_ROWS)
            x[part, :] = (get(part).astype(jnp.float32) * inverse).astype(jnp.bfloat16)

    scale(lambda part: out[2 * c + k, part, :], c * pair)
    for half in range(2):
        arrived(x.at[own_rows(left, half)], ("a_left", half))
    scale(lambda part: x[part, :], left * pair)
    for half in range(2):
        arrived(x.at[own_rows(right, half)], ("a_right", half))
    scale(lambda part: x[part, :], right * pair)
    arrived(x.at[own_rows(opp, 0)], "a_opp_l")
    arrived(x.at[own_rows(opp, 1)], "a_opp_r")

    @pl.when(k == 0)
    def _():
        pl.semaphore_signal(go, inc=1, device_id={"data": sib}, device_id_type=MESH)

    scale(lambda part: x[part, :], opp * pair)

    waited = swap + sum(exchange, []) + [pass_right, pass_left]
    for copy in waited:
        copy.wait_send()
    for chip in (right, left):
        pl.semaphore_signal(free, inc=1, device_id={"data": peer_of(chip)}, device_id_type=MESH)

    order = (c, left, right, opp)

    def load_w(step):
        load(w.at[2 * order[step] + k], w_buf.at[step % 2, ds(k * rows, rows)], ("w_own", step))
        arrived(w_sib.at[order[step]], ("w_swap", step))
        load(w_sib.at[order[step]], w_buf.at[step % 2, ds((1 - k) * rows, rows)], ("w_sib", step))

    load_w(0)
    load_w(1)

    @pl.loop(0, NS_ITERS - 1)
    def _(_):
        newton_schulz_poly(x, gram, poly)
        newton_schulz_step(x, poly, pl.ds(0, cols))

    newton_schulz_poly(x, gram, poly)
    pl.semaphore_wait(free, 2)

    chunks = [pl.ds(start, WIDE) for start in range(0, cols, WIDE)]
    for n, part in enumerate(chunks):
        newton_schulz_step(x, poly, part)
        push(x.at[own_rows(opp, 0), part], relay.at[0, :, part], peer_of(right), ("c_relay_l", n))
        push(x.at[own_rows(opp, 1), part], relay.at[1, :, part], peer_of(left), ("c_relay_r", n))
        push(x.at[rest_rows(right), part], out.at[2 * c + k, rest_rows(right), part], peer_of(right), ("c_left", n))
        push(x.at[rest_rows(left), part], out.at[2 * c + k, rest_rows(left), part], peer_of(left), ("c_right", n))

    def new_rows(mat, start, size, w_rows, get):
        @pl.loop(0, size // STEP_ROWS)
        def _(r):
            w_part = w_rows(r)
            part = ds(start + r * STEP_ROWS, STEP_ROWS)
            ortho = get(part).astype(jnp.float32) * rms_scale
            out[mat, part, :] = (w_part - LEARN_RATE * (ortho + WEIGHT_DECAY * w_part)).astype(jnp.bfloat16)

    last = chips - 1

    def update(step, get):
        chip = order[step]
        arrived(w_buf.at[step % 2, ds(k * rows, rows)], ("w_own", step))
        arrived(w_buf.at[step % 2, ds((1 - k) * rows, rows)], ("w_sib", step))
        start, size = (rest_start, rest) if step in (1, 2) else (0, pair)
        new_rows(
            2 * chip + k, c * pair + start, size, lambda r: w_buf[step % 2, ds(start + r * STEP_ROWS, STEP_ROWS), :],
            lambda part: get(chip, part))
        if step + 2 < chips:
            load_w(step + 2)
        place = out.at[2 * chip + k, block(c, step)]
        if step < last:
            push(place, place, peer_of(right), ("g_left", step))
            push(place, place, peer_of(left), ("g_right", step))
        else:
            parts = [out.at[2 * chip + k, block_part(c, step, way)] for way in range(2)]
            for way in range(2):
                push(parts[way], parts[way], peer_of(right), ("g_left", step, way))
                push(parts[1 - way], parts[1 - way], peer_of(left), ("g_right", step, 1 - way))
        push(place, place, sib, ("s_own", step))

    def update_ahead():
        for n, chip in enumerate((left, right)):
            arrived(w_ahead.at[n], ("w_ahead_l", "w_ahead_r")[n])
            new_rows(
                2 * c + k, chip * pair + ahead_start, ahead, lambda r: w_ahead[n, ds(r * STEP_ROWS, STEP_ROWS), :],
                lambda part: x[part, :])
            place = out.at[2 * c + k, ahead_rows(chip)]
            push(place, place, peer_of(right), ("e_left", n))
            push(place, place, peer_of(left), ("e_right", n))
            push(place, place, sib, ("s_ahead", n))

    update(0, lambda chip, part: x[part, :])
    update_ahead()
    for n, part in enumerate(chunks):
        arrived(relay.at[0, :, part], ("c_relay_l", n))
        push(relay.at[0, :, part], out.at[2 * left + k, own_rows(right, 0), part], peer_of(right), ("c_opp_l", n))
        arrived(relay.at[1, :, part], ("c_relay_r", n))
        push(relay.at[1, :, part], out.at[2 * right + k, own_rows(left, 1), part], peer_of(left), ("c_opp_r", n))

    def returned(chip, part):
        return out[2 * chip + k, part, :]

    for n, part in enumerate(chunks):
        arrived(out.at[2 * left + k, rest_rows(c), part], ("c_left", n))
    update(1, returned)
    for n, part in enumerate(chunks):
        arrived(out.at[2 * right + k, rest_rows(c), part], ("c_right", n))
    update(2, returned)
    for n, part in enumerate(chunks):
        arrived(out.at[2 * opp + k, own_rows(c, 0), part], ("c_opp_l", n))
        arrived(out.at[2 * opp + k, own_rows(c, 1), part], ("c_opp_r", n))
    update(3, returned)

    def near(chip, step):
        return lax.rem(chip + (0, chips - 1, 1, 2)[step], chips)

    def pass_on(mat, part, peer, key):
        push(out.at[mat, part], out.at[mat, part], peer, key)

    for step in range(last):
        mat_l, mat_r = 2 * near(left, step) + k, 2 * near(right, step) + k
        arrived(out.at[mat_l, block(left, step)], ("g_left", step))
        pass_on(mat_l, block_part(left, step, 0), peer_of(right), ("f_left", step))
        pass_on(mat_l, block(left, step), sib, ("s_left", step))
        arrived(out.at[mat_r, block(right, step)], ("g_right", step))
        pass_on(mat_r, block_part(right, step, 1), peer_of(left), ("f_right", step))
        pass_on(mat_r, block(right, step), sib, ("s_right", step))
        if step == 0:
            arrived(out.at[mat_l, ahead_rows(opp)], ("e_left", 0))
            pass_on(mat_l, ahead_rows(opp), peer_of(right), "fe_left")
            pass_on(mat_l, ahead_rows(opp), sib, ("s_ahead_l", 0))
            arrived(out.at[mat_l, ahead_rows(c)], ("e_left", 1))
            pass_on(mat_l, ahead_rows(c), sib, ("s_ahead_l", 1))
            arrived(out.at[mat_r, ahead_rows(c)], ("e_right", 0))
            pass_on(mat_r, ahead_rows(c), sib, ("s_ahead_r", 0))
            arrived(out.at[mat_r, ahead_rows(opp)], ("e_right", 1))
            pass_on(mat_r, ahead_rows(opp), peer_of(left), "fe_right")
            pass_on(mat_r, ahead_rows(opp), sib, ("s_ahead_r", 1))
    mat_l, mat_r = 2 * near(left, last) + k, 2 * near(right, last) + k
    for way in range(2):
        arrived(out.at[mat_l, block_part(left, last, way)], ("g_left", last, way))
        pass_on(mat_l, block_part(left, last, way), sib, ("s_left", last, way))
        arrived(out.at[mat_r, block_part(right, last, 1 - way)], ("g_right", last, 1 - way))
        pass_on(mat_r, block_part(right, last, 1 - way), sib, ("s_right", last, 1 - way))
        if way == 0:
            load(out.at[mat_l, block_part(left, last, 0)], tail_r, "tail_r")
            load(out.at[mat_r, block_part(right, last, 1)], tail_l, "tail_l")

    for step in range(last):
        mat = 2 * near(opp, step) + k
        arrived(out.at[mat, block_part(opp, step, 0)], ("f_left", step))
        pass_on(mat, block_part(opp, step, 0), sib, ("s_far_l", step))
        arrived(out.at[mat, block_part(opp, step, 1)], ("f_right", step))
        pass_on(mat, block_part(opp, step, 1), sib, ("s_far_r", step))
        if step == 0:
            arrived(out.at[mat, ahead_rows(right)], "fe_left")
            pass_on(mat, ahead_rows(right), sib, "s_far_ahead_l")
            arrived(out.at[mat, ahead_rows(left)], "fe_right")
            pass_on(mat, ahead_rows(left), sib, "s_far_ahead_r")

    def sib_ahead(chip):
        return ds(chip * pair + (1 - k) * (pair - ahead), ahead)

    def sib_start(chip, step):
        return chip * pair + (k * ahead if step in (1, 2) else 0)

    for step in range(chips):
        size = sum(sizes[step])
        arrived(out.at[2 * near(c, step) + 1 - k, ds(sib_start(c, step), size)], ("s_own", step))
        if step == last:
            for way in range(2):
                arrived(out.at[2 * near(left, step) + 1 - k, own_rows(left, way)], ("s_left", step, way))
                arrived(out.at[2 * near(right, step) + 1 - k, own_rows(right, way)], ("s_right", step, way))
        else:
            arrived(out.at[2 * near(left, step) + 1 - k, ds(sib_start(left, step), size)], ("s_left", step))
            arrived(out.at[2 * near(right, step) + 1 - k, ds(sib_start(right, step), size)], ("s_right", step))
            mat, start = 2 * near(opp, step) + 1 - k, sib_start(opp, step)
            arrived(out.at[mat, ds(start, sizes[step][0])], ("s_far_l", step))
            arrived(out.at[mat, ds(start + sizes[step][0], sizes[step][1])], ("s_far_r", step))
        if step == 0:
            for n, chip in enumerate((left, right)):
                arrived(out.at[2 * c + 1 - k, sib_ahead(chip)], ("s_ahead", n))
            for n, chip in enumerate((opp, c)):
                arrived(out.at[2 * left + 1 - k, sib_ahead(chip)], ("s_ahead_l", n))
            for n, chip in enumerate((c, opp)):
                arrived(out.at[2 * right + 1 - k, sib_ahead(chip)], ("s_ahead_r", n))
            arrived(out.at[2 * opp + 1 - k, sib_ahead(right)], "s_far_ahead_l")
            arrived(out.at[2 * opp + 1 - k, sib_ahead(left)], "s_far_ahead_r")
    arrived(tail_r, "tail_r")
    arrived(tail_l, "tail_l")
    for copy in sent:
        if not any(copy is done for done in waited):
            copy.wait_send()


def muon_step(group, mom, grad, w):
    mats, rows, cols = mom.shape
    chips, pair = group // 2, 2 * rows
    dim = pair * chips
    hbm = pl.BlockSpec(memory_space=pl.ANY)
    vmem = pl.BlockSpec(memory_space=pltpu.VMEM)
    return pl.pallas_call(
        functools.partial(muon_kernel, group),
        in_specs=[hbm, hbm, hbm],
        out_specs=[vmem, vmem, hbm, hbm, hbm],
        out_shape=[
            pltpu.VMEM((mats, dim, cols), jnp.bfloat16),
            pltpu.VMEM((mats, rows, cols), jnp.float32),
            pltpu.HBM((chips, rows, cols), jnp.float32),
            pltpu.HBM((rows, cols), jnp.bfloat16),
            pltpu.HBM((rows, cols), jnp.bfloat16),
        ],
        scratch_shapes=[
            pltpu.VMEM((dim, cols), jnp.bfloat16),
            pltpu.VMEM((dim, dim), jnp.bfloat16),
            pltpu.VMEM((dim, dim), jnp.bfloat16),
            pltpu.VMEM((2, rows, cols), jnp.bfloat16),
            pltpu.VMEM((2, pair, cols), jnp.float32),
            pltpu.VMEM((2, rows // 2, cols), jnp.float32),
            pltpu.VMEM((2, group, 8, 128), jnp.float32),
            pltpu.SemaphoreType.DMA((128,)),
            pltpu.SemaphoreType.DMA((128,)),
            pltpu.SemaphoreType.REGULAR,
            pltpu.SemaphoreType.REGULAR,
        ],
        compiler_params=pltpu.CompilerParams(
            collective_id=0, has_side_effects=True, vmem_limit_bytes=16 * 1024 * 1024
        ),
    )(mom, grad, w)


def run_copies(pairs, sem):
    copies = [pltpu.make_async_copy(src, dst, sem.at[n]) for n, (src, dst) in enumerate(pairs)]
    for copy in copies:
        copy.start()
    for copy in copies:
        copy.wait()


def place_of(params, group):
    me = lax.axis_index("data")
    rows = params.shape[1] // group
    chips = group // 2

    def part(chip, half=None):
        start = 2 * lax.rem(chip, chips) + (0 if half is None else half)
        return ds(start * rows, 2 * rows if half is None else rows)

    return lax.div(me, 2), lax.rem(me, 2), chips, part


def store_params_kernel(group, src, dst, sem):
    c, _, chips, part = place_of(src, group)
    pairs = []
    for par in range(2):
        for step in range(1, chips):
            mat = 2 * lax.rem(c + step, chips) + par
            pairs.append((src.at[mat], dst.at[mat]))
        for step in (0, 1, chips - 1):
            where = (2 * c + par, part(c + step))
            pairs.append((src.at[where], dst.at[where]))
    run_copies(pairs, sem)


def store_kernel(src, dst, sem):
    run_copies([(src.at[i], dst.at[i]) for i in range(src.shape[0])], sem)


def store_late_kernel(group, params, near_l, near_r, far_l, far_r, out, sem):
    c, k, _, part = place_of(out, group)
    pieces = ((near_l, k, 0), (near_r, k, 1), (far_l, 1 - k, 0), (far_r, 1 - k, 1))
    run_copies([(src, out.at[2 * c + par, part(c + 2, half)]) for src, par, half in pieces], sem)


def store_step(kernel, full, copies):
    return pl.pallas_call(
        kernel,
        in_specs=[pl.BlockSpec(memory_space=pltpu.VMEM)],
        out_specs=pl.BlockSpec(memory_space=pl.ANY),
        out_shape=jax.ShapeDtypeStruct(full.shape, full.dtype),
        scratch_shapes=[pltpu.SemaphoreType.DMA((copies,))],
        compiler_params=pltpu.CompilerParams(vmem_limit_bytes=1024 * 1024),
        cost_estimate=pl.CostEstimate(flops=1000 * full.size, bytes_accessed=2 * full.size, transcendentals=0),
    )(full)


def store_late(group, params, pieces):
    hbm = pl.BlockSpec(memory_space=pl.ANY)
    return pl.pallas_call(
        functools.partial(store_late_kernel, group),
        in_specs=[hbm] + [pl.BlockSpec(memory_space=pltpu.VMEM)] * 4,
        out_specs=hbm,
        out_shape=jax.ShapeDtypeStruct(params.shape, params.dtype),
        input_output_aliases={0: 0},
        scratch_shapes=[pltpu.SemaphoreType.DMA((4,))],
        compiler_params=pltpu.CompilerParams(vmem_limit_bytes=4 * 1024 * 1024),
    )(params, *pieces)


def solution(mesh):
    group = mesh.shape["data"]
    row_spec = P("stage", "data", None)
    full_spec = P("stage", None, None)

    def local_step(w_rows, mom_rows, grad_rows):
        params, mom_new, _, tail_r, tail_l = muon_step(group, mom_rows, grad_rows, w_rows)
        to_right = [(d, (d + 2) % group) for d in range(group)]
        to_left = [(d, (d - 2) % group) for d in range(group)]
        swap = [(d, d + 1 - 2 * (d % 2)) for d in range(group)]
        near = [lax.ppermute(tail_r, "data", to_right), lax.ppermute(tail_l, "data", to_left)]
        params = store_step(functools.partial(store_params_kernel, group), params, 2 * (group // 2 + 2))
        *near, params = lax.optimization_barrier((*near, params))
        far = [lax.ppermute(piece, "data", swap) for piece in near]
        mom_new = store_step(store_kernel, mom_new, mom_new.shape[0])
        *far, mom_new = lax.optimization_barrier((*far, mom_new))
        return store_late(group, params, near + far), mom_new

    return jax.shard_map(
        local_step, mesh=mesh, in_specs=(row_spec, row_spec, row_spec), out_specs=(full_spec, row_spec), check_vma=False
    )
```

```python
import functools
import math

import jax
import jax.numpy as jnp
from jax import lax
from jax.experimental import pallas as pl
from jax.experimental.pallas import tpu as pltpu
from jax.sharding import PartitionSpec as P

NS_ITERS = 5
MOMENTUM = 0.95
LEARN_RATE = 0.02
WEIGHT_DECAY = 0.1
NORM_EPS = 1e-7
COEF_A = 3.4445
COEF_B = -4.7750
COEF_C = 2.0315

MESH = pl.DeviceIdType.MESH
TILE = 256
WIDE = 512
SCALE_ROWS = 32
STEP_ROWS = 16
PREFETCH = 3


def ds(start, size):
    return pl.ds(pl.multiple_of(start, math.gcd(size, STEP_ROWS)), size)


def symmetric(dst, product, finish, dim):
    for j in range(0, dim, TILE):
        cols = slice(j, j + TILE)
        block = finish(product(slice(j, dim), cols), slice(j, dim), cols)
        dst[j:, cols] = block
        for i in range(j + TILE, dim, TILE):
            dst[cols, i : i + TILE] = block[i - j : i - j + TILE].T


def newton_schulz_poly(x, gram, poly):
    dim = gram.shape[0]

    def outer(rows, cols):
        return lax.dot_general(x[rows, :], x[cols, :], (((1,), (1,)), ((), ())), preferred_element_type=jnp.float32)

    def square(rows, cols):
        return jnp.dot(gram[rows, :], gram[:, cols], preferred_element_type=jnp.float32)

    symmetric(gram, outer, lambda prod, rows, cols: prod.astype(jnp.bfloat16), dim)
    symmetric(
        poly,
        square,
        lambda prod, rows, cols: (COEF_B * gram[rows, cols].astype(jnp.float32) + COEF_C * prod).astype(jnp.bfloat16),
        dim,
    )


def newton_schulz_step(x, poly, part):
    old = x[:, part]
    prod = jnp.dot(poly[...], old, preferred_element_type=jnp.float32)
    x[:, part] = (COEF_A * old.astype(jnp.float32) + prod).astype(jnp.bfloat16)


def muon_kernel(group, mom, grad, w, out, mom_new, w_sib, tail_r, tail_l, x, gram, poly, relay, w_buf, w_ahead, sq, send, recv, go, free):
    chips = group // 2
    mats, rows, cols = mom.shape
    pair = 2 * rows
    dim = pair * chips
    rms_scale = 0.2 * math.sqrt(max(dim, cols))
    me = lax.axis_index("data")
    c, k = lax.div(me, 2), lax.rem(me, 2)
    sib = 2 * c + 1 - k
    right, left, opp = (lax.rem(c + step, chips) for step in (1, chips - 1, 2))

    def peer_of(chip):
        return 2 * chip + k

    def own_rows(chip, half=None):
        if half is None:
            return ds(chip * pair, pair)
        return ds(chip * pair + half * rows, rows)

    ahead = rows // 2
    ahead_start, rest_start, rest = k * (pair - ahead), (1 - k) * ahead, pair - ahead

    def ahead_rows(chip):
        return ds(chip * pair + ahead_start, ahead)

    def rest_rows(chip):
        return ds(chip * pair + rest_start, rest)

    split = STEP_ROWS * (rest // STEP_ROWS // 2)
    sizes = ((rows, rows), (rest - split, split), (split, rest - split), (rows, rows))

    def block(chip, step):
        return rest_rows(chip) if step in (1, 2) else own_rows(chip)

    def block_part(chip, step, way):
        start = rest_start if step in (1, 2) else 0
        return ds(chip * pair + start + way * sizes[step][0], sizes[step][way])

    def mine(chip, half=None):
        return out.at[2 * chip + k, own_rows(c, half)]

    sent, slots = [], {}

    def slot(key):
        return slots.setdefault(key, len(slots))

    def remote(src, dst, peer, key):
        copy = pltpu.make_async_remote_copy(
            src_ref=src, dst_ref=dst, send_sem=send.at[len(sent)], recv_sem=recv.at[slot(key)],
            device_id={"data": peer}, device_id_type=MESH)
        sent.append(copy)
        return copy

    def push(src, dst, peer, key):
        copy = remote(src, dst, peer, key)
        copy.start()
        return copy

    def load(src, dst, key):
        pltpu.make_async_copy(src, dst, recv.at[slot(key)]).start()

    def arrived(dst, key):
        pltpu.make_async_copy(dst, dst, recv.at[slot(key)]).wait()

    steps = (opp, left, right, c)

    def prefetch(n):
        if n < mats:
            par, step = divmod(n, chips)
            chip = steps[step]
            load(mom.at[2 * chip + par], mom_new.at[2 * chip + par], ("mom", step, par))
            load(grad.at[2 * chip + par], out.at[2 * chip + k, own_rows(left, par)], ("grad", step, par))

    for n in range(PREFETCH):
        prefetch(n)

    barrier = pltpu.get_barrier_semaphore()
    for step in range(1, group):
        pl.semaphore_signal(barrier, inc=1, device_id={"data": lax.rem(me + step, group)}, device_id_type=MESH)

    def momentum(step, chip, par):
        mat = 2 * chip + par
        base = jnp.where(k == par, c * pair + k * rows, right * pair)
        arrived(mom_new.at[mat], ("mom", step, par))
        arrived(out.at[2 * chip + k, own_rows(left, par)], ("grad", step, par))
        prefetch(par * chips + step + PREFETCH)

        def body(r, total):
            part = ds(r * STEP_ROWS, STEP_ROWS)
            low = out[2 * chip + k, ds(left * pair + par * rows + r * STEP_ROWS, STEP_ROWS), :]
            new = MOMENTUM * mom_new[mat, part, :] + low.astype(jnp.float32)
            mom_new[mat, part, :] = new
            out[2 * chip + k, ds(base + r * STEP_ROWS, STEP_ROWS), :] = new.astype(jnp.bfloat16)
            square = new * new
            lanes = square[:, :128]
            for start in range(128, cols, 128):
                lanes = lanes + square[:, start : start + 128]
            for start in range(0, STEP_ROWS, 8):
                total = total + lanes[start : start + 8]
            return total

        sq[0, mat] = lax.fori_loop(0, rows // STEP_ROWS, body, jnp.zeros((8, 128), jnp.float32))

    swap = [
        remote(out.at[2 * chip + k, own_rows(right, 0)], out.at[2 * chip + 1 - k, own_rows(c, k)], sib, ("swap", step))
        for step, chip in enumerate(steps)
    ]
    exchange = [
        [
            remote(mine(opp, 0), relay.at[0], peer_of(right), "a_relay_l"),
            remote(mine(opp, 1), relay.at[1], peer_of(left), "a_relay_r"),
        ],
        [remote(mine(left, half), x.at[own_rows(c, half)], peer_of(left), ("a_right", half)) for half in range(2)],
        [remote(mine(right, half), x.at[own_rows(c, half)], peer_of(right), ("a_left", half)) for half in range(2)],
        [],
    ]

    def swapped(step):
        arrived(mine(steps[step], 1 - k), ("swap", step))

    for step, chip in enumerate(steps):
        momentum(step, chip, 0)
        if step == 0:
            pl.semaphore_wait(barrier, group - 1)

        @pl.when(k == 1)
        def _():
            swap[step].start()

        @pl.when(k == 0)
        def _():
            for copy in exchange[step][:1]:
                copy.start()
            if step > 0:
                swapped(step - 1)
                for copy in exchange[step - 1][1:]:
                    copy.start()

    for step, chip in enumerate(steps):
        momentum(step, chip, 1)

        @pl.when(k == 0)
        def _():
            swap[step].start()
            if step == 0:
                swapped(chips - 1)

    for step in range(1, group):
        dest = lax.rem(me + step, group)
        push(sq.at[0, dest], sq.at[1, step], dest, ("sq", step))
    for step, chip in enumerate((c, left, right, opp)):
        push(w.at[2 * chip + 1 - k], w_sib.at[chip], sib, ("w_swap", step))

    @pl.when(k == 1)
    def _():
        pl.semaphore_wait(go, 1)
        for step in range(chips):
            swapped(step)
            for copy in exchange[step]:
                copy.start()

    arrived(relay.at[0], "a_relay_l")
    pass_right = push(relay.at[0], x.at[own_rows(left, 0)], peer_of(right), "a_opp_l")
    arrived(relay.at[1], "a_relay_r")
    pass_left = push(relay.at[1], x.at[own_rows(right, 1)], peer_of(left), "a_opp_r")
    push(w.at[2 * right + k, ds(k * ahead, ahead)], w_ahead.at[0], peer_of(right), "w_ahead_l")
    push(w.at[2 * left + k, ds(k * ahead, ahead)], w_ahead.at[1], peer_of(left), "w_ahead_r")

    total = sq[0, me]
    for step in range(1, group):
        arrived(sq.at[1, step], ("sq", step))
        total = total + sq[1, step]
    norm = jnp.sqrt(jnp.sum(total, keepdims=True))
    inverse = 1.0 / (norm + NORM_EPS)

    def scale(get, base):
        @pl.loop(0, pair // SCALE_ROWS)
        def _(r):
            part = ds(base + r * SCALE_ROWS, SCALE_ROWS)
            x[part, :] = (get(part).astype(jnp.float32) * inverse).astype(jnp.bfloat16)

    scale(lambda part: out[2 * c + k, part, :], c * pair)
    for half in range(2):
        arrived(x.at[own_rows(left, half)], ("a_left", half))
    scale(lambda part: x[part, :], left * pair)
    for half in range(2):
        arrived(x.at[own_rows(right, half)], ("a_right", half))
    scale(lambda part: x[part, :], right * pair)
    arrived(x.at[own_rows(opp, 0)], "a_opp_l")
    arrived(x.at[own_rows(opp, 1)], "a_opp_r")

    @pl.when(k == 0)
    def _():
        pl.semaphore_signal(go, inc=1, device_id={"data": sib}, device_id_type=MESH)

    scale(lambda part: x[part, :], opp * pair)

    waited = swap + sum(exchange, []) + [pass_right, pass_left]
    for copy in waited:
        copy.wait_send()
    for chip in (right, left):
        pl.semaphore_signal(free, inc=1, device_id={"data": peer_of(chip)}, device_id_type=MESH)

    order = (c, left, right, opp)

    def load_w(step):
        load(w.at[2 * order[step] + k], w_buf.at[step % 2, ds(k * rows, rows)], ("w_own", step))
        arrived(w_sib.at[order[step]], ("w_swap", step))
        load(w_sib.at[order[step]], w_buf.at[step % 2, ds((1 - k) * rows, rows)], ("w_sib", step))

    load_w(0)
    load_w(1)

    @pl.loop(0, NS_ITERS - 1)
    def _(_):
        newton_schulz_poly(x, gram, poly)
        newton_schulz_step(x, poly, pl.ds(0, cols))

    newton_schulz_poly(x, gram, poly)
    pl.semaphore_wait(free, 2)

    chunks = [pl.ds(start, WIDE) for start in range(0, cols, WIDE)]
    for n, part in enumerate(chunks):
        newton_schulz_step(x, poly, part)
        push(x.at[own_rows(opp, 0), part], relay.at[0, :, part], peer_of(right), ("c_relay_l", n))
        push(x.at[own_rows(opp, 1), part], relay.at[1, :, part], peer_of(left), ("c_relay_r", n))
        push(x.at[rest_rows(right), part], out.at[2 * c + k, rest_rows(right), part], peer_of(right), ("c_left", n))
        push(x.at[rest_rows(left), part], out.at[2 * c + k, rest_rows(left), part], peer_of(left), ("c_right", n))

    def new_rows(mat, start, size, w_rows, get):
        @pl.loop(0, size // STEP_ROWS)
        def _(r):
            w_part = w_rows(r)
            part = ds(start + r * STEP_ROWS, STEP_ROWS)
            ortho = get(part).astype(jnp.float32) * rms_scale
            out[mat, part, :] = (w_part - LEARN_RATE * (ortho + WEIGHT_DECAY * w_part)).astype(jnp.bfloat16)

    last = chips - 1

    def update(step, get):
        chip = order[step]
        arrived(w_buf.at[step % 2, ds(k * rows, rows)], ("w_own", step))
        arrived(w_buf.at[step % 2, ds((1 - k) * rows, rows)], ("w_sib", step))
        start, size = (rest_start, rest) if step in (1, 2) else (0, pair)
        new_rows(
            2 * chip + k, c * pair + start, size, lambda r: w_buf[step % 2, ds(start + r * STEP_ROWS, STEP_ROWS), :],
            lambda part: get(chip, part))
        if step + 2 < chips:
            load_w(step + 2)
        place = out.at[2 * chip + k, block(c, step)]
        if step < last:
            push(place, place, peer_of(right), ("g_left", step))
            push(place, place, peer_of(left), ("g_right", step))
        else:
            parts = [out.at[2 * chip + k, block_part(c, step, way)] for way in range(2)]
            for way in range(2):
                push(parts[way], parts[way], peer_of(right), ("g_left", step, way))
                push(parts[1 - way], parts[1 - way], peer_of(left), ("g_right", step, 1 - way))
        push(place, place, sib, ("s_own", step))

    def update_ahead():
        for n, chip in enumerate((left, right)):
            arrived(w_ahead.at[n], ("w_ahead_l", "w_ahead_r")[n])
            new_rows(
                2 * c + k, chip * pair + ahead_start, ahead, lambda r: w_ahead[n, ds(r * STEP_ROWS, STEP_ROWS), :],
                lambda part: x[part, :])
            place = out.at[2 * c + k, ahead_rows(chip)]
            push(place, place, peer_of(right), ("e_left", n))
            push(place, place, peer_of(left), ("e_right", n))
            push(place, place, sib, ("s_ahead", n))

    update(0, lambda chip, part: x[part, :])
    update_ahead()
    for n, part in enumerate(chunks):
        arrived(relay.at[0, :, part], ("c_relay_l", n))
        push(relay.at[0, :, part], out.at[2 * left + k, own_rows(right, 0), part], peer_of(right), ("c_opp_l", n))
        arrived(relay.at[1, :, part], ("c_relay_r", n))
        push(relay.at[1, :, part], out.at[2 * right + k, own_rows(left, 1), part], peer_of(left), ("c_opp_r", n))

    def returned(chip, part):
        return out[2 * chip + k, part, :]

    for n, part in enumerate(chunks):
        arrived(out.at[2 * left + k, rest_rows(c), part], ("c_left", n))
    update(1, returned)
    for n, part in enumerate(chunks):
        arrived(out.at[2 * right + k, rest_rows(c), part], ("c_right", n))
    update(2, returned)
    for n, part in enumerate(chunks):
        arrived(out.at[2 * opp + k, own_rows(c, 0), part], ("c_opp_l", n))
        arrived(out.at[2 * opp + k, own_rows(c, 1), part], ("c_opp_r", n))
    update(3, returned)

    def near(chip, step):
        return lax.rem(chip + (0, chips - 1, 1, 2)[step], chips)

    def pass_on(mat, part, peer, key):
        push(out.at[mat, part], out.at[mat, part], peer, key)

    for step in range(last):
        mat_l, mat_r = 2 * near(left, step) + k, 2 * near(right, step) + k
        arrived(out.at[mat_l, block(left, step)], ("g_left", step))
        pass_on(mat_l, block_part(left, step, 0), peer_of(right), ("f_left", step))
        pass_on(mat_l, block(left, step), sib, ("s_left", step))
        arrived(out.at[mat_r, block(right, step)], ("g_right", step))
        pass_on(mat_r, block_part(right, step, 1), peer_of(left), ("f_right", step))
        pass_on(mat_r, block(right, step), sib, ("s_right", step))
        if step == 0:
            arrived(out.at[mat_l, ahead_rows(opp)], ("e_left", 0))
            pass_on(mat_l, ahead_rows(opp), peer_of(right), "fe_left")
            pass_on(mat_l, ahead_rows(opp), sib, ("s_ahead_l", 0))
            arrived(out.at[mat_l, ahead_rows(c)], ("e_left", 1))
            pass_on(mat_l, ahead_rows(c), sib, ("s_ahead_l", 1))
            arrived(out.at[mat_r, ahead_rows(c)], ("e_right", 0))
            pass_on(mat_r, ahead_rows(c), sib, ("s_ahead_r", 0))
            arrived(out.at[mat_r, ahead_rows(opp)], ("e_right", 1))
            pass_on(mat_r, ahead_rows(opp), peer_of(left), "fe_right")
            pass_on(mat_r, ahead_rows(opp), sib, ("s_ahead_r", 1))
    mat_l, mat_r = 2 * near(left, last) + k, 2 * near(right, last) + k
    for way in range(2):
        arrived(out.at[mat_l, block_part(left, last, way)], ("g_left", last, way))
        pass_on(mat_l, block_part(left, last, way), sib, ("s_left", last, way))
        arrived(out.at[mat_r, block_part(right, last, 1 - way)], ("g_right", last, 1 - way))
        pass_on(mat_r, block_part(right, last, 1 - way), sib, ("s_right", last, 1 - way))
        if way == 0:
            load(out.at[mat_l, block_part(left, last, 0)], tail_r, "tail_r")
            load(out.at[mat_r, block_part(right, last, 1)], tail_l, "tail_l")

    for step in range(last):
        mat = 2 * near(opp, step) + k
        arrived(out.at[mat, block_part(opp, step, 0)], ("f_left", step))
        pass_on(mat, block_part(opp, step, 0), sib, ("s_far_l", step))
        arrived(out.at[mat, block_part(opp, step, 1)], ("f_right", step))
        pass_on(mat, block_part(opp, step, 1), sib, ("s_far_r", step))
        if step == 0:
            arrived(out.at[mat, ahead_rows(right)], "fe_left")
            pass_on(mat, ahead_rows(right), sib, "s_far_ahead_l")
            arrived(out.at[mat, ahead_rows(left)], "fe_right")
            pass_on(mat, ahead_rows(left), sib, "s_far_ahead_r")

    def sib_ahead(chip):
        return ds(chip * pair + (1 - k) * (pair - ahead), ahead)

    def sib_start(chip, step):
        return chip * pair + (k * ahead if step in (1, 2) else 0)

    for step in range(chips):
        size = sum(sizes[step])
        arrived(out.at[2 * near(c, step) + 1 - k, ds(sib_start(c, step), size)], ("s_own", step))
        if step == last:
            for way in range(2):
                arrived(out.at[2 * near(left, step) + 1 - k, own_rows(left, way)], ("s_left", step, way))
                arrived(out.at[2 * near(right, step) + 1 - k, own_rows(right, way)], ("s_right", step, way))
        else:
            arrived(out.at[2 * near(left, step) + 1 - k, ds(sib_start(left, step), size)], ("s_left", step))
            arrived(out.at[2 * near(right, step) + 1 - k, ds(sib_start(right, step), size)], ("s_right", step))
            mat, start = 2 * near(opp, step) + 1 - k, sib_start(opp, step)
            arrived(out.at[mat, ds(start, sizes[step][0])], ("s_far_l", step))
            arrived(out.at[mat, ds(start + sizes[step][0], sizes[step][1])], ("s_far_r", step))
        if step == 0:
            for n, chip in enumerate((left, right)):
                arrived(out.at[2 * c + 1 - k, sib_ahead(chip)], ("s_ahead", n))
            for n, chip in enumerate((opp, c)):
                arrived(out.at[2 * left + 1 - k, sib_ahead(chip)], ("s_ahead_l", n))
            for n, chip in enumerate((c, opp)):
                arrived(out.at[2 * right + 1 - k, sib_ahead(chip)], ("s_ahead_r", n))
            arrived(out.at[2 * opp + 1 - k, sib_ahead(right)], "s_far_ahead_l")
            arrived(out.at[2 * opp + 1 - k, sib_ahead(left)], "s_far_ahead_r")
    arrived(tail_r, "tail_r")
    arrived(tail_l, "tail_l")
    for copy in sent:
        if not any(copy is done for done in waited):
            copy.wait_send()


def muon_step(group, mom, grad, w):
    mats, rows, cols = mom.shape
    chips, pair = group // 2, 2 * rows
    dim = pair * chips
    hbm = pl.BlockSpec(memory_space=pl.ANY)
    vmem = pl.BlockSpec(memory_space=pltpu.VMEM)
    return pl.pallas_call(
        functools.partial(muon_kernel, group),
        in_specs=[hbm, hbm, hbm],
        out_specs=[vmem, vmem, hbm, hbm, hbm],
        out_shape=[
            pltpu.VMEM((mats, dim, cols), jnp.bfloat16),
            pltpu.VMEM((mats, rows, cols), jnp.float32),
            pltpu.HBM((chips, rows, cols), jnp.float32),
            pltpu.HBM((rows, cols), jnp.bfloat16),
            pltpu.HBM((rows, cols), jnp.bfloat16),
        ],
        scratch_shapes=[
            pltpu.VMEM((dim, cols), jnp.bfloat16),
            pltpu.VMEM((dim, dim), jnp.bfloat16),
            pltpu.VMEM((dim, dim), jnp.bfloat16),
            pltpu.VMEM((2, rows, cols), jnp.bfloat16),
            pltpu.VMEM((2, pair, cols), jnp.float32),
            pltpu.VMEM((2, rows // 2, cols), jnp.float32),
            pltpu.VMEM((2, group, 8, 128), jnp.float32),
            pltpu.SemaphoreType.DMA((160,)),
            pltpu.SemaphoreType.DMA((160,)),
            pltpu.SemaphoreType.REGULAR,
            pltpu.SemaphoreType.REGULAR,
        ],
        compiler_params=pltpu.CompilerParams(
            collective_id=0, has_side_effects=True, vmem_limit_bytes=16 * 1024 * 1024
        ),
    )(mom, grad, w)


def run_copies(pairs, sem):
    copies = [pltpu.make_async_copy(src, dst, sem.at[n]) for n, (src, dst) in enumerate(pairs)]
    for copy in copies:
        copy.start()
    for copy in copies:
        copy.wait()


def place_of(params, group):
    me = lax.axis_index("data")
    rows = params.shape[1] // group
    chips = group // 2

    def part(chip, half=None):
        start = 2 * lax.rem(chip, chips) + (0 if half is None else half)
        return ds(start * rows, 2 * rows if half is None else rows)

    return lax.div(me, 2), lax.rem(me, 2), chips, part


def store_params_kernel(group, src, dst, sem):
    c, _, chips, part = place_of(src, group)
    pairs = []
    for par in range(2):
        for step in range(1, chips):
            mat = 2 * lax.rem(c + step, chips) + par
            pairs.append((src.at[mat], dst.at[mat]))
        for step in (0, 1, chips - 1):
            where = (2 * c + par, part(c + step))
            pairs.append((src.at[where], dst.at[where]))
    run_copies(pairs, sem)


def store_kernel(src, dst, sem):
    run_copies([(src.at[i], dst.at[i]) for i in range(src.shape[0])], sem)


def store_late_kernel(group, params, near_l, near_r, far_l, far_r, out, sem):
    c, k, _, part = place_of(out, group)
    pieces = ((near_l, k, 0), (near_r, k, 1), (far_l, 1 - k, 0), (far_r, 1 - k, 1))
    run_copies([(src, out.at[2 * c + par, part(c + 2, half)]) for src, par, half in pieces], sem)


def store_step(kernel, full, copies):
    return pl.pallas_call(
        kernel,
        in_specs=[pl.BlockSpec(memory_space=pltpu.VMEM)],
        out_specs=pl.BlockSpec(memory_space=pl.ANY),
        out_shape=jax.ShapeDtypeStruct(full.shape, full.dtype),
        scratch_shapes=[pltpu.SemaphoreType.DMA((copies,))],
        compiler_params=pltpu.CompilerParams(vmem_limit_bytes=1024 * 1024),
        cost_estimate=pl.CostEstimate(flops=1000 * full.size, bytes_accessed=2 * full.size, transcendentals=0),
    )(full)


def store_late(group, params, pieces):
    hbm = pl.BlockSpec(memory_space=pl.ANY)
    return pl.pallas_call(
        functools.partial(store_late_kernel, group),
        in_specs=[hbm] + [pl.BlockSpec(memory_space=pltpu.VMEM)] * 4,
        out_specs=hbm,
        out_shape=jax.ShapeDtypeStruct(params.shape, params.dtype),
        input_output_aliases={0: 0},
        scratch_shapes=[pltpu.SemaphoreType.DMA((4,))],
        compiler_params=pltpu.CompilerParams(vmem_limit_bytes=4 * 1024 * 1024),
    )(params, *pieces)


def solution(mesh):
    group = mesh.shape["data"]
    row_spec = P("stage", "data", None)
    full_spec = P("stage", None, None)

    def local_step(w_rows, mom_rows, grad_rows):
        params, mom_new, _, tail_r, tail_l = muon_step(group, mom_rows, grad_rows, w_rows)
        to_right = [(d, (d + 2) % group) for d in range(group)]
        to_left = [(d, (d - 2) % group) for d in range(group)]
        swap = [(d, d + 1 - 2 * (d % 2)) for d in range(group)]
        near = [lax.ppermute(tail_r, "data", to_right), lax.ppermute(tail_l, "data", to_left)]
        params = store_step(functools.partial(store_params_kernel, group), params, 2 * (group // 2 + 2))
        mom_new = store_step(store_kernel, mom_new, mom_new.shape[0])
        *near, params, mom_new = lax.optimization_barrier((*near, params, mom_new))
        far = [lax.ppermute(piece, "data", swap) for piece in near]
        return store_late(group, params, near + far), mom_new

    return jax.shard_map(
        local_step, mesh=mesh, in_specs=(row_spec, row_spec, row_spec), out_specs=(full_spec, row_spec), check_vma=False
    )
```

```python
import functools
import math

import jax
import jax.numpy as jnp
from jax import lax
from jax.experimental import pallas as pl
from jax.experimental.pallas import tpu as pltpu
from jax.sharding import PartitionSpec as P

NS_ITERS = 5
MOMENTUM = 0.95
LEARN_RATE = 0.02
WEIGHT_DECAY = 0.1
NORM_EPS = 1e-7
COEF_A = 3.4445
COEF_B = -4.7750
COEF_C = 2.0315

MESH = pl.DeviceIdType.MESH
TILE = 256
WIDE = 1024
SCALE_ROWS = 32
STEP_ROWS = 16
PREFETCH = 3


def ds(start, size):
    return pl.ds(pl.multiple_of(start, math.gcd(size, STEP_ROWS)), size)


def mirror(dst, block, start, cols):
    for i in range(start, start + block.shape[0], TILE):
        if not cols.start <= i < cols.stop:
            dst[cols, i : i + TILE] = block[i - start : i - start + TILE].T


def outer(x, rows, cols):
    prod = lax.dot_general(x[rows, :], x[cols, :], (((1,), (1,)), ((), ())), preferred_element_type=jnp.float32)
    return prod.astype(jnp.bfloat16)


def gram_of(x, gram, start, stop):
    for j in range(start, stop, TILE):
        cols = slice(j, j + TILE)
        block = outer(x, slice(j, stop), cols)
        gram[j:stop, cols] = block
        mirror(gram, block, j, cols)


def gram_last(x, gram):
    dim = gram.shape[0]
    cols = slice(dim - TILE, dim)
    block = outer(x, slice(0, dim), cols)
    gram[:, cols] = block
    mirror(gram, block, 0, cols)


def newton_schulz_poly(gram, poly):
    dim = gram.shape[0]
    for j in range(0, dim, TILE):
        rows, cols = slice(j, dim), slice(j, j + TILE)
        square = jnp.dot(gram[rows, :], gram[:, cols], preferred_element_type=jnp.float32)
        block = (COEF_B * gram[rows, cols].astype(jnp.float32) + COEF_C * square).astype(jnp.bfloat16)
        poly[rows, cols] = block
        mirror(poly, block, j, cols)


def newton_schulz_step(x, poly, part):
    old = x[:, part]
    prod = jnp.dot(poly[...], old, preferred_element_type=jnp.float32)
    x[:, part] = (COEF_A * old.astype(jnp.float32) + prod).astype(jnp.bfloat16)


def muon_kernel(group, mom, grad, w, out, mom_new, w_sib, tail_r, tail_l, x, gram, poly, relay, w_buf, w_ahead, sq, send, recv, go, free):
    chips = group // 2
    mats, rows, cols = mom.shape
    pair = 2 * rows
    dim = pair * chips
    rms_scale = 0.2 * math.sqrt(max(dim, cols))
    me = lax.axis_index("data")
    c, k = lax.div(me, 2), lax.rem(me, 2)
    sib = 2 * c + 1 - k
    right, left, opp = (lax.rem(c + step, chips) for step in (1, chips - 1, 2))

    def peer_of(chip):
        return 2 * chip + k

    def own_rows(chip, half=None):
        if half is None:
            return ds(chip * pair, pair)
        return ds(chip * pair + half * rows, rows)

    ahead = rows // 2
    ahead_start, rest_start, rest = k * (pair - ahead), (1 - k) * ahead, pair - ahead

    def ahead_rows(chip):
        return ds(chip * pair + ahead_start, ahead)

    def rest_rows(chip):
        return ds(chip * pair + rest_start, rest)

    split = STEP_ROWS * (rest // STEP_ROWS // 2)
    sizes = ((rows, rows), (rest - split, split), (split, rest - split), (rows, rows))

    def block(chip, step):
        return rest_rows(chip) if step in (1, 2) else own_rows(chip)

    def block_part(chip, step, way):
        start = rest_start if step in (1, 2) else 0
        return ds(chip * pair + start + way * sizes[step][0], sizes[step][way])

    def mine(chip, half=None):
        return out.at[2 * chip + k, own_rows(c, half)]

    sent, slots = [], {}

    def slot(key):
        return slots.setdefault(key, len(slots))

    def remote(src, dst, peer, key):
        copy = pltpu.make_async_remote_copy(
            src_ref=src, dst_ref=dst, send_sem=send.at[len(sent)], recv_sem=recv.at[slot(key)],
            device_id={"data": peer}, device_id_type=MESH)
        sent.append(copy)
        return copy

    def push(src, dst, peer, key):
        copy = remote(src, dst, peer, key)
        copy.start()
        return copy

    def load(src, dst, key):
        pltpu.make_async_copy(src, dst, recv.at[slot(key)]).start()

    def arrived(dst, key):
        pltpu.make_async_copy(dst, dst, recv.at[slot(key)]).wait()

    steps = (opp, left, right, c)

    def prefetch(n):
        if n < mats:
            par, step = divmod(n, chips)
            chip = steps[step]
            load(mom.at[2 * chip + par], mom_new.at[2 * chip + par], ("mom", step, par))
            load(grad.at[2 * chip + par], out.at[2 * chip + k, own_rows(left, par)], ("grad", step, par))

    for n in range(PREFETCH):
        prefetch(n)

    barrier = pltpu.get_barrier_semaphore()
    for step in range(1, group):
        pl.semaphore_signal(barrier, inc=1, device_id={"data": lax.rem(me + step, group)}, device_id_type=MESH)
    pl.semaphore_wait(barrier, group - 1)

    def momentum(step, chip, par):
        mat = 2 * chip + par
        base = jnp.where(k == par, c * pair + k * rows, right * pair)
        arrived(mom_new.at[mat], ("mom", step, par))
        arrived(out.at[2 * chip + k, own_rows(left, par)], ("grad", step, par))
        prefetch(par * chips + step + PREFETCH)

        def body(r, total):
            part = ds(r * STEP_ROWS, STEP_ROWS)
            low = out[2 * chip + k, ds(left * pair + par * rows + r * STEP_ROWS, STEP_ROWS), :]
            new = MOMENTUM * mom_new[mat, part, :] + low.astype(jnp.float32)
            mom_new[mat, part, :] = new
            out[2 * chip + k, ds(base + r * STEP_ROWS, STEP_ROWS), :] = new.astype(jnp.bfloat16)
            square = new * new
            lanes = square[:, :128]
            for start in range(128, cols, 128):
                lanes = lanes + square[:, start : start + 128]
            for start in range(0, STEP_ROWS, 8):
                total = total + lanes[start : start + 8]
            return total

        sq[0, mat] = lax.fori_loop(0, rows // STEP_ROWS, body, jnp.zeros((8, 128), jnp.float32))

    swap = [
        remote(out.at[2 * chip + k, own_rows(right, 0)], out.at[2 * chip + 1 - k, own_rows(c, k)], sib, ("swap", step))
        for step, chip in enumerate(steps)
    ]
    def x_rows(place, start=0, size=pair):
        return ds(place * pair + start, size)

    exchange = [
        [
            remote(mine(opp, 0), relay.at[0], peer_of(right), "a_relay_l"),
            remote(mine(opp, 1), relay.at[1], peer_of(left), "a_relay_r"),
        ],
        [remote(mine(left, half), x.at[x_rows(2, half * rows, rows)], peer_of(left), ("a_right", half)) for half in range(2)],
        [remote(mine(right, half), x.at[x_rows(1, half * rows, rows)], peer_of(right), ("a_left", half)) for half in range(2)],
        [],
    ]

    def swapped(step):
        arrived(mine(steps[step], 1 - k), ("swap", step))

    for step, chip in enumerate(steps):
        momentum(step, chip, 0)

        @pl.when(k == 1)
        def _():
            swap[step].start()

        @pl.when(k == 0)
        def _():
            for copy in exchange[step][:1]:
                copy.start()
            if step > 0:
                swapped(step - 1)
                for copy in exchange[step - 1][1:]:
                    copy.start()

    for step, chip in enumerate(steps):
        momentum(step, chip, 1)

        @pl.when(k == 0)
        def _():
            swap[step].start()
            if step == 0:
                swapped(chips - 1)

    for step in range(1, group):
        dest = lax.rem(me + step, group)
        push(sq.at[0, dest], sq.at[1, step], dest, ("sq", step))
    for step, chip in enumerate((c, left, right, opp)):
        push(w.at[2 * chip + 1 - k], w_sib.at[chip], sib, ("w_swap", step))

    @pl.when(k == 1)
    def _():
        pl.semaphore_wait(go, 1)
        for step in range(chips):
            swapped(step)
            for copy in exchange[step]:
                copy.start()

    arrived(relay.at[0], "a_relay_l")
    pass_right = push(relay.at[0], x.at[x_rows(3, 0, rows)], peer_of(right), "a_opp_l")
    arrived(relay.at[1], "a_relay_r")
    pass_left = push(relay.at[1], x.at[x_rows(3, rows, rows)], peer_of(left), "a_opp_r")
    push(w.at[2 * right + k, ds(k * ahead, ahead)], w_ahead.at[0], peer_of(right), "w_ahead_l")
    push(w.at[2 * left + k, ds(k * ahead, ahead)], w_ahead.at[1], peer_of(left), "w_ahead_r")

    total = sq[0, me]
    for step in range(1, group):
        arrived(sq.at[1, step], ("sq", step))
        total = total + sq[1, step]
    norm = jnp.sqrt(jnp.sum(total, keepdims=True))
    inverse = 1.0 / (norm + NORM_EPS)

    def scale(place, get):
        @pl.loop(0, pair // SCALE_ROWS)
        def _(r):
            part = x_rows(place, r * SCALE_ROWS, SCALE_ROWS)
            x[part, :] = (get(r, part).astype(jnp.float32) * inverse).astype(jnp.bfloat16)

    def arrived_row(_, part):
        return x[part, :]

    scale(0, lambda r, _: out[2 * c + k, ds(c * pair + r * SCALE_ROWS, SCALE_ROWS), :])
    for place, key in ((1, "a_left"), (2, "a_right")):
        for half in range(2):
            arrived(x.at[x_rows(place, half * rows, rows)], (key, half))
        scale(place, arrived_row)
    gram_of(x, gram, 0, dim - TILE)
    arrived(x.at[x_rows(3, 0, rows)], "a_opp_l")
    arrived(x.at[x_rows(3, rows, rows)], "a_opp_r")

    @pl.when(k == 0)
    def _():
        pl.semaphore_signal(go, inc=1, device_id={"data": sib}, device_id_type=MESH)

    scale(3, arrived_row)

    waited = swap + sum(exchange, []) + [pass_right, pass_left]
    for copy in waited:
        copy.wait_send()
    for chip in (right, left):
        pl.semaphore_signal(free, inc=1, device_id={"data": peer_of(chip)}, device_id_type=MESH)

    order = (c, left, right, opp)

    def load_w(step):
        load(w.at[2 * order[step] + k], w_buf.at[step % 2, ds(k * rows, rows)], ("w_own", step))
        arrived(w_sib.at[order[step]], ("w_swap", step))
        load(w_sib.at[order[step]], w_buf.at[step % 2, ds((1 - k) * rows, rows)], ("w_sib", step))

    load_w(0)
    load_w(1)

    gram_last(x, gram)

    @pl.loop(0, NS_ITERS - 1)
    def _(_):
        newton_schulz_poly(gram, poly)
        newton_schulz_step(x, poly, pl.ds(0, cols))
        gram_of(x, gram, 0, dim)

    newton_schulz_poly(gram, poly)
    pl.semaphore_wait(free, 2)

    chunks = [pl.ds(start, WIDE) for start in range(0, cols, WIDE)]
    for n, part in enumerate(chunks):
        newton_schulz_step(x, poly, part)
        push(x.at[x_rows(3, 0, rows), part], relay.at[0, :, part], peer_of(right), ("c_relay_l", n))
        push(x.at[x_rows(3, rows, rows), part], relay.at[1, :, part], peer_of(left), ("c_relay_r", n))
        push(x.at[x_rows(2, rest_start, rest), part], out.at[2 * c + k, rest_rows(right), part], peer_of(right), ("c_left", n))
        push(x.at[x_rows(1, rest_start, rest), part], out.at[2 * c + k, rest_rows(left), part], peer_of(left), ("c_right", n))

    def new_rows(mat, start, size, w_rows, get):
        @pl.loop(0, size // STEP_ROWS)
        def _(r):
            w_part = w_rows(r)
            part = ds(start + r * STEP_ROWS, STEP_ROWS)
            ortho = get(r, part).astype(jnp.float32) * rms_scale
            out[mat, part, :] = (w_part - LEARN_RATE * (ortho + WEIGHT_DECAY * w_part)).astype(jnp.bfloat16)

    last = chips - 1

    def update(step, get):
        chip = order[step]
        arrived(w_buf.at[step % 2, ds(k * rows, rows)], ("w_own", step))
        arrived(w_buf.at[step % 2, ds((1 - k) * rows, rows)], ("w_sib", step))
        start, size = (rest_start, rest) if step in (1, 2) else (0, pair)
        new_rows(
            2 * chip + k, c * pair + start, size, lambda r: w_buf[step % 2, ds(start + r * STEP_ROWS, STEP_ROWS), :],
            get)
        if step + 2 < chips:
            load_w(step + 2)
        place = out.at[2 * chip + k, block(c, step)]
        if step < last:
            push(place, place, peer_of(right), ("g_left", step))
            push(place, place, peer_of(left), ("g_right", step))
        else:
            parts = [out.at[2 * chip + k, block_part(c, step, way)] for way in range(2)]
            for way in range(2):
                push(parts[way], parts[way], peer_of(right), ("g_left", step, way))
                push(parts[1 - way], parts[1 - way], peer_of(left), ("g_right", step, 1 - way))
        push(place, place, sib, ("s_own", step))

    def update_ahead():
        for n, chip in enumerate((left, right)):
            arrived(w_ahead.at[n], ("w_ahead_l", "w_ahead_r")[n])
            new_rows(
                2 * c + k, chip * pair + ahead_start, ahead, lambda r: w_ahead[n, ds(r * STEP_ROWS, STEP_ROWS), :],
                lambda r, _: x[x_rows(1 + n, ahead_start + r * STEP_ROWS, STEP_ROWS), :])
            place = out.at[2 * c + k, ahead_rows(chip)]
            push(place, place, peer_of(right), ("e_left", n))
            push(place, place, peer_of(left), ("e_right", n))
            push(place, place, sib, ("s_ahead", n))

    update(0, lambda r, _: x[x_rows(0, r * STEP_ROWS, STEP_ROWS), :])
    update_ahead()
    for n, part in enumerate(chunks):
        arrived(relay.at[0, :, part], ("c_relay_l", n))
        push(relay.at[0, :, part], out.at[2 * left + k, own_rows(right, 0), part], peer_of(right), ("c_opp_l", n))
        arrived(relay.at[1, :, part], ("c_relay_r", n))
        push(relay.at[1, :, part], out.at[2 * right + k, own_rows(left, 1), part], peer_of(left), ("c_opp_r", n))

    for n, part in enumerate(chunks):
        arrived(out.at[2 * left + k, rest_rows(c), part], ("c_left", n))
    update(1, lambda _, part: out[2 * left + k, part, :])
    for n, part in enumerate(chunks):
        arrived(out.at[2 * right + k, rest_rows(c), part], ("c_right", n))
    update(2, lambda _, part: out[2 * right + k, part, :])
    for n, part in enumerate(chunks):
        arrived(out.at[2 * opp + k, own_rows(c, 0), part], ("c_opp_l", n))
        arrived(out.at[2 * opp + k, own_rows(c, 1), part], ("c_opp_r", n))
    update(3, lambda _, part: out[2 * opp + k, part, :])

    def near(chip, step):
        return lax.rem(chip + (0, chips - 1, 1, 2)[step], chips)

    def pass_on(mat, part, peer, key):
        push(out.at[mat, part], out.at[mat, part], peer, key)

    for step in range(last):
        mat_l, mat_r = 2 * near(left, step) + k, 2 * near(right, step) + k
        arrived(out.at[mat_l, block(left, step)], ("g_left", step))
        pass_on(mat_l, block_part(left, step, 0), peer_of(right), ("f_left", step))
        pass_on(mat_l, block(left, step), sib, ("s_left", step))
        arrived(out.at[mat_r, block(right, step)], ("g_right", step))
        pass_on(mat_r, block_part(right, step, 1), peer_of(left), ("f_right", step))
        pass_on(mat_r, block(right, step), sib, ("s_right", step))
        if step == 0:
            arrived(out.at[mat_l, ahead_rows(opp)], ("e_left", 0))
            pass_on(mat_l, ahead_rows(opp), peer_of(right), "fe_left")
            pass_on(mat_l, ahead_rows(opp), sib, ("s_ahead_l", 0))
            arrived(out.at[mat_l, ahead_rows(c)], ("e_left", 1))
            pass_on(mat_l, ahead_rows(c), sib, ("s_ahead_l", 1))
            arrived(out.at[mat_r, ahead_rows(c)], ("e_right", 0))
            pass_on(mat_r, ahead_rows(c), sib, ("s_ahead_r", 0))
            arrived(out.at[mat_r, ahead_rows(opp)], ("e_right", 1))
            pass_on(mat_r, ahead_rows(opp), peer_of(left), "fe_right")
            pass_on(mat_r, ahead_rows(opp), sib, ("s_ahead_r", 1))
    mat_l, mat_r = 2 * near(left, last) + k, 2 * near(right, last) + k
    for way in range(2):
        arrived(out.at[mat_l, block_part(left, last, way)], ("g_left", last, way))
        pass_on(mat_l, block_part(left, last, way), sib, ("s_left", last, way))
        arrived(out.at[mat_r, block_part(right, last, 1 - way)], ("g_right", last, 1 - way))
        pass_on(mat_r, block_part(right, last, 1 - way), sib, ("s_right", last, 1 - way))
        if way == 0:
            load(out.at[mat_l, block_part(left, last, 0)], tail_r, "tail_r")
            load(out.at[mat_r, block_part(right, last, 1)], tail_l, "tail_l")

    for step in range(last):
        mat = 2 * near(opp, step) + k
        arrived(out.at[mat, block_part(opp, step, 0)], ("f_left", step))
        pass_on(mat, block_part(opp, step, 0), sib, ("s_far_l", step))
        arrived(out.at[mat, block_part(opp, step, 1)], ("f_right", step))
        pass_on(mat, block_part(opp, step, 1), sib, ("s_far_r", step))
        if step == 0:
            arrived(out.at[mat, ahead_rows(right)], "fe_left")
            pass_on(mat, ahead_rows(right), sib, "s_far_ahead_l")
            arrived(out.at[mat, ahead_rows(left)], "fe_right")
            pass_on(mat, ahead_rows(left), sib, "s_far_ahead_r")

    def sib_ahead(chip):
        return ds(chip * pair + (1 - k) * (pair - ahead), ahead)

    def sib_start(chip, step):
        return chip * pair + (k * ahead if step in (1, 2) else 0)

    for step in range(chips):
        size = sum(sizes[step])
        arrived(out.at[2 * near(c, step) + 1 - k, ds(sib_start(c, step), size)], ("s_own", step))
        if step == last:
            for way in range(2):
                arrived(out.at[2 * near(left, step) + 1 - k, own_rows(left, way)], ("s_left", step, way))
                arrived(out.at[2 * near(right, step) + 1 - k, own_rows(right, way)], ("s_right", step, way))
        else:
            arrived(out.at[2 * near(left, step) + 1 - k, ds(sib_start(left, step), size)], ("s_left", step))
            arrived(out.at[2 * near(right, step) + 1 - k, ds(sib_start(right, step), size)], ("s_right", step))
            mat, start = 2 * near(opp, step) + 1 - k, sib_start(opp, step)
            arrived(out.at[mat, ds(start, sizes[step][0])], ("s_far_l", step))
            arrived(out.at[mat, ds(start + sizes[step][0], sizes[step][1])], ("s_far_r", step))
        if step == 0:
            for n, chip in enumerate((left, right)):
                arrived(out.at[2 * c + 1 - k, sib_ahead(chip)], ("s_ahead", n))
            for n, chip in enumerate((opp, c)):
                arrived(out.at[2 * left + 1 - k, sib_ahead(chip)], ("s_ahead_l", n))
            for n, chip in enumerate((c, opp)):
                arrived(out.at[2 * right + 1 - k, sib_ahead(chip)], ("s_ahead_r", n))
            arrived(out.at[2 * opp + 1 - k, sib_ahead(right)], "s_far_ahead_l")
            arrived(out.at[2 * opp + 1 - k, sib_ahead(left)], "s_far_ahead_r")
    arrived(tail_r, "tail_r")
    arrived(tail_l, "tail_l")
    for copy in sent:
        if not any(copy is done for done in waited):
            copy.wait_send()


def muon_step(group, mom, grad, w):
    mats, rows, cols = mom.shape
    chips, pair = group // 2, 2 * rows
    dim = pair * chips
    hbm = pl.BlockSpec(memory_space=pl.ANY)
    vmem = pl.BlockSpec(memory_space=pltpu.VMEM)
    return pl.pallas_call(
        functools.partial(muon_kernel, group),
        in_specs=[hbm, hbm, hbm],
        out_specs=[vmem, vmem, hbm, hbm, hbm],
        out_shape=[
            pltpu.VMEM((mats, dim, cols), jnp.bfloat16),
            pltpu.VMEM((mats, rows, cols), jnp.float32),
            pltpu.HBM((chips, rows, cols), jnp.float32),
            pltpu.HBM((rows, cols), jnp.bfloat16),
            pltpu.HBM((rows, cols), jnp.bfloat16),
        ],
        scratch_shapes=[
            pltpu.VMEM((dim, cols), jnp.bfloat16),
            pltpu.VMEM((dim, dim), jnp.bfloat16),
            pltpu.VMEM((dim, dim), jnp.bfloat16),
            pltpu.VMEM((2, rows, cols), jnp.bfloat16),
            pltpu.VMEM((2, pair, cols), jnp.float32),
            pltpu.VMEM((2, rows // 2, cols), jnp.float32),
            pltpu.VMEM((2, group, 8, 128), jnp.float32),
            pltpu.SemaphoreType.DMA((128,)),
            pltpu.SemaphoreType.DMA((128,)),
            pltpu.SemaphoreType.REGULAR,
            pltpu.SemaphoreType.REGULAR,
        ],
        compiler_params=pltpu.CompilerParams(
            collective_id=0, has_side_effects=True, vmem_limit_bytes=18 * 1024 * 1024
        ),
    )(mom, grad, w)


def run_copies(pairs, sem):
    copies = [pltpu.make_async_copy(src, dst, sem.at[n]) for n, (src, dst) in enumerate(pairs)]
    for copy in copies:
        copy.start()
    for copy in copies:
        copy.wait()


def place_of(params, group):
    me = lax.axis_index("data")
    rows = params.shape[1] // group
    chips = group // 2

    def part(chip, half=None):
        start = 2 * lax.rem(chip, chips) + (0 if half is None else half)
        return ds(start * rows, 2 * rows if half is None else rows)

    return lax.div(me, 2), lax.rem(me, 2), chips, part


def store_params_kernel(group, src, dst, sem):
    c, _, chips, part = place_of(src, group)
    pairs = []
    for par in range(2):
        for step in range(1, chips):
            mat = 2 * lax.rem(c + step, chips) + par
            pairs.append((src.at[mat], dst.at[mat]))
        for step in (0, 1, chips - 1):
            where = (2 * c + par, part(c + step))
            pairs.append((src.at[where], dst.at[where]))
    run_copies(pairs, sem)


def store_kernel(src, dst, sem):
    run_copies([(src.at[i], dst.at[i]) for i in range(src.shape[0])], sem)


def store_late_kernel(group, params, near_l, near_r, far_l, far_r, out, sem):
    c, k, _, part = place_of(out, group)
    pieces = ((near_l, k, 0), (near_r, k, 1), (far_l, 1 - k, 0), (far_r, 1 - k, 1))
    run_copies([(src, out.at[2 * c + par, part(c + 2, half)]) for src, par, half in pieces], sem)


def store_step(kernel, full, copies):
    return pl.pallas_call(
        kernel,
        in_specs=[pl.BlockSpec(memory_space=pltpu.VMEM)],
        out_specs=pl.BlockSpec(memory_space=pl.ANY),
        out_shape=jax.ShapeDtypeStruct(full.shape, full.dtype),
        scratch_shapes=[pltpu.SemaphoreType.DMA((copies,))],
        compiler_params=pltpu.CompilerParams(vmem_limit_bytes=1024 * 1024),
        cost_estimate=pl.CostEstimate(flops=1000 * full.size, bytes_accessed=2 * full.size, transcendentals=0),
    )(full)


def store_late(group, params, pieces):
    hbm = pl.BlockSpec(memory_space=pl.ANY)
    return pl.pallas_call(
        functools.partial(store_late_kernel, group),
        in_specs=[hbm] + [pl.BlockSpec(memory_space=pltpu.VMEM)] * 4,
        out_specs=hbm,
        out_shape=jax.ShapeDtypeStruct(params.shape, params.dtype),
        input_output_aliases={0: 0},
        scratch_shapes=[pltpu.SemaphoreType.DMA((4,))],
        compiler_params=pltpu.CompilerParams(vmem_limit_bytes=4 * 1024 * 1024),
    )(params, *pieces)


def solution(mesh):
    group = mesh.shape["data"]
    row_spec = P("stage", "data", None)
    full_spec = P("stage", None, None)

    def local_step(w_rows, mom_rows, grad_rows):
        params, mom_new, _, tail_r, tail_l = muon_step(group, mom_rows, grad_rows, w_rows)
        to_right = [(d, (d + 2) % group) for d in range(group)]
        to_left = [(d, (d - 2) % group) for d in range(group)]
        swap = [(d, d + 1 - 2 * (d % 2)) for d in range(group)]
        near = [lax.ppermute(tail_r, "data", to_right), lax.ppermute(tail_l, "data", to_left)]
        params = store_step(functools.partial(store_params_kernel, group), params, 2 * (group // 2 + 2))
        *near, params = lax.optimization_barrier((*near, params))
        far = [lax.ppermute(piece, "data", swap) for piece in near]
        mom_new = store_step(store_kernel, mom_new, mom_new.shape[0])
        *far, mom_new = lax.optimization_barrier((*far, mom_new))
        return store_late(group, params, near + far), mom_new

    return jax.shard_map(
        local_step, mesh=mesh, in_specs=(row_spec, row_spec, row_spec), out_specs=(full_spec, row_spec), check_vma=False
    )
```

```python
import functools
import math

import jax
import jax.numpy as jnp
from jax import lax
from jax.experimental import pallas as pl
from jax.experimental.pallas import tpu as pltpu
from jax.sharding import PartitionSpec as P

NS_ITERS = 5
MOMENTUM = 0.95
LEARN_RATE = 0.02
WEIGHT_DECAY = 0.1
NORM_EPS = 1e-7
COEF_A = 3.4445
COEF_B = -4.7750
COEF_C = 2.0315

MESH = pl.DeviceIdType.MESH
TILE = 256
WIDE = 1024
SCALE_ROWS = 32
STEP_ROWS = 16
PREFETCH = 3
AHEAD = 3


def ds(start, size):
    return pl.ds(pl.multiple_of(start, math.gcd(size, STEP_ROWS)), size)


def mirror(dst, block, start, cols):
    for i in range(start, start + block.shape[0], TILE):
        if not cols.start <= i < cols.stop:
            dst[cols, i : i + TILE] = block[i - start : i - start + TILE].T


def outer(x, rows, cols):
    prod = lax.dot_general(x[rows, :], x[cols, :], (((1,), (1,)), ((), ())), preferred_element_type=jnp.float32)
    return prod.astype(jnp.bfloat16)


def gram_of(x, gram, start, stop):
    for j in range(start, stop, TILE):
        cols = slice(j, j + TILE)
        block = outer(x, slice(j, stop), cols)
        gram[j:stop, cols] = block
        mirror(gram, block, j, cols)


def gram_last(x, gram):
    dim = gram.shape[0]
    cols = slice(dim - TILE, dim)
    block = outer(x, slice(0, dim), cols)
    gram[:, cols] = block
    mirror(gram, block, 0, cols)


def newton_schulz_poly(gram, poly):
    dim = gram.shape[0]
    for j in range(0, dim, TILE):
        rows, cols = slice(j, dim), slice(j, j + TILE)
        square = jnp.dot(gram[rows, :], gram[:, cols], preferred_element_type=jnp.float32)
        block = (COEF_B * gram[rows, cols].astype(jnp.float32) + COEF_C * square).astype(jnp.bfloat16)
        poly[rows, cols] = block
        mirror(poly, block, j, cols)


def newton_schulz_step(x, poly, part):
    old = x[:, part]
    prod = jnp.dot(poly[...], old, preferred_element_type=jnp.float32)
    x[:, part] = (COEF_A * old.astype(jnp.float32) + prod).astype(jnp.bfloat16)


def muon_kernel(group, mom, grad, w, out, mom_new, w_sib, tail_r, tail_l, x, gram, poly, relay, w_buf, w_ahead, sq, send, recv, go, free):
    chips = group // 2
    mats, rows, cols = mom.shape
    pair = 2 * rows
    dim = pair * chips
    rms_scale = 0.2 * math.sqrt(max(dim, cols))
    me = lax.axis_index("data")
    c, k = lax.div(me, 2), lax.rem(me, 2)
    sib = 2 * c + 1 - k
    right, left, opp = (lax.rem(c + step, chips) for step in (1, chips - 1, 2))

    def peer_of(chip):
        return 2 * chip + k

    def own_rows(chip, half=None):
        if half is None:
            return ds(chip * pair, pair)
        return ds(chip * pair + half * rows, rows)

    ahead = rows // AHEAD
    ahead_start, rest_start, rest = k * (pair - ahead), (1 - k) * ahead, pair - ahead

    def ahead_rows(chip):
        return ds(chip * pair + ahead_start, ahead)

    def rest_rows(chip):
        return ds(chip * pair + rest_start, rest)

    split = STEP_ROWS * (rest // STEP_ROWS // 2)
    sizes = ((rows, rows), (rest - split, split), (split, rest - split), (rows, rows))

    def block(chip, step):
        return rest_rows(chip) if step in (1, 2) else own_rows(chip)

    def block_part(chip, step, way):
        start = rest_start if step in (1, 2) else 0
        return ds(chip * pair + start + way * sizes[step][0], sizes[step][way])

    def mine(chip, half=None):
        return out.at[2 * chip + k, own_rows(c, half)]

    sent, slots = [], {}

    def slot(key):
        return slots.setdefault(key, len(slots))

    def remote(src, dst, peer, key):
        copy = pltpu.make_async_remote_copy(
            src_ref=src, dst_ref=dst, send_sem=send.at[len(sent)], recv_sem=recv.at[slot(key)],
            device_id={"data": peer}, device_id_type=MESH)
        sent.append(copy)
        return copy

    def push(src, dst, peer, key):
        copy = remote(src, dst, peer, key)
        copy.start()
        return copy

    def load(src, dst, key):
        pltpu.make_async_copy(src, dst, recv.at[slot(key)]).start()

    def arrived(dst, key):
        pltpu.make_async_copy(dst, dst, recv.at[slot(key)]).wait()

    steps = (opp, left, right, c)

    def prefetch(n):
        if n < mats:
            par, step = divmod(n, chips)
            chip = steps[step]
            load(mom.at[2 * chip + par], mom_new.at[2 * chip + par], ("mom", step, par))
            load(grad.at[2 * chip + par], out.at[2 * chip + k, own_rows(left, par)], ("grad", step, par))

    for n in range(PREFETCH):
        prefetch(n)

    barrier = pltpu.get_barrier_semaphore()
    for step in range(1, group):
        pl.semaphore_signal(barrier, inc=1, device_id={"data": lax.rem(me + step, group)}, device_id_type=MESH)
    pl.semaphore_wait(barrier, group - 1)

    def momentum(step, chip, par):
        mat = 2 * chip + par
        base = jnp.where(k == par, c * pair + k * rows, right * pair)
        arrived(mom_new.at[mat], ("mom", step, par))
        arrived(out.at[2 * chip + k, own_rows(left, par)], ("grad", step, par))
        prefetch(par * chips + step + PREFETCH)

        def body(r, total):
            part = ds(r * STEP_ROWS, STEP_ROWS)
            low = out[2 * chip + k, ds(left * pair + par * rows + r * STEP_ROWS, STEP_ROWS), :]
            new = MOMENTUM * mom_new[mat, part, :] + low.astype(jnp.float32)
            mom_new[mat, part, :] = new
            out[2 * chip + k, ds(base + r * STEP_ROWS, STEP_ROWS), :] = new.astype(jnp.bfloat16)
            square = new * new
            lanes = square[:, :128]
            for start in range(128, cols, 128):
                lanes = lanes + square[:, start : start + 128]
            for start in range(0, STEP_ROWS, 8):
                total = total + lanes[start : start + 8]
            return total

        sq[0, mat] = lax.fori_loop(0, rows // STEP_ROWS, body, jnp.zeros((8, 128), jnp.float32))

    swap = [
        remote(out.at[2 * chip + k, own_rows(right, 0)], out.at[2 * chip + 1 - k, own_rows(c, k)], sib, ("swap", step))
        for step, chip in enumerate(steps)
    ]
    def x_rows(place, start=0, size=pair):
        return ds(place * pair + start, size)

    exchange = [
        [
            remote(mine(opp, 0), relay.at[0], peer_of(right), "a_relay_l"),
            remote(mine(opp, 1), relay.at[1], peer_of(left), "a_relay_r"),
        ],
        [remote(mine(left, half), x.at[x_rows(2, half * rows, rows)], peer_of(left), ("a_right", half)) for half in range(2)],
        [remote(mine(right, half), x.at[x_rows(1, half * rows, rows)], peer_of(right), ("a_left", half)) for half in range(2)],
        [],
    ]

    def swapped(step):
        arrived(mine(steps[step], 1 - k), ("swap", step))

    for step, chip in enumerate(steps):
        momentum(step, chip, 0)

        @pl.when(k == 1)
        def _():
            swap[step].start()

        @pl.when(k == 0)
        def _():
            for copy in exchange[step][:1]:
                copy.start()
            if step > 0:
                swapped(step - 1)
                for copy in exchange[step - 1][1:]:
                    copy.start()

    for step, chip in enumerate(steps):
        momentum(step, chip, 1)

        @pl.when(k == 0)
        def _():
            swap[step].start()
            if step == 0:
                swapped(chips - 1)

    for step in range(1, group):
        dest = lax.rem(me + step, group)
        push(sq.at[0, dest], sq.at[1, step], dest, ("sq", step))
    for step, chip in enumerate((c, left, right, opp)):
        push(w.at[2 * chip + 1 - k], w_sib.at[chip], sib, ("w_swap", step))

    @pl.when(k == 1)
    def _():
        pl.semaphore_wait(go, 1)
        for step in range(chips):
            swapped(step)
            for copy in exchange[step]:
                copy.start()

    arrived(relay.at[0], "a_relay_l")
    pass_right = push(relay.at[0], x.at[x_rows(3, 0, rows)], peer_of(right), "a_opp_l")
    arrived(relay.at[1], "a_relay_r")
    pass_left = push(relay.at[1], x.at[x_rows(3, rows, rows)], peer_of(left), "a_opp_r")
    push(w.at[2 * right + k, ds(k * (rows - ahead), ahead)], w_ahead.at[0], peer_of(right), "w_ahead_l")
    push(w.at[2 * left + k, ds(k * (rows - ahead), ahead)], w_ahead.at[1], peer_of(left), "w_ahead_r")

    total = sq[0, me]
    for step in range(1, group):
        arrived(sq.at[1, step], ("sq", step))
        total = total + sq[1, step]
    norm = jnp.sqrt(jnp.sum(total, keepdims=True))
    inverse = 1.0 / (norm + NORM_EPS)

    def scale(place, get):
        @pl.loop(0, pair // SCALE_ROWS)
        def _(r):
            part = x_rows(place, r * SCALE_ROWS, SCALE_ROWS)
            x[part, :] = (get(r, part).astype(jnp.float32) * inverse).astype(jnp.bfloat16)

    def arrived_row(_, part):
        return x[part, :]

    scale(0, lambda r, _: out[2 * c + k, ds(c * pair + r * SCALE_ROWS, SCALE_ROWS), :])
    for place, key in ((1, "a_left"), (2, "a_right")):
        for half in range(2):
            arrived(x.at[x_rows(place, half * rows, rows)], (key, half))
        scale(place, arrived_row)
    gram_of(x, gram, 0, dim - TILE)
    arrived(x.at[x_rows(3, 0, rows)], "a_opp_l")
    arrived(x.at[x_rows(3, rows, rows)], "a_opp_r")

    @pl.when(k == 0)
    def _():
        pl.semaphore_signal(go, inc=1, device_id={"data": sib}, device_id_type=MESH)

    scale(3, arrived_row)

    waited = swap + sum(exchange, []) + [pass_right, pass_left]
    for copy in waited:
        copy.wait_send()
    for chip in (right, left):
        pl.semaphore_signal(free, inc=1, device_id={"data": peer_of(chip)}, device_id_type=MESH)

    order = (c, left, right, opp)

    def load_w(step):
        load(w.at[2 * order[step] + k], w_buf.at[step % 2, ds(k * rows, rows)], ("w_own", step))
        arrived(w_sib.at[order[step]], ("w_swap", step))
        load(w_sib.at[order[step]], w_buf.at[step % 2, ds((1 - k) * rows, rows)], ("w_sib", step))

    load_w(0)
    load_w(1)

    gram_last(x, gram)

    @pl.loop(0, NS_ITERS - 1)
    def _(_):
        newton_schulz_poly(gram, poly)
        newton_schulz_step(x, poly, pl.ds(0, cols))
        gram_of(x, gram, 0, dim)

    newton_schulz_poly(gram, poly)
    pl.semaphore_wait(free, 2)

    chunks = [pl.ds(start, WIDE) for start in range(0, cols, WIDE)]
    for n, part in enumerate(chunks):
        newton_schulz_step(x, poly, part)
        push(x.at[x_rows(3, 0, rows), part], relay.at[0, :, part], peer_of(right), ("c_relay_l", n))
        push(x.at[x_rows(3, rows, rows), part], relay.at[1, :, part], peer_of(left), ("c_relay_r", n))
        push(x.at[x_rows(2, rest_start, rest), part], out.at[2 * c + k, rest_rows(right), part], peer_of(right), ("c_left", n))
        push(x.at[x_rows(1, rest_start, rest), part], out.at[2 * c + k, rest_rows(left), part], peer_of(left), ("c_right", n))

    def new_rows(mat, start, size, w_rows, get):
        @pl.loop(0, size // STEP_ROWS)
        def _(r):
            w_part = w_rows(r)
            part = ds(start + r * STEP_ROWS, STEP_ROWS)
            ortho = get(r, part).astype(jnp.float32) * rms_scale
            out[mat, part, :] = (w_part - LEARN_RATE * (ortho + WEIGHT_DECAY * w_part)).astype(jnp.bfloat16)

    last = chips - 1

    def update(step, get):
        chip = order[step]
        arrived(w_buf.at[step % 2, ds(k * rows, rows)], ("w_own", step))
        arrived(w_buf.at[step % 2, ds((1 - k) * rows, rows)], ("w_sib", step))
        start, size = (rest_start, rest) if step in (1, 2) else (0, pair)
        new_rows(
            2 * chip + k, c * pair + start, size, lambda r: w_buf[step % 2, ds(start + r * STEP_ROWS, STEP_ROWS), :],
            get)
        if step + 2 < chips:
            load_w(step + 2)
        place = out.at[2 * chip + k, block(c, step)]
        if step < last:
            push(place, place, peer_of(right), ("g_left", step))
            push(place, place, peer_of(left), ("g_right", step))
        else:
            parts = [out.at[2 * chip + k, block_part(c, step, way)] for way in range(2)]
            for way in range(2):
                push(parts[way], parts[way], peer_of(right), ("g_left", step, way))
                push(parts[1 - way], parts[1 - way], peer_of(left), ("g_right", step, 1 - way))
        push(place, place, sib, ("s_own", step))

    def update_ahead():
        for n, chip in enumerate((left, right)):
            arrived(w_ahead.at[n], ("w_ahead_l", "w_ahead_r")[n])
            new_rows(
                2 * c + k, chip * pair + ahead_start, ahead, lambda r: w_ahead[n, ds(r * STEP_ROWS, STEP_ROWS), :],
                lambda r, _: x[x_rows(1 + n, ahead_start + r * STEP_ROWS, STEP_ROWS), :])
            place = out.at[2 * c + k, ahead_rows(chip)]
            push(place, place, peer_of(right), ("e_left", n))
            push(place, place, peer_of(left), ("e_right", n))
            push(place, place, sib, ("s_ahead", n))

    update(0, lambda r, _: x[x_rows(0, r * STEP_ROWS, STEP_ROWS), :])
    update_ahead()
    for n, part in enumerate(chunks):
        arrived(relay.at[0, :, part], ("c_relay_l", n))
        push(relay.at[0, :, part], out.at[2 * left + k, own_rows(right, 0), part], peer_of(right), ("c_opp_l", n))
        arrived(relay.at[1, :, part], ("c_relay_r", n))
        push(relay.at[1, :, part], out.at[2 * right + k, own_rows(left, 1), part], peer_of(left), ("c_opp_r", n))

    for n, part in enumerate(chunks):
        arrived(out.at[2 * left + k, rest_rows(c), part], ("c_left", n))
    update(1, lambda _, part: out[2 * left + k, part, :])
    for n, part in enumerate(chunks):
        arrived(out.at[2 * right + k, rest_rows(c), part], ("c_right", n))
    update(2, lambda _, part: out[2 * right + k, part, :])
    for n, part in enumerate(chunks):
        arrived(out.at[2 * opp + k, own_rows(c, 0), part], ("c_opp_l", n))
        arrived(out.at[2 * opp + k, own_rows(c, 1), part], ("c_opp_r", n))
    update(3, lambda _, part: out[2 * opp + k, part, :])

    def near(chip, step):
        return lax.rem(chip + (0, chips - 1, 1, 2)[step], chips)

    def pass_on(mat, part, peer, key):
        push(out.at[mat, part], out.at[mat, part], peer, key)

    for step in range(last):
        mat_l, mat_r = 2 * near(left, step) + k, 2 * near(right, step) + k
        arrived(out.at[mat_l, block(left, step)], ("g_left", step))
        pass_on(mat_l, block_part(left, step, 0), peer_of(right), ("f_left", step))
        pass_on(mat_l, block(left, step), sib, ("s_left", step))
        arrived(out.at[mat_r, block(right, step)], ("g_right", step))
        pass_on(mat_r, block_part(right, step, 1), peer_of(left), ("f_right", step))
        pass_on(mat_r, block(right, step), sib, ("s_right", step))
        if step == 0:
            arrived(out.at[mat_l, ahead_rows(opp)], ("e_left", 0))
            pass_on(mat_l, ahead_rows(opp), peer_of(right), "fe_left")
            pass_on(mat_l, ahead_rows(opp), sib, ("s_ahead_l", 0))
            arrived(out.at[mat_l, ahead_rows(c)], ("e_left", 1))
            pass_on(mat_l, ahead_rows(c), sib, ("s_ahead_l", 1))
            arrived(out.at[mat_r, ahead_rows(c)], ("e_right", 0))
            pass_on(mat_r, ahead_rows(c), sib, ("s_ahead_r", 0))
            arrived(out.at[mat_r, ahead_rows(opp)], ("e_right", 1))
            pass_on(mat_r, ahead_rows(opp), peer_of(left), "fe_right")
            pass_on(mat_r, ahead_rows(opp), sib, ("s_ahead_r", 1))
    mat_l, mat_r = 2 * near(left, last) + k, 2 * near(right, last) + k
    for way in range(2):
        arrived(out.at[mat_l, block_part(left, last, way)], ("g_left", last, way))
        pass_on(mat_l, block_part(left, last, way), sib, ("s_left", last, way))
        arrived(out.at[mat_r, block_part(right, last, 1 - way)], ("g_right", last, 1 - way))
        pass_on(mat_r, block_part(right, last, 1 - way), sib, ("s_right", last, 1 - way))
        if way == 0:
            load(out.at[mat_l, block_part(left, last, 0)], tail_r, "tail_r")
            load(out.at[mat_r, block_part(right, last, 1)], tail_l, "tail_l")

    for step in range(last):
        mat = 2 * near(opp, step) + k
        arrived(out.at[mat, block_part(opp, step, 0)], ("f_left", step))
        pass_on(mat, block_part(opp, step, 0), sib, ("s_far_l", step))
        arrived(out.at[mat, block_part(opp, step, 1)], ("f_right", step))
        pass_on(mat, block_part(opp, step, 1), sib, ("s_far_r", step))
        if step == 0:
            arrived(out.at[mat, ahead_rows(right)], "fe_left")
            pass_on(mat, ahead_rows(right), sib, "s_far_ahead_l")
            arrived(out.at[mat, ahead_rows(left)], "fe_right")
            pass_on(mat, ahead_rows(left), sib, "s_far_ahead_r")

    def sib_ahead(chip):
        return ds(chip * pair + (1 - k) * (pair - ahead), ahead)

    def sib_start(chip, step):
        return chip * pair + (k * ahead if step in (1, 2) else 0)

    for step in range(chips):
        size = sum(sizes[step])
        arrived(out.at[2 * near(c, step) + 1 - k, ds(sib_start(c, step), size)], ("s_own", step))
        if step == last:
            for way in range(2):
                arrived(out.at[2 * near(left, step) + 1 - k, own_rows(left, way)], ("s_left", step, way))
                arrived(out.at[2 * near(right, step) + 1 - k, own_rows(right, way)], ("s_right", step, way))
        else:
            arrived(out.at[2 * near(left, step) + 1 - k, ds(sib_start(left, step), size)], ("s_left", step))
            arrived(out.at[2 * near(right, step) + 1 - k, ds(sib_start(right, step), size)], ("s_right", step))
            mat, start = 2 * near(opp, step) + 1 - k, sib_start(opp, step)
            arrived(out.at[mat, ds(start, sizes[step][0])], ("s_far_l", step))
            arrived(out.at[mat, ds(start + sizes[step][0], sizes[step][1])], ("s_far_r", step))
        if step == 0:
            for n, chip in enumerate((left, right)):
                arrived(out.at[2 * c + 1 - k, sib_ahead(chip)], ("s_ahead", n))
            for n, chip in enumerate((opp, c)):
                arrived(out.at[2 * left + 1 - k, sib_ahead(chip)], ("s_ahead_l", n))
            for n, chip in enumerate((c, opp)):
                arrived(out.at[2 * right + 1 - k, sib_ahead(chip)], ("s_ahead_r", n))
            arrived(out.at[2 * opp + 1 - k, sib_ahead(right)], "s_far_ahead_l")
            arrived(out.at[2 * opp + 1 - k, sib_ahead(left)], "s_far_ahead_r")
    arrived(tail_r, "tail_r")
    arrived(tail_l, "tail_l")
    for copy in sent:
        if not any(copy is done for done in waited):
            copy.wait_send()


def muon_step(group, mom, grad, w):
    mats, rows, cols = mom.shape
    chips, pair = group // 2, 2 * rows
    dim = pair * chips
    hbm = pl.BlockSpec(memory_space=pl.ANY)
    vmem = pl.BlockSpec(memory_space=pltpu.VMEM)
    return pl.pallas_call(
        functools.partial(muon_kernel, group),
        in_specs=[hbm, hbm, hbm],
        out_specs=[vmem, vmem, hbm, hbm, hbm],
        out_shape=[
            pltpu.VMEM((mats, dim, cols), jnp.bfloat16),
            pltpu.VMEM((mats, rows, cols), jnp.float32),
            pltpu.HBM((chips, rows, cols), jnp.float32),
            pltpu.HBM((rows, cols), jnp.bfloat16),
            pltpu.HBM((rows, cols), jnp.bfloat16),
        ],
        scratch_shapes=[
            pltpu.VMEM((dim, cols), jnp.bfloat16),
            pltpu.VMEM((dim, dim), jnp.bfloat16),
            pltpu.VMEM((dim, dim), jnp.bfloat16),
            pltpu.VMEM((2, rows, cols), jnp.bfloat16),
            pltpu.VMEM((2, pair, cols), jnp.float32),
            pltpu.VMEM((2, rows // AHEAD, cols), jnp.float32),
            pltpu.VMEM((2, group, 8, 128), jnp.float32),
            pltpu.SemaphoreType.DMA((128,)),
            pltpu.SemaphoreType.DMA((128,)),
            pltpu.SemaphoreType.REGULAR,
            pltpu.SemaphoreType.REGULAR,
        ],
        compiler_params=pltpu.CompilerParams(
            collective_id=0, has_side_effects=True, vmem_limit_bytes=18 * 1024 * 1024
        ),
    )(mom, grad, w)


def run_copies(pairs, sem):
    copies = [pltpu.make_async_copy(src, dst, sem.at[n]) for n, (src, dst) in enumerate(pairs)]
    for copy in copies:
        copy.start()
    for copy in copies:
        copy.wait()


def place_of(params, group):
    me = lax.axis_index("data")
    rows = params.shape[1] // group
    chips = group // 2

    def part(chip, half=None):
        start = 2 * lax.rem(chip, chips) + (0 if half is None else half)
        return ds(start * rows, 2 * rows if half is None else rows)

    return lax.div(me, 2), lax.rem(me, 2), chips, part


def store_params_kernel(group, src, dst, sem):
    c, _, chips, part = place_of(src, group)
    pairs = []
    for par in range(2):
        for step in range(1, chips):
            mat = 2 * lax.rem(c + step, chips) + par
            pairs.append((src.at[mat], dst.at[mat]))
        for step in (0, 1, chips - 1):
            where = (2 * c + par, part(c + step))
            pairs.append((src.at[where], dst.at[where]))
    run_copies(pairs, sem)


def store_kernel(src, dst, sem):
    run_copies([(src.at[i], dst.at[i]) for i in range(src.shape[0])], sem)


def store_late_kernel(group, params, near_l, near_r, far_l, far_r, out, sem):
    c, k, _, part = place_of(out, group)
    pieces = ((near_l, k, 0), (near_r, k, 1), (far_l, 1 - k, 0), (far_r, 1 - k, 1))
    run_copies([(src, out.at[2 * c + par, part(c + 2, half)]) for src, par, half in pieces], sem)


def store_step(kernel, full, copies):
    return pl.pallas_call(
        kernel,
        in_specs=[pl.BlockSpec(memory_space=pltpu.VMEM)],
        out_specs=pl.BlockSpec(memory_space=pl.ANY),
        out_shape=jax.ShapeDtypeStruct(full.shape, full.dtype),
        scratch_shapes=[pltpu.SemaphoreType.DMA((copies,))],
        compiler_params=pltpu.CompilerParams(vmem_limit_bytes=1024 * 1024),
        cost_estimate=pl.CostEstimate(flops=1000 * full.size, bytes_accessed=2 * full.size, transcendentals=0),
    )(full)


def store_late(group, params, pieces):
    hbm = pl.BlockSpec(memory_space=pl.ANY)
    return pl.pallas_call(
        functools.partial(store_late_kernel, group),
        in_specs=[hbm] + [pl.BlockSpec(memory_space=pltpu.VMEM)] * 4,
        out_specs=hbm,
        out_shape=jax.ShapeDtypeStruct(params.shape, params.dtype),
        input_output_aliases={0: 0},
        scratch_shapes=[pltpu.SemaphoreType.DMA((4,))],
        compiler_params=pltpu.CompilerParams(vmem_limit_bytes=4 * 1024 * 1024),
    )(params, *pieces)


def solution(mesh):
    group = mesh.shape["data"]
    row_spec = P("stage", "data", None)
    full_spec = P("stage", None, None)

    def local_step(w_rows, mom_rows, grad_rows):
        params, mom_new, _, tail_r, tail_l = muon_step(group, mom_rows, grad_rows, w_rows)
        to_right = [(d, (d + 2) % group) for d in range(group)]
        to_left = [(d, (d - 2) % group) for d in range(group)]
        swap = [(d, d + 1 - 2 * (d % 2)) for d in range(group)]
        near = [lax.ppermute(tail_r, "data", to_right), lax.ppermute(tail_l, "data", to_left)]
        params = store_step(functools.partial(store_params_kernel, group), params, 2 * (group // 2 + 2))
        *near, params = lax.optimization_barrier((*near, params))
        far = [lax.ppermute(piece, "data", swap) for piece in near]
        mom_new = store_step(store_kernel, mom_new, mom_new.shape[0])
        *far, mom_new = lax.optimization_barrier((*far, mom_new))
        return store_late(group, params, near + far), mom_new

    return jax.shard_map(
        local_step, mesh=mesh, in_specs=(row_spec, row_spec, row_spec), out_specs=(full_spec, row_spec), check_vma=False
    )
```

```python
import functools
import math

import jax
import jax.numpy as jnp
from jax import lax
from jax.experimental import pallas as pl
from jax.experimental.pallas import tpu as pltpu
from jax.sharding import PartitionSpec as P

NS_ITERS = 5
MOMENTUM = 0.95
LEARN_RATE = 0.02
WEIGHT_DECAY = 0.1
NORM_EPS = 1e-7
COEF_A = 3.4445
COEF_B = -4.7750
COEF_C = 2.0315

MESH = pl.DeviceIdType.MESH
TILE = 256
WIDE = 1024
SCALE_ROWS = 32
STEP_ROWS = 16
PREFETCH = 3


def ds(start, size):
    return pl.ds(pl.multiple_of(start, math.gcd(size, STEP_ROWS)), size)


def symmetric(dst, product, finish, dim):
    for j in range(0, dim, TILE):
        cols = slice(j, j + TILE)
        block = finish(product(slice(j, dim), cols), slice(j, dim), cols)
        dst[j:, cols] = block
        for i in range(j + TILE, dim, TILE):
            dst[cols, i : i + TILE] = block[i - j : i - j + TILE].T


def newton_schulz_poly(x, gram, poly):
    dim = gram.shape[0]

    def outer(rows, cols):
        return lax.dot_general(x[rows, :], x[cols, :], (((1,), (1,)), ((), ())), preferred_element_type=jnp.float32)

    def square(rows, cols):
        return jnp.dot(gram[rows, :], gram[:, cols], preferred_element_type=jnp.float32)

    symmetric(gram, outer, lambda prod, rows, cols: prod.astype(jnp.bfloat16), dim)
    symmetric(
        poly,
        square,
        lambda prod, rows, cols: (COEF_B * gram[rows, cols].astype(jnp.float32) + COEF_C * prod).astype(jnp.bfloat16),
        dim,
    )


def newton_schulz_step(x, poly, part):
    old = x[:, part]
    prod = jnp.dot(poly[...], old, preferred_element_type=jnp.float32)
    x[:, part] = (COEF_A * old.astype(jnp.float32) + prod).astype(jnp.bfloat16)


def muon_kernel(group, mom, grad, w, out, mom_new, w_sib, tail_r, tail_l, x, gram, poly, relay, w_buf, w_ahead, sq, send, recv, go, free):
    chips = group // 2
    mats, rows, cols = mom.shape
    pair = 2 * rows
    dim = pair * chips
    rms_scale = 0.2 * math.sqrt(max(dim, cols))
    me = lax.axis_index("data")
    c, k = lax.div(me, 2), lax.rem(me, 2)
    sib = 2 * c + 1 - k
    right, left, opp = (lax.rem(c + step, chips) for step in (1, chips - 1, 2))

    def peer_of(chip):
        return 2 * chip + k

    def own_rows(chip, half=None):
        if half is None:
            return ds(chip * pair, pair)
        return ds(chip * pair + half * rows, rows)

    ahead = rows // 2
    ahead_start, rest_start, rest = k * (pair - ahead), (1 - k) * ahead, pair - ahead

    def ahead_rows(chip):
        return ds(chip * pair + ahead_start, ahead)

    def rest_rows(chip):
        return ds(chip * pair + rest_start, rest)

    split = STEP_ROWS * (rest // STEP_ROWS // 2)
    sizes = ((rows, rows), (rest - split, split), (split, rest - split), (rows, rows))

    def block(chip, step):
        return rest_rows(chip) if step in (1, 2) else own_rows(chip)

    def block_part(chip, step, way):
        start = rest_start if step in (1, 2) else 0
        return ds(chip * pair + start + way * sizes[step][0], sizes[step][way])

    def mine(chip, half=None):
        return out.at[2 * chip + k, own_rows(c, half)]

    sent, slots = [], {}

    def slot(key):
        return slots.setdefault(key, len(slots))

    def remote(src, dst, peer, key):
        copy = pltpu.make_async_remote_copy(
            src_ref=src, dst_ref=dst, send_sem=send.at[len(sent)], recv_sem=recv.at[slot(key)],
            device_id={"data": peer}, device_id_type=MESH)
        sent.append(copy)
        return copy

    def push(src, dst, peer, key):
        copy = remote(src, dst, peer, key)
        copy.start()
        return copy

    def load(src, dst, key):
        pltpu.make_async_copy(src, dst, recv.at[slot(key)]).start()

    def arrived(dst, key):
        pltpu.make_async_copy(dst, dst, recv.at[slot(key)]).wait()

    steps = (opp, left, right, c)

    def prefetch(n):
        if n < mats:
            par, step = divmod(n, chips)
            chip = steps[step]
            load(mom.at[2 * chip + par], mom_new.at[2 * chip + par], ("mom", step, par))
            load(grad.at[2 * chip + par], out.at[2 * chip + k, own_rows(left, par)], ("grad", step, par))

    for n in range(PREFETCH):
        prefetch(n)

    barrier = pltpu.get_barrier_semaphore()
    for step in range(1, group):
        pl.semaphore_signal(barrier, inc=1, device_id={"data": lax.rem(me + step, group)}, device_id_type=MESH)

    def momentum(step, chip, par):
        mat = 2 * chip + par
        base = jnp.where(k == par, c * pair + k * rows, right * pair)
        arrived(mom_new.at[mat], ("mom", step, par))
        arrived(out.at[2 * chip + k, own_rows(left, par)], ("grad", step, par))
        prefetch(par * chips + step + PREFETCH)

        def body(r, total):
            part = ds(r * STEP_ROWS, STEP_ROWS)
            low = out[2 * chip + k, ds(left * pair + par * rows + r * STEP_ROWS, STEP_ROWS), :]
            new = MOMENTUM * mom_new[mat, part, :] + low.astype(jnp.float32)
            mom_new[mat, part, :] = new
            out[2 * chip + k, ds(base + r * STEP_ROWS, STEP_ROWS), :] = new.astype(jnp.bfloat16)
            square = new * new
            lanes = square[:, :128]
            for start in range(128, cols, 128):
                lanes = lanes + square[:, start : start + 128]
            for start in range(0, STEP_ROWS, 8):
                total = total + lanes[start : start + 8]
            return total

        sq[0, mat] = lax.fori_loop(0, rows // STEP_ROWS, body, jnp.zeros((8, 128), jnp.float32))

    swap = [
        remote(out.at[2 * chip + k, own_rows(right, 0)], out.at[2 * chip + 1 - k, own_rows(c, k)], sib, ("swap", step))
        for step, chip in enumerate(steps)
    ]
    exchange = [
        [
            remote(mine(opp, 0), relay.at[0], peer_of(right), "a_relay_l"),
            remote(mine(opp, 1), relay.at[1], peer_of(left), "a_relay_r"),
        ],
        [remote(mine(left, half), x.at[own_rows(c, half)], peer_of(left), ("a_right", half)) for half in range(2)],
        [remote(mine(right, half), x.at[own_rows(c, half)], peer_of(right), ("a_left", half)) for half in range(2)],
        [],
    ]

    def swapped(step):
        arrived(mine(steps[step], 1 - k), ("swap", step))

    for step, chip in enumerate(steps):
        momentum(step, chip, 0)
        if step == 0:
            pl.semaphore_wait(barrier, group - 1)

        @pl.when(k == 1)
        def _():
            swap[step].start()

        @pl.when(k == 0)
        def _():
            for copy in exchange[step][:1]:
                copy.start()
            if step > 0:
                swapped(step - 1)
                for copy in exchange[step - 1][1:]:
                    copy.start()

    for step, chip in enumerate(steps):
        momentum(step, chip, 1)

        @pl.when(k == 0)
        def _():
            swap[step].start()
            if step == 0:
                swapped(chips - 1)

    for step in range(1, group):
        dest = lax.rem(me + step, group)
        push(sq.at[0, dest], sq.at[1, step], dest, ("sq", step))
    for step, chip in enumerate((c, left, right, opp)):
        push(w.at[2 * chip + 1 - k], w_sib.at[chip], sib, ("w_swap", step))

    @pl.when(k == 1)
    def _():
        pl.semaphore_wait(go, 1)
        for step in range(chips):
            swapped(step)
            for copy in exchange[step]:
                copy.start()

    arrived(relay.at[0], "a_relay_l")
    pass_right = push(relay.at[0], x.at[own_rows(left, 0)], peer_of(right), "a_opp_l")
    arrived(relay.at[1], "a_relay_r")
    pass_left = push(relay.at[1], x.at[own_rows(right, 1)], peer_of(left), "a_opp_r")
    push(w.at[2 * right + k, ds(k * ahead, ahead)], w_ahead.at[0], peer_of(right), "w_ahead_l")
    push(w.at[2 * left + k, ds(k * ahead, ahead)], w_ahead.at[1], peer_of(left), "w_ahead_r")

    total = sq[0, me]
    for step in range(1, group):
        arrived(sq.at[1, step], ("sq", step))
        total = total + sq[1, step]
    norm = jnp.sqrt(jnp.sum(total, keepdims=True))
    inverse = 1.0 / (norm + NORM_EPS)

    def scale(get, base):
        @pl.loop(0, pair // SCALE_ROWS)
        def _(r):
            part = ds(base + r * SCALE_ROWS, SCALE_ROWS)
            x[part, :] = (get(part).astype(jnp.float32) * inverse).astype(jnp.bfloat16)

    scale(lambda part: out[2 * c + k, part, :], c * pair)
    for half in range(2):
        arrived(x.at[own_rows(left, half)], ("a_left", half))
    scale(lambda part: x[part, :], left * pair)
    for half in range(2):
        arrived(x.at[own_rows(right, half)], ("a_right", half))
    scale(lambda part: x[part, :], right * pair)
    arrived(x.at[own_rows(opp, 0)], "a_opp_l")
    arrived(x.at[own_rows(opp, 1)], "a_opp_r")

    @pl.when(k == 0)
    def _():
        pl.semaphore_signal(go, inc=1, device_id={"data": sib}, device_id_type=MESH)

    scale(lambda part: x[part, :], opp * pair)

    waited = swap + sum(exchange, []) + [pass_right, pass_left]
    for copy in waited:
        copy.wait_send()
    for chip in (right, left):
        pl.semaphore_signal(free, inc=1, device_id={"data": peer_of(chip)}, device_id_type=MESH)

    order = (c, left, right, opp)

    def load_w(step):
        load(w.at[2 * order[step] + k], w_buf.at[step % 2, ds(k * rows, rows)], ("w_own", step))
        arrived(w_sib.at[order[step]], ("w_swap", step))
        load(w_sib.at[order[step]], w_buf.at[step % 2, ds((1 - k) * rows, rows)], ("w_sib", step))

    load_w(0)
    load_w(1)

    @pl.loop(0, NS_ITERS - 1)
    def _(_):
        newton_schulz_poly(x, gram, poly)
        newton_schulz_step(x, poly, pl.ds(0, cols))

    newton_schulz_poly(x, gram, poly)
    pl.semaphore_wait(free, 2)

    chunks = [pl.ds(start, WIDE) for start in range(0, cols, WIDE)]
    for n, part in enumerate(chunks):
        newton_schulz_step(x, poly, part)
        push(x.at[own_rows(opp, 0), part], relay.at[0, :, part], peer_of(right), ("c_relay_l", n))
        push(x.at[own_rows(opp, 1), part], relay.at[1, :, part], peer_of(left), ("c_relay_r", n))
        push(x.at[rest_rows(right), part], out.at[2 * c + k, rest_rows(right), part], peer_of(right), ("c_left", n))
        push(x.at[rest_rows(left), part], out.at[2 * c + k, rest_rows(left), part], peer_of(left), ("c_right", n))

    def new_rows(mat, start, size, w_rows, get):
        @pl.loop(0, size // STEP_ROWS)
        def _(r):
            w_part = w_rows(r)
            part = ds(start + r * STEP_ROWS, STEP_ROWS)
            ortho = get(part).astype(jnp.float32) * rms_scale
            out[mat, part, :] = (w_part - LEARN_RATE * (ortho + WEIGHT_DECAY * w_part)).astype(jnp.bfloat16)

    last = chips - 1

    def update(step, get):
        chip = order[step]
        arrived(w_buf.at[step % 2, ds(k * rows, rows)], ("w_own", step))
        arrived(w_buf.at[step % 2, ds((1 - k) * rows, rows)], ("w_sib", step))
        start, size = (rest_start, rest) if step in (1, 2) else (0, pair)
        new_rows(
            2 * chip + k, c * pair + start, size, lambda r: w_buf[step % 2, ds(start + r * STEP_ROWS, STEP_ROWS), :],
            lambda part: get(chip, part))
        if step + 2 < chips:
            load_w(step + 2)
        place = out.at[2 * chip + k, block(c, step)]
        if step < last:
            push(place, place, peer_of(right), ("g_left", step))
            push(place, place, peer_of(left), ("g_right", step))
        else:
            parts = [out.at[2 * chip + k, block_part(c, step, way)] for way in range(2)]
            for way in range(2):
                push(parts[way], parts[way], peer_of(right), ("g_left", step, way))
                push(parts[1 - way], parts[1 - way], peer_of(left), ("g_right", step, 1 - way))
        push(place, place, sib, ("s_own", step))

    def update_ahead():
        for n, chip in enumerate((left, right)):
            arrived(w_ahead.at[n], ("w_ahead_l", "w_ahead_r")[n])
            new_rows(
                2 * c + k, chip * pair + ahead_start, ahead, lambda r: w_ahead[n, ds(r * STEP_ROWS, STEP_ROWS), :],
                lambda part: x[part, :])
            place = out.at[2 * c + k, ahead_rows(chip)]
            push(place, place, peer_of(right), ("e_left", n))
            push(place, place, peer_of(left), ("e_right", n))
            push(place, place, sib, ("s_ahead", n))

    update(0, lambda chip, part: x[part, :])
    update_ahead()
    for n, part in enumerate(chunks):
        arrived(relay.at[0, :, part], ("c_relay_l", n))
        push(relay.at[0, :, part], out.at[2 * left + k, own_rows(right, 0), part], peer_of(right), ("c_opp_l", n))
        arrived(relay.at[1, :, part], ("c_relay_r", n))
        push(relay.at[1, :, part], out.at[2 * right + k, own_rows(left, 1), part], peer_of(left), ("c_opp_r", n))

    def returned(chip, part):
        return out[2 * chip + k, part, :]

    for n, part in enumerate(chunks):
        arrived(out.at[2 * left + k, rest_rows(c), part], ("c_left", n))
    update(1, returned)
    for n, part in enumerate(chunks):
        arrived(out.at[2 * right + k, rest_rows(c), part], ("c_right", n))
    update(2, returned)
    for n, part in enumerate(chunks):
        arrived(out.at[2 * opp + k, own_rows(c, 0), part], ("c_opp_l", n))
        arrived(out.at[2 * opp + k, own_rows(c, 1), part], ("c_opp_r", n))
    update(3, returned)

    def near(chip, step):
        return lax.rem(chip + (0, chips - 1, 1, 2)[step], chips)

    def pass_on(mat, part, peer, key):
        push(out.at[mat, part], out.at[mat, part], peer, key)

    for step in range(last):
        mat_l, mat_r = 2 * near(left, step) + k, 2 * near(right, step) + k
        arrived(out.at[mat_l, block(left, step)], ("g_left", step))
        pass_on(mat_l, block_part(left, step, 0), peer_of(right), ("f_left", step))
        pass_on(mat_l, block(left, step), sib, ("s_left", step))
        arrived(out.at[mat_r, block(right, step)], ("g_right", step))
        pass_on(mat_r, block_part(right, step, 1), peer_of(left), ("f_right", step))
        pass_on(mat_r, block(right, step), sib, ("s_right", step))
        if step == 0:
            arrived(out.at[mat_l, ahead_rows(opp)], ("e_left", 0))
            pass_on(mat_l, ahead_rows(opp), peer_of(right), "fe_left")
            pass_on(mat_l, ahead_rows(opp), sib, ("s_ahead_l", 0))
            arrived(out.at[mat_l, ahead_rows(c)], ("e_left", 1))
            pass_on(mat_l, ahead_rows(c), sib, ("s_ahead_l", 1))
            arrived(out.at[mat_r, ahead_rows(c)], ("e_right", 0))
            pass_on(mat_r, ahead_rows(c), sib, ("s_ahead_r", 0))
            arrived(out.at[mat_r, ahead_rows(opp)], ("e_right", 1))
            pass_on(mat_r, ahead_rows(opp), peer_of(left), "fe_right")
            pass_on(mat_r, ahead_rows(opp), sib, ("s_ahead_r", 1))
    mat_l, mat_r = 2 * near(left, last) + k, 2 * near(right, last) + k
    for way in range(2):
        arrived(out.at[mat_l, block_part(left, last, way)], ("g_left", last, way))
        pass_on(mat_l, block_part(left, last, way), sib, ("s_left", last, way))
        arrived(out.at[mat_r, block_part(right, last, 1 - way)], ("g_right", last, 1 - way))
        pass_on(mat_r, block_part(right, last, 1 - way), sib, ("s_right", last, 1 - way))
        if way == 0:
            load(out.at[mat_l, block_part(left, last, 0)], tail_r, "tail_r")
            load(out.at[mat_r, block_part(right, last, 1)], tail_l, "tail_l")

    for step in range(last):
        mat = 2 * near(opp, step) + k
        arrived(out.at[mat, block_part(opp, step, 0)], ("f_left", step))
        pass_on(mat, block_part(opp, step, 0), sib, ("s_far_l", step))
        arrived(out.at[mat, block_part(opp, step, 1)], ("f_right", step))
        pass_on(mat, block_part(opp, step, 1), sib, ("s_far_r", step))
        if step == 0:
            arrived(out.at[mat, ahead_rows(right)], "fe_left")
            pass_on(mat, ahead_rows(right), sib, "s_far_ahead_l")
            arrived(out.at[mat, ahead_rows(left)], "fe_right")
            pass_on(mat, ahead_rows(left), sib, "s_far_ahead_r")

    def sib_ahead(chip):
        return ds(chip * pair + (1 - k) * (pair - ahead), ahead)

    def sib_start(chip, step):
        return chip * pair + (k * ahead if step in (1, 2) else 0)

    for step in range(chips):
        size = sum(sizes[step])
        arrived(out.at[2 * near(c, step) + 1 - k, ds(sib_start(c, step), size)], ("s_own", step))
        if step == last:
            for way in range(2):
                arrived(out.at[2 * near(left, step) + 1 - k, own_rows(left, way)], ("s_left", step, way))
                arrived(out.at[2 * near(right, step) + 1 - k, own_rows(right, way)], ("s_right", step, way))
        else:
            arrived(out.at[2 * near(left, step) + 1 - k, ds(sib_start(left, step), size)], ("s_left", step))
            arrived(out.at[2 * near(right, step) + 1 - k, ds(sib_start(right, step), size)], ("s_right", step))
            mat, start = 2 * near(opp, step) + 1 - k, sib_start(opp, step)
            arrived(out.at[mat, ds(start, sizes[step][0])], ("s_far_l", step))
            arrived(out.at[mat, ds(start + sizes[step][0], sizes[step][1])], ("s_far_r", step))
        if step == 0:
            for n, chip in enumerate((left, right)):
                arrived(out.at[2 * c + 1 - k, sib_ahead(chip)], ("s_ahead", n))
            for n, chip in enumerate((opp, c)):
                arrived(out.at[2 * left + 1 - k, sib_ahead(chip)], ("s_ahead_l", n))
            for n, chip in enumerate((c, opp)):
                arrived(out.at[2 * right + 1 - k, sib_ahead(chip)], ("s_ahead_r", n))
            arrived(out.at[2 * opp + 1 - k, sib_ahead(right)], "s_far_ahead_l")
            arrived(out.at[2 * opp + 1 - k, sib_ahead(left)], "s_far_ahead_r")
    arrived(tail_r, "tail_r")
    arrived(tail_l, "tail_l")
    for copy in sent:
        if not any(copy is done for done in waited):
            copy.wait_send()


def muon_step(group, mom, grad, w):
    mats, rows, cols = mom.shape
    chips, pair = group // 2, 2 * rows
    dim = pair * chips
    hbm = pl.BlockSpec(memory_space=pl.ANY)
    vmem = pl.BlockSpec(memory_space=pltpu.VMEM)
    return pl.pallas_call(
        functools.partial(muon_kernel, group),
        in_specs=[hbm, hbm, hbm],
        out_specs=[vmem, vmem, hbm, hbm, hbm],
        out_shape=[
            pltpu.VMEM((mats, dim, cols), jnp.bfloat16),
            pltpu.VMEM((mats, rows, cols), jnp.float32),
            pltpu.HBM((chips, rows, cols), jnp.float32),
            pltpu.HBM((rows, cols), jnp.bfloat16),
            pltpu.HBM((rows, cols), jnp.bfloat16),
        ],
        scratch_shapes=[
            pltpu.VMEM((dim, cols), jnp.bfloat16),
            pltpu.VMEM((dim, dim), jnp.bfloat16),
            pltpu.VMEM((dim, dim), jnp.bfloat16),
            pltpu.VMEM((2, rows, cols), jnp.bfloat16),
            pltpu.VMEM((2, pair, cols), jnp.float32),
            pltpu.VMEM((2, rows // 2, cols), jnp.float32),
            pltpu.VMEM((2, group, 8, 128), jnp.float32),
            pltpu.SemaphoreType.DMA((128,)),
            pltpu.SemaphoreType.DMA((128,)),
            pltpu.SemaphoreType.REGULAR,
            pltpu.SemaphoreType.REGULAR,
        ],
        compiler_params=pltpu.CompilerParams(
            collective_id=0, has_side_effects=True, vmem_limit_bytes=16 * 1024 * 1024
        ),
    )(mom, grad, w)


def run_copies(pairs, sem):
    copies = [pltpu.make_async_copy(src, dst, sem.at[n]) for n, (src, dst) in enumerate(pairs)]
    for copy in copies:
        copy.start()
    for copy in copies:
        copy.wait()


def place_of(params, group):
    me = lax.axis_index("data")
    rows = params.shape[1] // group
    chips = group // 2

    def part(chip, half=None):
        start = 2 * lax.rem(chip, chips) + (0 if half is None else half)
        return ds(start * rows, 2 * rows if half is None else rows)

    return lax.div(me, 2), lax.rem(me, 2), chips, part


def store_params_kernel(group, src, dst, sem):
    c, _, chips, part = place_of(src, group)
    pairs = []
    for par in range(2):
        for step in range(1, chips):
            mat = 2 * lax.rem(c + step, chips) + par
            pairs.append((src.at[mat], dst.at[mat]))
        for step in (0, 1, chips - 1):
            where = (2 * c + par, part(c + step))
            pairs.append((src.at[where], dst.at[where]))
    run_copies(pairs, sem)


def store_first_kernel(count, src, dst, sem):
    run_copies([(src.at[i], dst.at[i]) for i in range(count)], sem)


def store_rest_kernel(count, src, _, dst, sem):
    run_copies([(src.at[i], dst.at[i]) for i in range(count, src.shape[0])], sem)


def store_late_kernel(group, params, near_l, near_r, far_l, far_r, out, sem):
    c, k, _, part = place_of(out, group)
    pieces = ((near_l, k, 0), (near_r, k, 1), (far_l, 1 - k, 0), (far_r, 1 - k, 1))
    run_copies([(src, out.at[2 * c + par, part(c + 2, half)]) for src, par, half in pieces], sem)


def store_step(kernel, full, copies):
    return pl.pallas_call(
        kernel,
        in_specs=[pl.BlockSpec(memory_space=pltpu.VMEM)],
        out_specs=pl.BlockSpec(memory_space=pl.ANY),
        out_shape=jax.ShapeDtypeStruct(full.shape, full.dtype),
        scratch_shapes=[pltpu.SemaphoreType.DMA((copies,))],
        compiler_params=pltpu.CompilerParams(vmem_limit_bytes=1024 * 1024),
        cost_estimate=pl.CostEstimate(flops=1000 * full.size, bytes_accessed=2 * full.size, transcendentals=0),
    )(full)


def store_rest(count, full, stored):
    hbm = pl.BlockSpec(memory_space=pl.ANY)
    return pl.pallas_call(
        functools.partial(store_rest_kernel, count),
        in_specs=[pl.BlockSpec(memory_space=pltpu.VMEM), hbm],
        out_specs=hbm,
        out_shape=jax.ShapeDtypeStruct(full.shape, full.dtype),
        input_output_aliases={1: 0},
        scratch_shapes=[pltpu.SemaphoreType.DMA((full.shape[0] - count,))],
        compiler_params=pltpu.CompilerParams(vmem_limit_bytes=1024 * 1024),
        cost_estimate=pl.CostEstimate(flops=1000 * full.size, bytes_accessed=2 * full.size, transcendentals=0),
    )(full, stored)


def store_late(group, params, pieces):
    hbm = pl.BlockSpec(memory_space=pl.ANY)
    return pl.pallas_call(
        functools.partial(store_late_kernel, group),
        in_specs=[hbm] + [pl.BlockSpec(memory_space=pltpu.VMEM)] * 4,
        out_specs=hbm,
        out_shape=jax.ShapeDtypeStruct(params.shape, params.dtype),
        input_output_aliases={0: 0},
        scratch_shapes=[pltpu.SemaphoreType.DMA((4,))],
        compiler_params=pltpu.CompilerParams(vmem_limit_bytes=4 * 1024 * 1024),
    )(params, *pieces)


def solution(mesh):
    group = mesh.shape["data"]
    row_spec = P("stage", "data", None)
    full_spec = P("stage", None, None)

    def local_step(w_rows, mom_rows, grad_rows):
        params, mom_new, _, tail_r, tail_l = muon_step(group, mom_rows, grad_rows, w_rows)
        to_right = [(d, (d + 2) % group) for d in range(group)]
        to_left = [(d, (d - 2) % group) for d in range(group)]
        swap = [(d, d + 1 - 2 * (d % 2)) for d in range(group)]
        near = [lax.ppermute(tail_r, "data", to_right), lax.ppermute(tail_l, "data", to_left)]
        params = store_step(functools.partial(store_params_kernel, group), params, 2 * (group // 2 + 2))
        first = mom_new.shape[0] // 4
        mom_out = store_step(functools.partial(store_first_kernel, first), mom_new, first)
        *near, params, mom_out = lax.optimization_barrier((*near, params, mom_out))
        far = [lax.ppermute(piece, "data", swap) for piece in near]
        mom_out = store_rest(first, mom_new, mom_out)
        *far, mom_out = lax.optimization_barrier((*far, mom_out))
        return store_late(group, params, near + far), mom_out

    return jax.shard_map(
        local_step, mesh=mesh, in_specs=(row_spec, row_spec, row_spec), out_specs=(full_spec, row_spec), check_vma=False
    )
```

```python
import functools
import math

import jax
import jax.numpy as jnp
from jax import lax
from jax.experimental import pallas as pl
from jax.experimental.pallas import tpu as pltpu
from jax.sharding import PartitionSpec as P

NS_ITERS = 5
MOMENTUM = 0.95
LEARN_RATE = 0.02
WEIGHT_DECAY = 0.1
NORM_EPS = 1e-7
COEF_A = 3.4445
COEF_B = -4.7750
COEF_C = 2.0315

MESH = pl.DeviceIdType.MESH
TILE = 256
WIDE = 1024
SCALE_ROWS = 32
STEP_ROWS = 16
PREFETCH = 3


def ds(start, size):
    return pl.ds(pl.multiple_of(start, math.gcd(size, STEP_ROWS)), size)


def symmetric(dst, product, finish, dim):
    for j in range(0, dim, TILE):
        cols = slice(j, j + TILE)
        block = finish(product(slice(j, dim), cols), slice(j, dim), cols)
        dst[j:, cols] = block
        for i in range(j + TILE, dim, TILE):
            dst[cols, i : i + TILE] = block[i - j : i - j + TILE].T


def newton_schulz_poly(x, gram, poly):
    dim = gram.shape[0]

    def outer(rows, cols):
        return lax.dot_general(x[rows, :], x[cols, :], (((1,), (1,)), ((), ())), preferred_element_type=jnp.float32)

    def square(rows, cols):
        return jnp.dot(gram[rows, :], gram[:, cols], preferred_element_type=jnp.float32)

    symmetric(gram, outer, lambda prod, rows, cols: prod.astype(jnp.bfloat16), dim)
    symmetric(
        poly,
        square,
        lambda prod, rows, cols: (COEF_B * gram[rows, cols].astype(jnp.float32) + COEF_C * prod).astype(jnp.bfloat16),
        dim,
    )


def newton_schulz_step(x, poly, part):
    old = x[:, part]
    prod = jnp.dot(poly[...], old, preferred_element_type=jnp.float32)
    x[:, part] = (COEF_A * old.astype(jnp.float32) + prod).astype(jnp.bfloat16)


def muon_kernel(group, mom, grad, w, out, mom_new, w_sib, tail_r, tail_l, x, gram, poly, relay, w_buf, w_ahead, sq, send, recv, go, free):
    chips = group // 2
    mats, rows, cols = mom.shape
    pair = 2 * rows
    dim = pair * chips
    rms_scale = 0.2 * math.sqrt(max(dim, cols))
    me = lax.axis_index("data")
    c, k = lax.div(me, 2), lax.rem(me, 2)
    sib = 2 * c + 1 - k
    right, left, opp = (lax.rem(c + step, chips) for step in (1, chips - 1, 2))

    def peer_of(chip):
        return 2 * chip + k

    def own_rows(chip, half=None):
        if half is None:
            return ds(chip * pair, pair)
        return ds(chip * pair + half * rows, rows)

    ahead = rows // 2
    ahead_start, rest_start, rest = k * (pair - ahead), (1 - k) * ahead, pair - ahead

    def ahead_rows(chip):
        return ds(chip * pair + ahead_start, ahead)

    def rest_rows(chip):
        return ds(chip * pair + rest_start, rest)

    split = STEP_ROWS * (rest // STEP_ROWS // 2)
    sizes = ((rows, rows), (rest - split, split), (split, rest - split), (rows, rows))

    def block(chip, step):
        return rest_rows(chip) if step in (1, 2) else own_rows(chip)

    def block_part(chip, step, way):
        start = rest_start if step in (1, 2) else 0
        return ds(chip * pair + start + way * sizes[step][0], sizes[step][way])

    def mine(chip, half=None):
        return out.at[2 * chip + k, own_rows(c, half)]

    sent, slots = [], {}

    def slot(key):
        return slots.setdefault(key, len(slots))

    def remote(src, dst, peer, key):
        copy = pltpu.make_async_remote_copy(
            src_ref=src, dst_ref=dst, send_sem=send.at[len(sent)], recv_sem=recv.at[slot(key)],
            device_id={"data": peer}, device_id_type=MESH)
        sent.append(copy)
        return copy

    def push(src, dst, peer, key):
        copy = remote(src, dst, peer, key)
        copy.start()
        return copy

    def load(src, dst, key):
        pltpu.make_async_copy(src, dst, recv.at[slot(key)]).start()

    def arrived(dst, key):
        pltpu.make_async_copy(dst, dst, recv.at[slot(key)]).wait()

    steps = (opp, left, right, c)

    def prefetch(n):
        if n < mats:
            par, step = divmod(n, chips)
            chip = steps[step]
            load(mom.at[2 * chip + par], mom_new.at[2 * chip + par], ("mom", step, par))
            load(grad.at[2 * chip + par], out.at[2 * chip + k, own_rows(left, par)], ("grad", step, par))

    for n in range(PREFETCH):
        prefetch(n)

    barrier = pltpu.get_barrier_semaphore()
    for step in range(1, group):
        pl.semaphore_signal(barrier, inc=1, device_id={"data": lax.rem(me + step, group)}, device_id_type=MESH)

    def momentum(step, chip, par):
        mat = 2 * chip + par
        base = jnp.where(k == par, c * pair + k * rows, right * pair)
        arrived(mom_new.at[mat], ("mom", step, par))
        arrived(out.at[2 * chip + k, own_rows(left, par)], ("grad", step, par))
        prefetch(par * chips + step + PREFETCH)

        def body(r, total):
            part = ds(r * STEP_ROWS, STEP_ROWS)
            low = out[2 * chip + k, ds(left * pair + par * rows + r * STEP_ROWS, STEP_ROWS), :]
            new = MOMENTUM * mom_new[mat, part, :] + low.astype(jnp.float32)
            mom_new[mat, part, :] = new
            out[2 * chip + k, ds(base + r * STEP_ROWS, STEP_ROWS), :] = new.astype(jnp.bfloat16)
            square = new * new
            lanes = square[:, :128]
            for start in range(128, cols, 128):
                lanes = lanes + square[:, start : start + 128]
            for start in range(0, STEP_ROWS, 8):
                total = total + lanes[start : start + 8]
            return total

        sq[0, mat] = lax.fori_loop(0, rows // STEP_ROWS, body, jnp.zeros((8, 128), jnp.float32))

    swap = [
        remote(out.at[2 * chip + k, own_rows(right, 0)], out.at[2 * chip + 1 - k, own_rows(c, k)], sib, ("swap", step))
        for step, chip in enumerate(steps)
    ]
    exchange = [
        [
            remote(mine(opp, 0), relay.at[0], peer_of(right), "a_relay_l"),
            remote(mine(opp, 1), relay.at[1], peer_of(left), "a_relay_r"),
        ],
        [remote(mine(left, half), x.at[own_rows(c, half)], peer_of(left), ("a_right", half)) for half in range(2)],
        [remote(mine(right, half), x.at[own_rows(c, half)], peer_of(right), ("a_left", half)) for half in range(2)],
        [],
    ]

    def swapped(step):
        arrived(mine(steps[step], 1 - k), ("swap", step))

    for step, chip in enumerate(steps):
        momentum(step, chip, 0)
        if step == 0:
            pl.semaphore_wait(barrier, group - 1)

        @pl.when(k == 1)
        def _():
            swap[step].start()

        @pl.when(k == 0)
        def _():
            for copy in exchange[step][:1]:
                copy.start()
            if step > 0:
                swapped(step - 1)
                for copy in exchange[step - 1][1:]:
                    copy.start()

    for step, chip in enumerate(steps):
        momentum(step, chip, 1)

        @pl.when(k == 0)
        def _():
            swap[step].start()
            if step == 0:
                swapped(chips - 1)

    for step in range(1, group):
        dest = lax.rem(me + step, group)
        push(sq.at[0, dest], sq.at[1, step], dest, ("sq", step))
    for step, chip in enumerate((c, left, right, opp)):
        push(w.at[2 * chip + 1 - k], w_sib.at[chip], sib, ("w_swap", step))

    @pl.when(k == 1)
    def _():
        pl.semaphore_wait(go, 1)
        for step in range(chips):
            swapped(step)
            for copy in exchange[step]:
                copy.start()

    arrived(relay.at[0], "a_relay_l")
    pass_right = push(relay.at[0], x.at[own_rows(left, 0)], peer_of(right), "a_opp_l")
    arrived(relay.at[1], "a_relay_r")
    pass_left = push(relay.at[1], x.at[own_rows(right, 1)], peer_of(left), "a_opp_r")
    push(w.at[2 * right + k, ds(k * ahead, ahead)], w_ahead.at[0], peer_of(right), "w_ahead_l")
    push(w.at[2 * left + k, ds(k * ahead, ahead)], w_ahead.at[1], peer_of(left), "w_ahead_r")

    total = sq[0, me]
    for step in range(1, group):
        arrived(sq.at[1, step], ("sq", step))
        total = total + sq[1, step]
    norm = jnp.sqrt(jnp.sum(total, keepdims=True))
    inverse = 1.0 / (norm + NORM_EPS)

    def scale(get, base):
        @pl.loop(0, pair // SCALE_ROWS)
        def _(r):
            part = ds(base + r * SCALE_ROWS, SCALE_ROWS)
            x[part, :] = (get(part).astype(jnp.float32) * inverse).astype(jnp.bfloat16)

    scale(lambda part: out[2 * c + k, part, :], c * pair)
    for half in range(2):
        arrived(x.at[own_rows(left, half)], ("a_left", half))
    scale(lambda part: x[part, :], left * pair)
    for half in range(2):
        arrived(x.at[own_rows(right, half)], ("a_right", half))
    scale(lambda part: x[part, :], right * pair)
    arrived(x.at[own_rows(opp, 0)], "a_opp_l")
    arrived(x.at[own_rows(opp, 1)], "a_opp_r")

    @pl.when(k == 0)
    def _():
        pl.semaphore_signal(go, inc=1, device_id={"data": sib}, device_id_type=MESH)

    scale(lambda part: x[part, :], opp * pair)

    waited = swap + sum(exchange, []) + [pass_right, pass_left]
    for copy in waited:
        copy.wait_send()
    for chip in (right, left):
        pl.semaphore_signal(free, inc=1, device_id={"data": peer_of(chip)}, device_id_type=MESH)

    order = (c, left, right, opp)

    def load_w(step):
        load(w.at[2 * order[step] + k], w_buf.at[step % 2, ds(k * rows, rows)], ("w_own", step))
        arrived(w_sib.at[order[step]], ("w_swap", step))
        load(w_sib.at[order[step]], w_buf.at[step % 2, ds((1 - k) * rows, rows)], ("w_sib", step))

    load_w(0)
    load_w(1)

    @pl.loop(0, NS_ITERS - 1)
    def _(_):
        newton_schulz_poly(x, gram, poly)
        newton_schulz_step(x, poly, pl.ds(0, cols))

    newton_schulz_poly(x, gram, poly)
    pl.semaphore_wait(free, 2)

    chunks = [pl.ds(start, WIDE) for start in range(0, cols, WIDE)]
    for n, part in enumerate(chunks):
        newton_schulz_step(x, poly, part)
        push(x.at[own_rows(opp, 0), part], relay.at[0, :, part], peer_of(right), ("c_relay_l", n))
        push(x.at[own_rows(opp, 1), part], relay.at[1, :, part], peer_of(left), ("c_relay_r", n))
        push(x.at[rest_rows(right), part], out.at[2 * c + k, rest_rows(right), part], peer_of(right), ("c_left", n))
        push(x.at[rest_rows(left), part], out.at[2 * c + k, rest_rows(left), part], peer_of(left), ("c_right", n))

    def new_rows(mat, start, size, w_rows, get):
        @pl.loop(0, size // STEP_ROWS)
        def _(r):
            w_part = w_rows(r)
            part = ds(start + r * STEP_ROWS, STEP_ROWS)
            ortho = get(part).astype(jnp.float32) * rms_scale
            out[mat, part, :] = (w_part - LEARN_RATE * (ortho + WEIGHT_DECAY * w_part)).astype(jnp.bfloat16)

    last = chips - 1

    def update(step, get):
        chip = order[step]
        arrived(w_buf.at[step % 2, ds(k * rows, rows)], ("w_own", step))
        arrived(w_buf.at[step % 2, ds((1 - k) * rows, rows)], ("w_sib", step))
        start, size = (rest_start, rest) if step in (1, 2) else (0, pair)
        new_rows(
            2 * chip + k, c * pair + start, size, lambda r: w_buf[step % 2, ds(start + r * STEP_ROWS, STEP_ROWS), :],
            lambda part: get(chip, part))
        if step + 2 < chips:
            load_w(step + 2)
        place = out.at[2 * chip + k, block(c, step)]
        if step < last:
            push(place, place, peer_of(right), ("g_left", step))
            push(place, place, peer_of(left), ("g_right", step))
        else:
            parts = [out.at[2 * chip + k, block_part(c, step, way)] for way in range(2)]
            for way in range(2):
                push(parts[way], parts[way], peer_of(right), ("g_left", step, way))
                push(parts[1 - way], parts[1 - way], peer_of(left), ("g_right", step, 1 - way))
        push(place, place, sib, ("s_own", step))

    def update_ahead():
        for n, chip in enumerate((left, right)):
            arrived(w_ahead.at[n], ("w_ahead_l", "w_ahead_r")[n])
            new_rows(
                2 * c + k, chip * pair + ahead_start, ahead, lambda r: w_ahead[n, ds(r * STEP_ROWS, STEP_ROWS), :],
                lambda part: x[part, :])
            place = out.at[2 * c + k, ahead_rows(chip)]
            push(place, place, peer_of(right), ("e_left", n))
            push(place, place, peer_of(left), ("e_right", n))
            push(place, place, sib, ("s_ahead", n))

    update(0, lambda chip, part: x[part, :])
    update_ahead()
    for n, part in enumerate(chunks):
        arrived(relay.at[0, :, part], ("c_relay_l", n))
        push(relay.at[0, :, part], out.at[2 * left + k, own_rows(right, 0), part], peer_of(right), ("c_opp_l", n))
        arrived(relay.at[1, :, part], ("c_relay_r", n))
        push(relay.at[1, :, part], out.at[2 * right + k, own_rows(left, 1), part], peer_of(left), ("c_opp_r", n))

    def returned(chip, part):
        return out[2 * chip + k, part, :]

    for n, part in enumerate(chunks):
        arrived(out.at[2 * left + k, rest_rows(c), part], ("c_left", n))
    update(1, returned)
    for n, part in enumerate(chunks):
        arrived(out.at[2 * right + k, rest_rows(c), part], ("c_right", n))
    update(2, returned)
    for n, part in enumerate(chunks):
        arrived(out.at[2 * opp + k, own_rows(c, 0), part], ("c_opp_l", n))
        arrived(out.at[2 * opp + k, own_rows(c, 1), part], ("c_opp_r", n))
    update(3, returned)

    def near(chip, step):
        return lax.rem(chip + (0, chips - 1, 1, 2)[step], chips)

    def pass_on(mat, part, peer, key):
        push(out.at[mat, part], out.at[mat, part], peer, key)

    for step in range(last):
        mat_l, mat_r = 2 * near(left, step) + k, 2 * near(right, step) + k
        arrived(out.at[mat_l, block(left, step)], ("g_left", step))
        pass_on(mat_l, block_part(left, step, 0), peer_of(right), ("f_left", step))
        pass_on(mat_l, block(left, step), sib, ("s_left", step))
        arrived(out.at[mat_r, block(right, step)], ("g_right", step))
        pass_on(mat_r, block_part(right, step, 1), peer_of(left), ("f_right", step))
        pass_on(mat_r, block(right, step), sib, ("s_right", step))
        if step == 0:
            arrived(out.at[mat_l, ahead_rows(opp)], ("e_left", 0))
            pass_on(mat_l, ahead_rows(opp), peer_of(right), "fe_left")
            pass_on(mat_l, ahead_rows(opp), sib, ("s_ahead_l", 0))
            arrived(out.at[mat_l, ahead_rows(c)], ("e_left", 1))
            pass_on(mat_l, ahead_rows(c), sib, ("s_ahead_l", 1))
            arrived(out.at[mat_r, ahead_rows(c)], ("e_right", 0))
            pass_on(mat_r, ahead_rows(c), sib, ("s_ahead_r", 0))
            arrived(out.at[mat_r, ahead_rows(opp)], ("e_right", 1))
            pass_on(mat_r, ahead_rows(opp), peer_of(left), "fe_right")
            pass_on(mat_r, ahead_rows(opp), sib, ("s_ahead_r", 1))
    mat_l, mat_r = 2 * near(left, last) + k, 2 * near(right, last) + k
    for way in range(2):
        arrived(out.at[mat_l, block_part(left, last, way)], ("g_left", last, way))
        pass_on(mat_l, block_part(left, last, way), sib, ("s_left", last, way))
        arrived(out.at[mat_r, block_part(right, last, 1 - way)], ("g_right", last, 1 - way))
        pass_on(mat_r, block_part(right, last, 1 - way), sib, ("s_right", last, 1 - way))
        if way == 0:
            load(out.at[mat_l, block_part(left, last, 0)], tail_r, "tail_r")
            load(out.at[mat_r, block_part(right, last, 1)], tail_l, "tail_l")

    for step in range(last):
        mat = 2 * near(opp, step) + k
        arrived(out.at[mat, block_part(opp, step, 0)], ("f_left", step))
        pass_on(mat, block_part(opp, step, 0), sib, ("s_far_l", step))
        arrived(out.at[mat, block_part(opp, step, 1)], ("f_right", step))
        pass_on(mat, block_part(opp, step, 1), sib, ("s_far_r", step))
        if step == 0:
            arrived(out.at[mat, ahead_rows(right)], "fe_left")
            pass_on(mat, ahead_rows(right), sib, "s_far_ahead_l")
            arrived(out.at[mat, ahead_rows(left)], "fe_right")
            pass_on(mat, ahead_rows(left), sib, "s_far_ahead_r")

    def sib_ahead(chip):
        return ds(chip * pair + (1 - k) * (pair - ahead), ahead)

    def sib_start(chip, step):
        return chip * pair + (k * ahead if step in (1, 2) else 0)

    for step in range(chips):
        size = sum(sizes[step])
        arrived(out.at[2 * near(c, step) + 1 - k, ds(sib_start(c, step), size)], ("s_own", step))
        if step == last:
            for way in range(2):
                arrived(out.at[2 * near(left, step) + 1 - k, own_rows(left, way)], ("s_left", step, way))
                arrived(out.at[2 * near(right, step) + 1 - k, own_rows(right, way)], ("s_right", step, way))
        else:
            arrived(out.at[2 * near(left, step) + 1 - k, ds(sib_start(left, step), size)], ("s_left", step))
            arrived(out.at[2 * near(right, step) + 1 - k, ds(sib_start(right, step), size)], ("s_right", step))
            mat, start = 2 * near(opp, step) + 1 - k, sib_start(opp, step)
            arrived(out.at[mat, ds(start, sizes[step][0])], ("s_far_l", step))
            arrived(out.at[mat, ds(start + sizes[step][0], sizes[step][1])], ("s_far_r", step))
        if step == 0:
            for n, chip in enumerate((left, right)):
                arrived(out.at[2 * c + 1 - k, sib_ahead(chip)], ("s_ahead", n))
            for n, chip in enumerate((opp, c)):
                arrived(out.at[2 * left + 1 - k, sib_ahead(chip)], ("s_ahead_l", n))
            for n, chip in enumerate((c, opp)):
                arrived(out.at[2 * right + 1 - k, sib_ahead(chip)], ("s_ahead_r", n))
            arrived(out.at[2 * opp + 1 - k, sib_ahead(right)], "s_far_ahead_l")
            arrived(out.at[2 * opp + 1 - k, sib_ahead(left)], "s_far_ahead_r")
    arrived(tail_r, "tail_r")
    arrived(tail_l, "tail_l")
    for copy in sent:
        if not any(copy is done for done in waited):
            copy.wait_send()


def muon_step(group, mom, grad, w):
    mats, rows, cols = mom.shape
    chips, pair = group // 2, 2 * rows
    dim = pair * chips
    hbm = pl.BlockSpec(memory_space=pl.ANY)
    vmem = pl.BlockSpec(memory_space=pltpu.VMEM)
    return pl.pallas_call(
        functools.partial(muon_kernel, group),
        in_specs=[hbm, hbm, hbm],
        out_specs=[vmem, vmem, hbm, hbm, hbm],
        out_shape=[
            pltpu.VMEM((mats, dim, cols), jnp.bfloat16),
            pltpu.VMEM((mats, rows, cols), jnp.float32),
            pltpu.HBM((chips, rows, cols), jnp.float32),
            pltpu.HBM((rows, cols), jnp.bfloat16),
            pltpu.HBM((rows, cols), jnp.bfloat16),
        ],
        scratch_shapes=[
            pltpu.VMEM((dim, cols), jnp.bfloat16),
            pltpu.VMEM((dim, dim), jnp.bfloat16),
            pltpu.VMEM((dim, dim), jnp.bfloat16),
            pltpu.VMEM((2, rows, cols), jnp.bfloat16),
            pltpu.VMEM((2, pair, cols), jnp.float32),
            pltpu.VMEM((2, rows // 2, cols), jnp.float32),
            pltpu.VMEM((2, group, 8, 128), jnp.float32),
            pltpu.SemaphoreType.DMA((128,)),
            pltpu.SemaphoreType.DMA((128,)),
            pltpu.SemaphoreType.REGULAR,
            pltpu.SemaphoreType.REGULAR,
        ],
        compiler_params=pltpu.CompilerParams(
            collective_id=0, has_side_effects=True, vmem_limit_bytes=16 * 1024 * 1024
        ),
    )(mom, grad, w)


def run_copies(pairs, sem):
    copies = [pltpu.make_async_copy(src, dst, sem.at[n]) for n, (src, dst) in enumerate(pairs)]
    for copy in copies:
        copy.start()
    for copy in copies:
        copy.wait()


def place_of(params, group):
    me = lax.axis_index("data")
    rows = params.shape[1] // group
    chips = group // 2

    def part(chip, half=None):
        start = 2 * lax.rem(chip, chips) + (0 if half is None else half)
        return ds(start * rows, 2 * rows if half is None else rows)

    return lax.div(me, 2), lax.rem(me, 2), chips, part


def store_params_kernel(group, src, dst, sem):
    c, _, chips, part = place_of(src, group)
    pairs = []
    for par in range(2):
        for step in range(1, chips):
            mat = 2 * lax.rem(c + step, chips) + par
            pairs.append((src.at[mat], dst.at[mat]))
        for step in (0, 1, chips - 1):
            where = (2 * c + par, part(c + step))
            pairs.append((src.at[where], dst.at[where]))
    run_copies(pairs, sem)


def store_first_kernel(count, src, dst, sem):
    run_copies([(src.at[i], dst.at[i]) for i in range(count)], sem)


def store_rest_kernel(count, src, _, dst, sem):
    run_copies([(src.at[i], dst.at[i]) for i in range(count, src.shape[0])], sem)


def store_late_kernel(group, params, near_l, near_r, far_l, far_r, out, sem):
    c, k, _, part = place_of(out, group)
    pieces = ((near_l, k, 0), (near_r, k, 1), (far_l, 1 - k, 0), (far_r, 1 - k, 1))
    run_copies([(src, out.at[2 * c + par, part(c + 2, half)]) for src, par, half in pieces], sem)


def store_step(kernel, full, copies):
    return pl.pallas_call(
        kernel,
        in_specs=[pl.BlockSpec(memory_space=pltpu.VMEM)],
        out_specs=pl.BlockSpec(memory_space=pl.ANY),
        out_shape=jax.ShapeDtypeStruct(full.shape, full.dtype),
        scratch_shapes=[pltpu.SemaphoreType.DMA((copies,))],
        compiler_params=pltpu.CompilerParams(vmem_limit_bytes=1024 * 1024),
        cost_estimate=pl.CostEstimate(flops=1000 * full.size, bytes_accessed=2 * full.size, transcendentals=0),
    )(full)


def store_rest(count, full, stored):
    hbm = pl.BlockSpec(memory_space=pl.ANY)
    return pl.pallas_call(
        functools.partial(store_rest_kernel, count),
        in_specs=[pl.BlockSpec(memory_space=pltpu.VMEM), hbm],
        out_specs=hbm,
        out_shape=jax.ShapeDtypeStruct(full.shape, full.dtype),
        input_output_aliases={1: 0},
        scratch_shapes=[pltpu.SemaphoreType.DMA((full.shape[0] - count,))],
        compiler_params=pltpu.CompilerParams(vmem_limit_bytes=1024 * 1024),
        cost_estimate=pl.CostEstimate(flops=1000 * full.size, bytes_accessed=2 * full.size, transcendentals=0),
    )(full, stored)


def store_late(group, params, pieces):
    hbm = pl.BlockSpec(memory_space=pl.ANY)
    return pl.pallas_call(
        functools.partial(store_late_kernel, group),
        in_specs=[hbm] + [pl.BlockSpec(memory_space=pltpu.VMEM)] * 4,
        out_specs=hbm,
        out_shape=jax.ShapeDtypeStruct(params.shape, params.dtype),
        input_output_aliases={0: 0},
        scratch_shapes=[pltpu.SemaphoreType.DMA((4,))],
        compiler_params=pltpu.CompilerParams(vmem_limit_bytes=4 * 1024 * 1024),
    )(params, *pieces)


def solution(mesh):
    group = mesh.shape["data"]
    row_spec = P("stage", "data", None)
    full_spec = P("stage", None, None)

    def local_step(w_rows, mom_rows, grad_rows):
        params, mom_new, _, tail_r, tail_l = muon_step(group, mom_rows, grad_rows, w_rows)
        to_right = [(d, (d + 2) % group) for d in range(group)]
        to_left = [(d, (d - 2) % group) for d in range(group)]
        swap = [(d, d + 1 - 2 * (d % 2)) for d in range(group)]
        near = [lax.ppermute(tail_r, "data", to_right), lax.ppermute(tail_l, "data", to_left)]
        params = store_step(functools.partial(store_params_kernel, group), params, 2 * (group // 2 + 2))
        first = 3 * mom_new.shape[0] // 8
        mom_out = store_step(functools.partial(store_first_kernel, first), mom_new, first)
        *near, params, mom_out = lax.optimization_barrier((*near, params, mom_out))
        far = [lax.ppermute(piece, "data", swap) for piece in near]
        mom_out = store_rest(first, mom_new, mom_out)
        *far, mom_out = lax.optimization_barrier((*far, mom_out))
        return store_late(group, params, near + far), mom_out

    return jax.shard_map(
        local_step, mesh=mesh, in_specs=(row_spec, row_spec, row_spec), out_specs=(full_spec, row_spec), check_vma=False
    )
```
